32 devices in a mesh: gx: 4 (over y, x), gy: 4 (over z), gz: 2 (over core).
Axes of the slice: x: 2, y: 2, z: 4, core: 2. Of those that a mesh axis runs over, the one named last changes fastest.
Arguments:
- charges: float32 [128, 256, 256], P('gx', 'gy', 'gz'), may hold values from -8 to 8
- kernel_taps: float32 [5, 3, 17], replicated, may hold values from 0.08 to 0.4
Outputs:
- potential: float32 [128, 256, 256], P('gx', 'gy', 'gz')
The draws below stay inside these ranges and needn't reach their ends.
All inputs are finite; a program needn't handle non-finite values.
Results may differ from the reference program's by a relative error of at most 0.00029.
Values sent between devices are 32-bit elements; how exact they have to be, the bound alone decides.
A program may use at most 128 MiB of HBM per device.

```python
import math
import jax
import jax.numpy as jnp
from jax import lax

LEVELS = 5
TAPS = 17
NX = 128
NY = 256
NZ = 256


def block_levels(stream_key, shape, cuts, smallest, top_value):
    def one(dim, blocks):
        steps = jax.random.uniform(jax.random.fold_in(jax.random.fold_in(stream_key, 6), dim), (blocks,), jnp.float32, smallest / len(cuts), top_value / len(cuts))
        return jnp.repeat(jnp.exp(steps), shape[dim] // blocks).reshape((-1,) + (1,) * (len(shape) - dim - 1))

    loudness = one(*cuts[0])
    for cut in cuts[1:]:
        loudness = loudness * one(*cut)
    return loudness


def normal_values(stream_key, shape, width, most, shards=(), kind=jnp.bfloat16):
    factor_of = block_levels(stream_key, shape, shards, -0.22, 0.18) if shards else 1.0
    values = jax.random.normal(stream_key, shape, jnp.float32) * width * factor_of
    return jnp.minimum(jnp.maximum(values, -most), most).astype(kind)


def setup_inputs(seed: int = 0) -> dict:
    arg_keys = jax.random.split(jax.random.key(seed), 3)
    charges = normal_values(arg_keys[0], (NX, NY, NZ), 1.0, 8.0, ((0, 4), (1, 4), (2, 2)), jnp.float32)
    kernel_taps = jnp.clip(jnp.exp(jax.random.uniform(arg_keys[1], (LEVELS, 3, TAPS), jnp.float32, math.log(0.08), math.log(0.4))), 0.08, 0.4)
    return dict(charges=charges, kernel_taps=kernel_taps)


CUBIC = (-0.0625, 0.0, 0.5625, 1.0, 0.5625, 0.0, -0.0625)
PATTERNS = ("ij,jbc->ibc", "ij,ajc->aic", "ij,abj->abi")


def picks_matrix(weights, offsets):
    count = weights.shape[0]
    picks = (offsets[None, :, :] == jnp.arange(count, dtype=jnp.int32)[:, None, None]).astype(jnp.float32)
    return jnp.sum(weights.astype(jnp.float32)[:, None, None] * picks, axis=0)


def apply_axis(matrix, values, axis):
    return jnp.einsum(PATTERNS[axis], matrix, values, precision=lax.Precision.HIGHEST)


def stencil_padded(padded, taps_level):
    for axis in range(3):
        length = padded.shape[axis] - 16
        total = jnp.zeros(padded.shape[:axis] + (length,) + padded.shape[axis + 1:], jnp.float32)
        for offset in range(17):
            total = total + taps_level[axis, offset] * lax.slice_in_dim(padded, offset, offset + length, 1, axis)
        padded = total
    return padded


def restrict_padded(padded):
    cubic = jnp.array(CUBIC, jnp.float32)
    for axis in range(3):
        length = padded.shape[axis] - 6
        offsets = jnp.arange(length + 6, dtype=jnp.int32)[None, :] - 2 * jnp.arange(length // 2, dtype=jnp.int32)[:, None]
        padded = apply_axis(picks_matrix(cubic, offsets), padded, axis)
    return padded


def prolong_padded(padded):
    cubic = jnp.array(CUBIC, jnp.float32)
    for axis in range(3):
        length = padded.shape[axis] - 4
        offsets = 7 + jnp.arange(2 * length, dtype=jnp.int32)[:, None] - 2 * jnp.arange(length + 4, dtype=jnp.int32)[None, :]
        padded = apply_axis(picks_matrix(cubic, offsets), padded, axis)
    return padded


def reference(charges, kernel_taps):
    levels_charge = [charges]
    for level in range(1, LEVELS):
        levels_charge.append(restrict_padded(jnp.pad(levels_charge[-1], 3)))
    result = stencil_padded(jnp.pad(levels_charge[LEVELS - 1], 8), kernel_taps[LEVELS - 1])
    for level in range(LEVELS - 2, -1, -1):
        result = stencil_padded(jnp.pad(levels_charge[level], 8), kernel_taps[level]) + prolong_padded(jnp.pad(result, 2))
    return result
```

```python
import functools

import jax
import jax.numpy as jnp
from jax import lax
from jax.experimental import pallas as pl
from jax.experimental.pallas import tpu as pltpu
from jax.sharding import PartitionSpec as P

F32, BF16 = jnp.float32, jnp.bfloat16
LANES = 128
U0, U1, U2, U3 = 4, 4, 4, 5
AXES = ("gx", "gy", "gz")
ODD = (-0.0625, 0.5625, 0.5625, -0.0625)
SIDES = tuple((a, b) for a in (-1, 0, 1) for b in (-1, 0, 1) if (a, b) != (0, 0))


def split(v):
    hi = v.astype(BF16)
    return hi, (v - hi.astype(F32)).astype(BF16)


def mm(a, b):
    return jnp.dot(a, b, preferred_element_type=F32)


def exact(a, b):
    return jnp.dot(a, b, preferred_element_type=F32, precision=lax.Precision.HIGHEST)


def dot_right(v, w):
    hi, lo = split(v)
    out = mm(hi, w[0][...]) + mm(lo, w[0][...])
    return out if w[1] is None else out + mm(hi, w[1][...])


def dot_left(w_ref, v, terms):
    hi, lo = split(v)
    return mm(w_ref[...], jnp.concatenate([hi, lo, hi][:terms], axis=0))


def grids(rows, cols):
    return (
        lax.broadcasted_iota(jnp.int32, (rows, cols), 0),
        lax.broadcasted_iota(jnp.int32, (rows, cols), 1),
    )


def pick(taps, level, axis, diff, ok):
    out = jnp.zeros(diff.shape, F32)
    for t in range(17):
        out = jnp.where(diff == t, taps[level, axis, t], out)
    return jnp.where(ok, out, 0.0)


def cubic(diff, ok):
    d = jnp.abs(diff)
    out = jnp.where(d == 0, 1.0, jnp.where(d == 1, 0.5625, jnp.where(d == 3, -0.0625, 0.0)))
    return jnp.where(ok, out, 0.0).astype(F32)


def up(n, m):
    return -(-n // m) * m


def inside(v, n):
    return (v >= 0) & (v < n)


def kernel(counts, dims, taps, x_ref, out_ref, e0, l0, r0, y0, y1, e1, l1, r1, t1, s1, g2, u2, y2, p2, d1,
           w0h, w0l, m0, w1h, w1l, m1, w2h, w2l, m2, c2, pz2, py2, pz1, py1,
           sa, ra, sza, rza, sb, rb, szb, rzb, sg, rg):
    nx, ny, nz = counts
    bx, by, bz = dims
    here = tuple(lax.axis_index(a) for a in AXES)
    gx, gy, gz = here
    cx, cy, cz = bx // 2, by // 2, bz // 2
    fx, fy, fz = bx // 4, by // 4, bz // 4

    def there(dx, dy, dz):
        return inside(gx + dx, nx) & inside(gy + dy, ny) & inside(gz + dz, nz)

    partners = [(a, b, 0) for a, b in SIDES] + [(0, 0, -1), (0, 0, 1)]
    for dim, n in enumerate(counts):
        for d in range(2, n):
            for sgn in (-d, d):
                partners.append(tuple(sgn if k == dim else 0 for k in range(3)))
    barrier = pltpu.get_barrier_semaphore()
    total = jnp.int32(0)
    for p in partners:
        ok = there(*p)
        total = total + ok.astype(jnp.int32)

        @pl.when(ok)
        def _(p=p):
            pl.semaphore_signal(
                barrier, inc=1, device_id=(gx + p[0], gy + p[1], gz + p[2]),
                device_id_type=pl.DeviceIdType.MESH,
            )

    def zero_halo(ref, wx, wy, mx, my):
        for a, b in SIDES:
            @pl.when(jnp.logical_not(there(a, b, 0)))
            def _(a=a, b=b):
                xs = {-1: (0, wx), 0: (wx, mx), 1: (wx + mx, wx)}[a]
                ys = {-1: (0, wy), 0: (wy, my), 1: (wy + my, wy)}[b]
                ref[pl.ds(*xs), pl.ds(*ys), :] = jnp.zeros((xs[1], ys[1], LANES), F32)

    zero_halo(e0, 8, 8, bx, by)
    zero_halo(e1, 5, 16, cx // 2, cy)
    pl.semaphore_wait(barrier, total)

    def exchange(src, base, ref, wx, wy, mx, my, send, recv, near, far=False):
        out = []
        for k, (a, b) in enumerate(SIDES):
            if far and a == 0:
                continue
            rest_x = wx - near
            if far:
                sx = {-1: (near, rest_x), 1: (mx - wx, rest_x)}[a]
                tx = {-1: (wx + mx + near, rest_x), 1: (0, rest_x)}[a]
            else:
                sx = {-1: (0, near), 0: (0, mx), 1: (mx - near, near)}[a]
                tx = {-1: (wx + mx, near), 0: (wx, mx), 1: (wx - near, near)}[a]
            k += len(SIDES) if far else 0
            sy = {-1: (0, wy), 0: (0, my), 1: (my - wy, wy)}[b]
            ty = {-1: (wy + my, wy), 0: (wy, my), 1: (0, wy)}[b]
            copy = pltpu.make_async_remote_copy(
                src_ref=src.at[pl.ds(base[0] + sx[0], sx[1]), pl.ds(base[1] + sy[0], sy[1]), :],
                dst_ref=ref.at[pl.ds(*tx), pl.ds(*ty), :],
                send_sem=send.at[k], recv_sem=recv.at[k],
                device_id=(gx + a, gy + b, gz), device_id_type=pl.DeviceIdType.MESH,
            )
            out.append((there(a, b, 0), there(-a, -b, 0), copy))
        return out

    def across(src, base, left, right, ranges, send, recv):
        out = []
        for k, (ofs, xs, ys) in enumerate(ranges):
            for h, (dz, dst) in enumerate(((1, left), (-1, right))):
                source = (src if k == 0 else base)
                copy = pltpu.make_async_remote_copy(
                    src_ref=source.at[pl.ds(xs[0] - ofs[0], xs[1]), pl.ds(ys[0] - ofs[1], ys[1]), :],
                    dst_ref=dst.at[pl.ds(*xs), pl.ds(*ys), :],
                    send_sem=send.at[k, h], recv_sem=recv.at[k, h],
                    device_id=(gx, gy, gz + dz), device_id_type=pl.DeviceIdType.MESH,
                )
                out.append((there(0, 0, dz), there(0, 0, -dz), copy))
        return out

    def start(copies):
        for to, _, copy in copies:
            pl.when(to)(copy.start)

    def arrive(copies):
        for _, fro, copy in copies:
            pl.when(fro)(copy.wait_recv)

    def left_over(copies):
        for to, _, copy in copies:
            pl.when(to)(copy.wait_send)

    def pieces(wx, wy, mx, my, direct, near):
        o = (wx, wy) if direct else (0, 0)
        n = (0, 0)
        return [
            (o, (wx, mx), (wy, my)),
            (n, (wx - near, near), (0, my + 2 * wy)),
            (n, (wx + mx, near), (0, my + 2 * wy)),
            (n, (wx, mx), (0, wy)),
            (n, (wx, mx), (wy + my, wy)),
            (n, (0, wx - near), (0, my + 2 * wy)),
            (n, (wx + mx + near, wx - near), (0, my + 2 * wy)),
        ]

    xa = exchange(x_ref, (0, 0), e0, 8, 8, bx, by, sa, ra, 4)
    xa_far = exchange(x_ref, (0, 0), e0, 8, 8, bx, by, sa, ra, 4, True)
    za = across(x_ref, e0, l0, r0, pieces(8, 8, bx, by, True, 4), sza, rza)
    start(xa)
    start(za[:2])
    e0[pl.ds(8, bx), pl.ds(8, by), :] = x_ref[...]

    def put(h, l, v):
        hi, lo = split(v)
        h[...] = hi
        if l is not None:
            l[...] = lo

    def stack(ref, v, terms):
        hi, lo = split(v)
        ref[...] = jnp.concatenate([hi, hi, lo][:terms], axis=1)

    i, j = grids(2 * bz, bz)
    pos = jnp.where(i < bz + bz // 2, i, i - 2 * bz)
    k0 = pick(taps, 0, 2, pos - j + 8, inside(pos, bz + 8) | inside(pos + 8, 8))
    rz = cubic(pos - 2 * j, j < cz)
    put(w0h, w0l, jnp.concatenate([k0, rz], axis=1))
    i, j = grids(by + cy, by + 16)
    stack(m0, jnp.where(i < by, pick(taps, 0, 1, j - i, i < by), cubic(j - 8 - 2 * (i - by), i >= by)), 3)
    lane = lax.broadcasted_iota(jnp.int32, (1, LANES), 1)
    i, j = grids(2 * cz, LANES)
    pos = jnp.where(i < cz + cz // 2, i, i - 2 * cz)
    kk = j - 2
    top = cz + 4
    ok = (j < top) & inside(gz * cz + kk, nz * cz)
    rlane = LANES - fz
    put(w1h, w1l, pick(taps, 1, 2, pos - kk + 8, ok) + cubic(pos - 2 * (j - rlane), j >= rlane))
    ry1 = up(cy + 4, 8)
    i, j = grids(ry1 + fy, cy + 32)
    ok = (i < cy + 4) & inside(gy * cy + i - 2, ny * cy)
    stack(m1, pick(taps, 1, 1, j - 16 - (i - 2) + 8, ok) + cubic(j - 16 - 2 * (i - ry1), i >= ry1), 3)

    def plain(axis, level, n, pad, turned):
        i, j = grids(pad, pad)
        d = (i - j if turned else j - i) + 8
        return pick(taps, level, axis, d, (i < n) & (j < n))

    def rest(n, pad, big, turned_r):
        i, j = grids(*((big, pad) if turned_r else (pad, big)))
        c, f = (j, i) if turned_r else (i, j)
        return cubic(f - 2 * c, (c < n) & (f < 2 * n))

    def operators(axis, n2, first, rows, count):
        n3, n4 = n2 // 2, n2 // 4
        q = up(n2, LANES)
        i, j = grids(rows, q)
        g = first + i
        ok = (i < count) & inside(g, n2)
        one = pick(taps, 2, axis, j - g + 8, ok & (j < n2))
        pr = cubic(g - 2 * j, ok & (j < n3))
        r23, r34 = rest(n3, q, q, False), rest(n4, q, q, False)
        p34 = rest(n4, q, q, True)
        two = exact(exact(pr, plain(axis, 3, n3, q, False)), r23)
        three = exact(exact(exact(exact(pr, p34), plain(axis, 4, n4, q, False)), r34), r23)
        return one, two, three

    n2x, n2y, n2z = nx * fx, ny * fy, nz * fz
    ez, ey, ex = fz + 5, fy + 5, fx + 5
    tz = 40
    ops = operators(2, n2z, gz * fz - 2, tz, ez)
    cols = jnp.concatenate(list(ops) + [jnp.zeros((LANES - 3 * tz, ops[0].shape[1]), F32)], axis=0)
    put(w2h, w2l, cols.T)
    ty = up(ey, 8)
    ops = operators(1, n2y, gy * fy - 2, ty, ey)
    stack(m2, jnp.concatenate(list(ops), axis=0)[:, :n2y], 3)
    tx = up(ex, 8)
    ops = operators(0, n2x, gx * fx - 2, tx, ex)
    tall = [o.T for o in ops]
    for r in range(ex):
        a, b, c = (o[:n2x, r:r + 1] for o in tall)
        c2[r] = jnp.where(lane < tz, a, jnp.where(lane < 2 * tz, b, c))
    i, j = grids(LANES, LANES)
    src = i - jnp.where(i < tz, 0, jnp.where(i < 2 * tz, tz, 2 * tz)) - 2
    put(pz2, None, cubic((j - 2) - 2 * src, (i < 3 * tz) & (src < fz + 3) & (j < top) & inside(gz * cz + j - 2, nz * cz)))
    i, j = grids(ry1, up(ty, 16))
    stack(py2, cubic((i - 2) - 2 * (j - 2), (j < ey) & (i < cy + 4) & inside(gy * cy + i - 2, ny * cy)), 2)
    i, j = grids(LANES, bz)
    put(pz1, None, cubic(j - 2 * (i - 2), i < top))
    i, j = grids(by, up(ry1, 16))
    stack(py1, cubic(i - 2 * (j - 2), j < cy + 4), 2)

    flat = [k for k, (a, _) in enumerate(SIDES) if a == 0]
    tilted = [k for k, (a, _) in enumerate(SIDES) if a != 0]
    arrive([xa[k] for k in flat])
    start(za[6:10])
    arrive(za[:2] + za[6:10])

    wide = by + 16
    has_r, has_l = there(0, 0, 1), there(0, 0, -1)
    mask_r, mask_l = (lane < LANES // 2) & has_r, (lane >= LANES // 2) & has_l
    step0 = 4

    def level0(c):
        at = pl.ds(c * step0, step0)
        own = e0[at].reshape(step0 * wide, LANES)
        other = jnp.where(
            mask_r, r0[at].reshape(step0 * wide, LANES),
            jnp.where(mask_l, l0[at].reshape(step0 * wide, LANES), 0.0),
        )
        v = dot_right(jnp.concatenate([own, other], axis=1), (w0h, w0l))
        for k in range(step0):
            o = dot_left(m0, v[k * wide:(k + 1) * wide], 3)
            y0[c * step0 + k] = o[:by, :LANES]
            y1[c * step0 + k] = o[by:, LANES:]

    pl.loop(8 // step0, (8 + bx) // step0, unroll=U0)(level0)
    arrive([xa[k] for k in tilted])
    start(za[2:6])
    arrive(za[2:6])
    level0(4 // step0)
    level0((8 + bx) // step0)

    def restrict_x(ref, at):
        return (
            ref[at] + 0.5625 * (ref[at - 1] + ref[at + 1]) - 0.0625 * (ref[at - 3] + ref[at + 3])
        )

    @pl.loop(0, cx // 2)
    def _(p):
        a = restrict_x(y1, 8 + 4 * p)
        b = restrict_x(y1, 10 + 4 * p)
        t1[p] = jnp.where(lane < cz, a, pltpu.roll(b, cz, 1))

    own_copy = pltpu.make_async_copy(t1, e1.at[pl.ds(5, cx // 2), pl.ds(16, cy), :], sg.at[3, 0])
    own_copy.start()
    own_copy.wait()
    xb = exchange(e1, (5, 16), e1, 5, 16, cx // 2, cy, sb, rb, 2)
    xb_far = exchange(e1, (5, 16), e1, 5, 16, cx // 2, cy, sb, rb, 2, True)
    zb = across(e1, e1, l1, r1, pieces(5, 16, cx // 2, cy, False, 2), szb, rzb)
    start(xb)
    start(zb[:2])
    start(xa_far)
    start(xb_far)

    arrive([xb[k] for k in flat])
    start(zb[6:10])
    arrive(zb[:2] + zb[6:10])

    half = lax.rem(lane, cz) < cz // 2

    def level1(p):
        own = e1[p]
        other = jnp.where(half & has_r, r1[p], jnp.where(jnp.logical_not(half) & has_l, l1[p], 0.0))
        even = jnp.where(lane < cz, own, pltpu.roll(other, cz, 1))
        odd = jnp.where(lane < cz, pltpu.roll(own, cz, 1), other)
        h = own.shape[0]
        v = dot_right(jnp.concatenate([even, odd], axis=0), (w1h, w1l))
        o = dot_left(m1, jnp.concatenate([v[:h], v[h:]], axis=1), 3)
        s1[2 * p] = o[:, :LANES]
        s1[2 * p + 1] = o[:, LANES:]

    pl.loop(5, 5 + cx // 2, unroll=U1)(level1)
    arrive([xb[k] for k in tilted])
    start(zb[2:6])
    arrive(zb[2:6])
    pl.loop(3, 5, unroll=True)(level1)
    pl.loop(5 + cx // 2, 7 + cx // 2, unroll=True)(level1)

    per = LANES // fz
    def restrict_1(q):
        at = 10 + 2 * q
        rows = pl.ds(ry1, fy)
        v = (
            s1[at, rows] + 0.5625 * (s1[at - 1, rows] + s1[at + 1, rows])
            - 0.0625 * (s1[at - 3, rows] + s1[at + 3, rows])
        )
        return jnp.where(lane >= rlane, v, 0.0)

    np2 = fx // per
    for p in range(np2):
        acc = None
        for k in range(per):
            v = restrict_1(p * per + k)
            sh = (fz * k + LANES - rlane) % LANES
            v = pltpu.roll(v, sh, 1) if sh else v
            acc = v if acc is None else acc + v
        p2[p] = acc
    own_copy = pltpu.make_async_copy(p2, g2.at[gz, gy, pl.ds(gx * np2, np2)], sg.at[3, 1])
    own_copy.start()
    own_copy.wait()

    def spread(dim, n, ref, k0):
        out = []
        for m, d in enumerate([d for d in range(-(n - 1), n) if d]):
            dev = tuple(here[k] + (d if k == dim else 0) for k in range(3))
            copy = pltpu.make_async_remote_copy(
                src_ref=ref(here[dim]), dst_ref=ref(here[dim]),
                send_sem=sg.at[dim, m], recv_sem=rg.at[dim, m],
                device_id=dev, device_id_type=pl.DeviceIdType.MESH,
            )
            land = pltpu.make_async_remote_copy(
                src_ref=ref(here[dim]), dst_ref=ref(here[dim] - d),
                send_sem=sg.at[dim, m], recv_sem=rg.at[dim, m],
                device_id=dev, device_id_type=pl.DeviceIdType.MESH,
            )
            to = inside(here[dim] + d, n)
            fro = inside(here[dim] - d, n)
            out.append((to, fro, copy, land))
        return out

    def begin(copies):
        for to, _, copy, _ in copies:
            pl.when(to)(copy.start)

    def landed(copies):
        for _, fro, _, land in copies:
            pl.when(fro)(land.wait_recv)

    ca = spread(0, nx, lambda k: g2.at[gz, gy, pl.ds(k * np2, np2)], 0)
    begin(ca)
    landed(ca)
    cb = spread(1, ny, lambda k: g2.at[gz, k], 0)
    begin(cb)
    arrive(xa_far)
    start(za[10:])
    arrive(xb_far)
    start(zb[10:])
    arrive(za[10:])
    level0(0)
    level0((12 + bx) // step0)
    arrive(zb[10:])
    pl.loop(0, 3, unroll=True)(level1)
    pl.loop(7 + cx // 2, 10 + cx // 2, unroll=True)(level1)

    seen = lambda r: inside(gx * cx + r - 2, nx * cx).astype(F32)

    @pl.loop(0, cx + 4)
    def _(p):
        rows = pl.ds(0, ry1)
        acc = taps[1, 0, 0] * s1[p, rows]
        for t in range(1, 17):
            acc = acc + taps[1, 0, t] * s1[p + t, rows]
        d1[p] = acc

    @pl.loop(0, bx)
    def _(p):
        acc = taps[0, 0, 0] * y0[p]
        for t in range(1, 17):
            acc = acc + taps[0, 0, t] * y0[p + t]
        out_ref[p] = acc

    landed(cb)
    cc = spread(2, nz, lambda k: g2.at[k], 0)
    begin(cc)
    landed(cc)

    tiles = u2.shape[0]

    @pl.loop(0, nx * np2)
    def _(p):
        for b in range(ny):
            for k in range(per):
                for t in range(tiles):
                    acc = jnp.zeros((fy, LANES), F32)
                    for s in range(t * per, min(nz, (t + 1) * per)):
                        v = g2[s, b, p]
                        sh = (fz * (s - t * per - k)) % LANES
                        v = pltpu.roll(v, sh, 1) if sh else v
                        lo = fz * (s - t * per)
                        acc = jnp.where((lane >= lo) & (lane < lo + fz), v, acc)
                    u2[t, p * per + k, pl.ds(b * fy, fy), :] = acc

    step2 = 2

    @pl.loop(0, n2x // step2, unroll=U2)
    def _(c):
        at = pl.ds(c * step2, step2)
        v = jnp.concatenate([u2[t, at].reshape(step2 * n2y, LANES) for t in range(tiles)], axis=1)
        v = dot_right(v, (w2h, w2l))
        v = jnp.concatenate([v[k * n2y:(k + 1) * n2y] for k in range(step2)], axis=1)
        o = dot_left(m2, v, 3)
        for k in range(step2):
            w = o[:, k * LANES:(k + 1) * LANES]
            y2[c * step2 + k] = jnp.where(
                lane < tz, w[:ty], jnp.where(lane < 2 * tz, w[ty:2 * ty], w[2 * ty:])
            )

    parts = []
    for r in range(ex):
        acc = c2[r, pl.ds(0, 1)] * y2[0]
        for q in range(1, n2x):
            acc = acc + c2[r, pl.ds(q, 1)] * y2[q]
        parts.append(acc)
    v = dot_right(jnp.concatenate(parts, axis=0), (pz2, None))
    fill = up(ty, 16) - ty
    pro = []
    for r in range(ex):
        w = v[r * ty:(r + 1) * ty]
        if fill:
            w = jnp.concatenate([w, jnp.zeros((fill, LANES), F32)], axis=0)
        pro.append(dot_left(py2, w, 2))
    for p in range(cx + 4):
        m = (p - 2) // 2 + 2
        if p % 2 == 0:
            w = pro[m]
        else:
            w = 0.5625 * (pro[m] + pro[m + 1]) - 0.0625 * (pro[m - 1] + pro[m + 2])
        d1[p] = (d1[p] + w) * seen(p)

    fill1 = up(ry1, 16) - ry1

    @pl.loop(0, (cx + 4) // 2, unroll=U3)
    def _(c):
        v = dot_right(d1[pl.ds(2 * c, 2)].reshape(2 * ry1, LANES), (pz1, None))
        v = jnp.concatenate([v[:ry1], v[ry1:]], axis=1)
        if fill1:
            v = jnp.concatenate([v, jnp.zeros((fill1, 2 * LANES), F32)], axis=0)
        o = dot_left(py1, v, 2)
        y0[2 * c] = o[:, :LANES]
        y0[2 * c + 1] = o[:, LANES:]

    @pl.loop(0, cx)
    def _(m):
        at = m + 2
        out_ref[2 * m] = out_ref[2 * m] + y0[at]
        out_ref[2 * m + 1] = out_ref[2 * m + 1] + (
            0.5625 * (y0[at] + y0[at + 1]) - 0.0625 * (y0[at - 1] + y0[at + 2])
        )

    for group in (xa, xa_far, za, xb, xb_far, zb):
        left_over(group)
    for group in (ca, cb, cc):
        for to, _, copy, _ in group:
            pl.when(to)(copy.wait_send)


def per_device(counts, charges, kernel_taps):
    nx, ny, nz = counts
    bx, by, bz = dims = charges.shape
    assert bz == LANES
    cx, cy, cz = bx // 2, by // 2, bz // 2
    fx, fy, fz = bx // 4, by // 4, bz // 4
    n2x, n2y, n2z = nx * fx, ny * fy, nz * fz
    np2 = fx // (LANES // fz)
    ry1 = up(cy + 4, 8)
    ty = up(fy + 5, 8)
    tiles = up(n2z, LANES) // LANES
    V = pltpu.VMEM
    ext0 = (bx + 16, by + 16, LANES)
    ext1 = (cx // 2 + 10, cy + 32, LANES)
    wide = max(nx, ny, nz) * 2
    dma = pltpu.SemaphoreType.DMA
    scratch = [
        V(ext0, F32), V(ext0, F32), V(ext0, F32),
        V((bx + 16, by, LANES), F32), V((bx + 16, cy, LANES), F32),
        V(ext1, F32), V(ext1, F32), V(ext1, F32),
        V((cx // 2, cy, LANES), F32),
        V((cx + 20, ry1 + fy, LANES), F32),
        V((nz, ny, nx * np2, fy, LANES), F32),
        V((tiles, n2x, n2y, LANES), F32),
        V((n2x, ty, LANES), F32), V((np2, fy, LANES), F32), V((cx + 4, ry1, LANES), F32),
        V((2 * bz, bz + LANES), BF16), V((2 * bz, bz + LANES), BF16),
        V((by + cy, 3 * (by + 16)), BF16),
        V((2 * cz, LANES), BF16), V((2 * cz, LANES), BF16),
        V((ry1 + fy, 3 * (cy + 32)), BF16),
        V((tiles * LANES, LANES), BF16), V((tiles * LANES, LANES), BF16),
        V((3 * ty, 3 * n2y), BF16),
        V((fx + 5, n2x, LANES), F32),
        V((LANES, LANES), BF16), V((ry1, 2 * up(ty, 16)), BF16),
        V((LANES, bz), BF16), V((by, 2 * up(ry1, 16)), BF16),
        dma((16,)), dma((16,)), dma((7, 2)), dma((7, 2)),
        dma((16,)), dma((16,)), dma((7, 2)), dma((7, 2)),
        dma((4, wide)), dma((3, wide)),
    ]
    return pl.pallas_call(
        functools.partial(kernel, counts, dims),
        out_shape=jax.ShapeDtypeStruct(dims, F32),
        in_specs=[pl.BlockSpec(memory_space=pltpu.SMEM), pl.BlockSpec(memory_space=pltpu.VMEM)],
        out_specs=pl.BlockSpec(memory_space=pltpu.VMEM),
        scratch_shapes=scratch,
        compiler_params=pltpu.CompilerParams(
            collective_id=0, has_side_effects=True, vmem_limit_bytes=60 * 2**20
        ),
    )(kernel_taps, charges)


def solution(mesh):
    counts = tuple(mesh.shape[a] for a in AXES)
    return jax.shard_map(
        functools.partial(per_device, counts), mesh=mesh,
        in_specs=(P("gx", "gy", "gz"), P()), out_specs=P("gx", "gy", "gz"), check_vma=False,
    )
```

```python
import functools

import jax
import jax.numpy as jnp
from jax import lax
from jax.experimental import pallas as pl
from jax.experimental.pallas import tpu as pltpu
from jax.sharding import PartitionSpec as P

F32, BF16 = jnp.float32, jnp.bfloat16
LANES = 128
U0, U1, U2, U3 = 4, 4, 4, 5
AXES = ("gx", "gy", "gz")
ODD = (-0.0625, 0.5625, 0.5625, -0.0625)
SIDES = tuple((a, b) for a in (-1, 0, 1) for b in (-1, 0, 1) if (a, b) != (0, 0))


def split(v):
    hi = v.astype(BF16)
    return hi, (v - hi.astype(F32)).astype(BF16)


def mm(a, b):
    return jnp.dot(a, b, preferred_element_type=F32)


def exact(a, b):
    return jnp.dot(a, b, preferred_element_type=F32, precision=lax.Precision.HIGHEST)


def dot_right(v, w):
    hi, lo = split(v)
    out = mm(hi, w[0][...]) + mm(lo, w[0][...])
    return out if w[1] is None else out + mm(hi, w[1][...])


def dot_left(w_ref, v, terms):
    hi, lo = split(v)
    return mm(w_ref[...], jnp.concatenate([hi, lo, hi][:terms], axis=0))


def grids(rows, cols):
    return (
        lax.broadcasted_iota(jnp.int32, (rows, cols), 0),
        lax.broadcasted_iota(jnp.int32, (rows, cols), 1),
    )


def pick(taps, level, axis, diff, ok):
    out = jnp.zeros(diff.shape, F32)
    for t in range(17):
        out = jnp.where(diff == t, taps[level, axis, t], out)
    return jnp.where(ok, out, 0.0)


def cubic(diff, ok):
    d = jnp.abs(diff)
    out = jnp.where(d == 0, 1.0, jnp.where(d == 1, 0.5625, jnp.where(d == 3, -0.0625, 0.0)))
    return jnp.where(ok, out, 0.0).astype(F32)


def up(n, m):
    return -(-n // m) * m


def inside(v, n):
    return (v >= 0) & (v < n)


def kernel(counts, dims, taps, x_ref, out_ref, e0, l0, r0, y0, y1, t1, t1l, t1r, e1, sw, f1, h1, h1l, h1r, d1, pr,
           ua, am, v2, v2l, v2r, pq, yu, yd, xg, g2, u2, y2,
           w0h, w0l, m0, w1h, w1l, m1, w2h, w2l, m2, c2, pz2, py2, py1, my2, wz2, ss, rs, sg, rg):
    nx, ny, nz = counts
    bx, by, bz = dims
    here = tuple(lax.axis_index(a) for a in AXES)
    gx, gy, gz = here
    cx, cy, cz = bx // 2, by // 2, bz // 2
    fx, fy, fz = bx // 4, by // 4, bz // 4
    half1 = cx // 2
    per = LANES // fz
    np2 = fx // per

    def there(dx, dy, dz):
        return inside(gx + dx, nx) & inside(gy + dy, ny) & inside(gz + dz, nz)

    partners = []
    for dim, n in enumerate(counts):
        for d in range(1, n):
            for sgn in (-d, d):
                partners.append(tuple(sgn if k == dim else 0 for k in range(3)))
    barrier = pltpu.get_barrier_semaphore()
    total = jnp.int32(0)
    for p in partners:
        ok = there(*p)
        total = total + ok.astype(jnp.int32)

        @pl.when(ok)
        def _(p=p):
            pl.semaphore_signal(
                barrier, inc=1, device_id=(gx + p[0], gy + p[1], gz + p[2]),
                device_id_type=pl.DeviceIdType.MESH,
            )

    def clear(ref, d, *at):
        @pl.when(jnp.logical_not(there(*d)))
        def _():
            view = ref.at[at]
            view[...] = jnp.zeros(view.shape, F32)

    every = slice(None)
    clear(e0, (0, -1, 0), every, pl.ds(0, 8))
    clear(e0, (0, 1, 0), every, pl.ds(8 + by, 8))
    clear(y0, (-1, 0, 0), pl.ds(0, 8))
    clear(y0, (1, 0, 0), pl.ds(8 + bx, 8))
    clear(t1l, (-1, 0, 0), every)
    clear(t1r, (1, 0, 0), every)
    clear(f1, (0, -1, 0), every, pl.ds(0, 16))
    clear(f1, (0, 1, 0), every, pl.ds(16 + cy, 16))
    clear(yu, (0, -1, 0), every)
    clear(yd, (0, 1, 0), every)
    for ref in (ua, y1):
        ref[pl.ds(0, 8)] = jnp.zeros((8,) + ref.shape[1:], F32)
        ref[pl.ds(8 + bx, 8)] = jnp.zeros((8,) + ref.shape[1:], F32)
    am[pl.ds(0, 6)] = jnp.zeros((6,) + am.shape[1:], F32)
    am[pl.ds(cx + 9, 6)] = jnp.zeros((6,) + am.shape[1:], F32)
    pl.semaphore_wait(barrier, total)

    count = [0]

    def remote(src, dst, d):
        k = count[0]
        count[0] += 1
        copy = pltpu.make_async_remote_copy(
            src_ref=src, dst_ref=dst, send_sem=ss.at[k], recv_sem=rs.at[k],
            device_id=(gx + d[0], gy + d[1], gz + d[2]), device_id_type=pl.DeviceIdType.MESH,
        )
        return there(*d), there(-d[0], -d[1], -d[2]), copy

    def start(copies):
        for to, _, copy in copies:
            pl.when(to)(copy.start)

    def arrive(copies):
        for _, fro, copy in copies:
            pl.when(fro)(copy.wait_recv)

    def left_over(copies):
        for to, _, copy in copies:
            pl.when(to)(copy.wait_send)

    right, left, ahead, behind, above, below = (
        (1, 0, 0), (-1, 0, 0), (0, 1, 0), (0, -1, 0), (0, 0, 1), (0, 0, -1)
    )
    own_y = pl.ds(8, by)
    ya = [
        remote(x_ref.at[:, pl.ds(by - 8, 8)], e0.at[:, pl.ds(0, 8)], ahead),
        remote(x_ref.at[:, pl.ds(0, 8)], e0.at[:, pl.ds(8 + by, 8)], behind),
    ]
    za = [remote(x_ref, l0.at[:, own_y], above), remote(x_ref, r0.at[:, own_y], below)]
    zf = [
        remote(e0.at[:, pl.ds(k, 8)], ref.at[:, pl.ds(k, 8)], d)
        for k in (0, 8 + by) for ref, d in ((l0, above), (r0, below))
    ]
    z2 = [remote(v2, v2l, above), remote(v2, v2r, below)]
    yp = [
        remote(pq.at[:, pl.ds(fy, 8)], yu, ahead),
        remote(pq.at[:, pl.ds(fy + 8, 8)], yd, behind),
    ]
    xa = [
        [
            remote(y0.at[pl.ds(bx + k, 2)], y0.at[pl.ds(k, 2)], right),
            remote(y0.at[pl.ds(8 + k, 2)], y0.at[pl.ds(8 + bx + k, 2)], left),
        ]
        for k in range(0, 8, 2)
    ]
    xb = [remote(t1.at[pl.ds(half1 - 4, 6)], t1l, right), remote(t1.at[pl.ds(0, 6)], t1r, left)]
    yb = [
        remote(f1.at[:, pl.ds(cy, 16)], f1.at[:, pl.ds(0, 16)], ahead),
        remote(f1.at[:, pl.ds(16, 16)], f1.at[:, pl.ds(16 + cy, 16)], behind),
    ]
    zb = [remote(h1, h1l, above), remote(h1, h1r, below)]
    start(ya)
    start(za)

    def put(h, l, v):
        hi, lo = split(v)
        h[...] = hi
        if l is not None:
            l[...] = lo

    def stack(ref, v, terms):
        hi, lo = split(v)
        ref[...] = jnp.concatenate([hi, hi, lo][:terms], axis=1)

    def twice(pos, at, base, n):
        out = jnp.zeros(pos.shape, F32)
        for k, w in ((-3, -0.0625), (-1, 0.5625), (0, 1.0), (1, 0.5625), (3, -0.0625)):
            m = 2 * at + k
            out = out + w * cubic(pos - 2 * m, inside(base + m, n))
        return out

    def restrict_x(ref, at):
        return (
            ref[at] + 0.5625 * (ref[at - 1] + ref[at + 1]) - 0.0625 * (ref[at - 3] + ref[at + 3])
        )

    lane = lax.broadcasted_iota(jnp.int32, (1, LANES), 1)
    has_r, has_l = there(*above), there(*below)
    mask_r, mask_l = (lane < LANES // 2) & has_r, (lane >= LANES // 2) & has_l
    rows2 = fy + 16
    i, j = grids(rows2, by)
    stack(my2, twice(j, jnp.where(i < fy + 8, i, i - rows2), gy * cy, ny * cy), 2)
    i, j = grids(2 * bz, LANES)
    pos = jnp.where(i < bz + bz // 2, i, i - 2 * bz)
    put(wz2, None, jnp.where(j < fz, twice(pos, j, gz * cz, nz * cz), 0.0))

    @pl.loop(0, bx // 2, unroll=4)
    def _(c):
        o = dot_left(my2, jnp.concatenate([x_ref[2 * c], x_ref[2 * c + 1]], axis=1), 2)
        ua[8 + 2 * c] = o[:, :LANES]
        ua[9 + 2 * c] = o[:, LANES:]

    for m in range(-1, cx + 2):
        am[m + 7] = restrict_x(ua, 8 + 2 * m) * inside(gx * cx + m, nx * cx).astype(F32)
    for e in range(fx + 5):
        v2[e] = restrict_x(am, 3 + 2 * e)
    start(z2)

    e0[:, own_y, :] = x_ref[...]
    i, j = grids(2 * bz, bz)
    pos = jnp.where(i < bz + bz // 2, i, i - 2 * bz)
    k0 = pick(taps, 0, 2, pos - j + 8, inside(pos, bz + 8) | inside(pos + 8, 8))
    rz = cubic(pos - 2 * j, j < cz)
    put(w0h, w0l, jnp.concatenate([k0, rz], axis=1))
    i, j = grids(by + cy, by + 16)
    stack(m0, jnp.where(i < by, pick(taps, 0, 1, j - i, i < by), cubic(j - 8 - 2 * (i - by), i >= by)), 3)

    arrive(z2)
    parts = []
    for e in range(fx + 5):
        other = jnp.where(mask_r, v2r[e], jnp.where(mask_l, v2l[e], 0.0))
        parts.append(jnp.concatenate([v2[e], other], axis=1))
    v = dot_right(jnp.concatenate(parts, axis=0), (wz2, None))
    for g in range(np2 + 2):
        acc = None
        for s in range(per):
            e = per * (g - 1) + s + 2
            if 0 <= e < fx + 5:
                w = v[e * rows2:(e + 1) * rows2]
                w = pltpu.roll(w, fz * s, 1) if s else w
                acc = w if acc is None else acc + w
        pq[g] = acc
    start(yp)

    i, j = grids(2 * cz, LANES)
    pos = jnp.where(i < cz + cz // 2, i, i - 2 * cz)
    kk = j - 2
    top = cz + 4
    ok = (j < top) & inside(gz * cz + kk, nz * cz)
    k1 = pick(taps, 1, 2, pos - kk + 8, ok)
    i, j = grids(LANES, bz)
    fine_z = cubic(j - 2 * (i - 2), i < top)
    put(w1h, w1l, exact(k1, fine_z))
    ry1 = up(cy + 4, 8)
    i, j = grids(ry1, cy + 32)
    ok = (i < cy + 4) & inside(gy * cy + i - 2, ny * cy)
    stack(m1, pick(taps, 1, 1, j - 16 - (i - 2) + 8, ok), 3)
    i, j = grids(by, up(ry1, 16))
    stack(py1, cubic(i - 2 * (j - 2), j < cy + 4), 2)

    def plain(axis, level, n, pad, turned):
        i, j = grids(pad, pad)
        d = (i - j if turned else j - i) + 8
        return pick(taps, level, axis, d, (i < n) & (j < n))

    def rest(n, pad, big, turned_r):
        i, j = grids(*((big, pad) if turned_r else (pad, big)))
        c, f = (j, i) if turned_r else (i, j)
        return cubic(f - 2 * c, (c < n) & (f < 2 * n))

    def operators(axis, n2, first, rows, count):
        n3, n4 = n2 // 2, n2 // 4
        q = up(n2, LANES)
        i, j = grids(rows, q)
        g = first + i
        ok = (i < count) & inside(g, n2)
        one = pick(taps, 2, axis, j - g + 8, ok & (j < n2))
        pr = cubic(g - 2 * j, ok & (j < n3))
        r23, r34 = rest(n3, q, q, False), rest(n4, q, q, False)
        p34 = rest(n4, q, q, True)
        two = exact(exact(pr, plain(axis, 3, n3, q, False)), r23)
        three = exact(exact(exact(exact(pr, p34), plain(axis, 4, n4, q, False)), r34), r23)
        return one, two, three

    n2x, n2y, n2z = nx * fx, ny * fy, nz * fz
    ez, ey, ex = fz + 5, fy + 5, fx + 5
    tz = 40
    ops = operators(2, n2z, gz * fz - 2, tz, ez)
    cols = jnp.concatenate(list(ops) + [jnp.zeros((LANES - 3 * tz, ops[0].shape[1]), F32)], axis=0)
    put(w2h, w2l, cols.T)
    ty = up(ey, 8)
    ops = operators(1, n2y, gy * fy - 2, ty, ey)
    stack(m2, jnp.concatenate(list(ops), axis=0)[:, :n2y], 3)
    tx = up(ex, 8)
    ops = operators(0, n2x, gx * fx - 2, tx, ex)
    tall = [o.T for o in ops]
    for r in range(ex):
        a, b, c = (o[:n2x, r:r + 1] for o in tall)
        c2[r] = jnp.where(lane < tz, a, jnp.where(lane < 2 * tz, b, c))
    i, j = grids(LANES, LANES)
    src = i - jnp.where(i < tz, 0, jnp.where(i < 2 * tz, tz, 2 * tz)) - 2
    e1_z = cubic((j - 2) - 2 * src, (i < 3 * tz) & (src < fz + 3) & (j < top) & inside(gz * cz + j - 2, nz * cz))
    put(pz2, None, exact(e1_z, fine_z))
    i, j = grids(ry1, up(ty, 16))
    stack(py2, cubic((i - 2) - 2 * (j - 2), (j < ey) & (i < cy + 4) & inside(gy * cy + i - 2, ny * cy)), 2)
    arrive(ya)
    start(zf)
    arrive(za)
    arrive(yp)
    own = [pq[:, pl.ds(0, 8)] + yu[...]]
    if fy > 16:
        own.append(pq[:, pl.ds(8, fy - 16)])
    own.append(pq[:, pl.ds(fy - 8, 8)] + yd[...])
    xg[gx] = jnp.concatenate(own, axis=1)
    def spread(dim, n, ref, k0):
        out = []
        for m, d in enumerate([d for d in range(-(n - 1), n) if d]):
            dev = tuple(here[k] + (d if k == dim else 0) for k in range(3))
            copy = pltpu.make_async_remote_copy(
                src_ref=ref(here[dim]), dst_ref=ref(here[dim]),
                send_sem=sg.at[dim, m], recv_sem=rg.at[dim, m],
                device_id=dev, device_id_type=pl.DeviceIdType.MESH,
            )
            land = pltpu.make_async_remote_copy(
                src_ref=ref(here[dim]), dst_ref=ref(here[dim] - d),
                send_sem=sg.at[dim, m], recv_sem=rg.at[dim, m],
                device_id=dev, device_id_type=pl.DeviceIdType.MESH,
            )
            to = inside(here[dim] + d, n)
            fro = inside(here[dim] - d, n)
            out.append((to, fro, copy, land))
        return out

    def begin(copies):
        for to, _, copy, _ in copies:
            pl.when(to)(copy.start)

    def landed(copies):
        for _, fro, _, land in copies:
            pl.when(fro)(land.wait_recv)

    ca = spread(0, nx, lambda k: xg.at[k], 0)
    begin(ca)
    arrive(zf)

    wide = by + 16
    step0 = 4

    def level0(c):
        at = pl.ds(c * step0, step0)
        own = e0[at].reshape(step0 * wide, LANES)
        other = jnp.where(
            mask_r, r0[at].reshape(step0 * wide, LANES),
            jnp.where(mask_l, l0[at].reshape(step0 * wide, LANES), 0.0),
        )
        v = dot_right(jnp.concatenate([own, other], axis=1), (w0h, w0l))
        for k in range(step0):
            o = dot_left(m0, v[k * wide:(k + 1) * wide], 3)
            y0[8 + c * step0 + k] = o[:by, :LANES]
            y1[8 + c * step0 + k] = o[by:, LANES:]

    edge = 8 // step0
    for c in range(edge):
        level0(c)
        level0(bx // step0 - edge + c)
    start(xa[0])
    pl.loop(edge, bx // step0 - edge, unroll=True)(level0)

    landed(ca)
    for m in range(np2 * nx):
        acc = None
        for b in range(nx):
            k = m - np2 * b + 1
            if 0 <= k < np2 + 2:
                acc = xg[b, k] if acc is None else acc + xg[b, k]
        g2[gz, gy, m] = acc
    cb = spread(1, ny, lambda k: g2.at[gz, k], 0)
    begin(cb)

    for p in range(half1 + 2):
        a = restrict_x(y1, 4 + 4 * p)
        b = restrict_x(y1, 6 + 4 * p)
        t1[p] = jnp.where(lane < cz, a, pltpu.roll(b, cz, 1))
    start(xb)
    for k in range(1, 4):
        start(xa[k])

    def conv0(p):
        acc = taps[0, 0, 0] * y0[p]
        for t in range(1, 17):
            acc = acc + taps[0, 0, t] * y0[p + t]
        out_ref[p] = acc

    pl.loop(8, bx - 8)(conv0)

    arrive(xb)
    n1 = half1 + 10
    to_l, to_r = there(*left).astype(F32), there(*right).astype(F32)
    for k in range(n1):
        if k < 4:
            v = t1l[k]
        elif k < 6:
            v = t1l[k] + (t1[k - 4] * to_l if k == 4 else t1[k - 4])
        elif k < half1 + 4:
            v = t1[k - 4]
        elif k < half1 + 6:
            v = t1r[k - half1 - 4] + (t1[k - 4] * to_r if k == half1 + 5 else t1[k - 4])
        else:
            v = t1r[k - half1 - 4]
        e1[k] = v
        back = pltpu.roll(v, cz, 1)
        if k:
            sw[k - 1] = jnp.where(lane < cz, last, back)
        last = back

    @pl.loop(0, half1 + 2)
    def _(q):
        acc = taps[1, 0, 0] * e1[q]
        for t in range(1, 17):
            acc = acc + taps[1, 0, t] * (sw[q + (t - 1) // 2] if t % 2 else e1[q + t // 2])
        f1[q, pl.ds(16, cy), :] = acc

    start(yb)
    landed(cb)
    cc = spread(2, nz, lambda k: g2.at[k], 0)
    begin(cc)
    arrive(yb)
    for q in range(0, half1 + 2, 2):
        o = dot_left(m1, jnp.concatenate([f1[q], f1[q + 1]], axis=1), 3)
        h1[q] = o[:, :LANES]
        h1[q + 1] = o[:, LANES:]
    start(zb)
    landed(cc)
    seen = lambda r: inside(gx * cx + r - 2, nx * cx).astype(F32)
    tiles = u2.shape[0]

    @pl.loop(0, nx * np2)
    def _(p):
        for b in range(ny):
            for k in range(per):
                for t in range(tiles):
                    acc = jnp.zeros((fy, LANES), F32)
                    for s in range(t * per, min(nz, (t + 1) * per)):
                        v = g2[s, b, p]
                        sh = (fz * (s - t * per - k)) % LANES
                        v = pltpu.roll(v, sh, 1) if sh else v
                        lo = fz * (s - t * per)
                        acc = jnp.where((lane >= lo) & (lane < lo + fz), v, acc)
                    u2[t, p * per + k, pl.ds(b * fy, fy), :] = acc

    step2 = 2

    @pl.loop(0, n2x // step2, unroll=U2)
    def _(c):
        at = pl.ds(c * step2, step2)
        v = jnp.concatenate([u2[t, at].reshape(step2 * n2y, LANES) for t in range(tiles)], axis=1)
        v = dot_right(v, (w2h, w2l))
        v = jnp.concatenate([v[k * n2y:(k + 1) * n2y] for k in range(step2)], axis=1)
        o = dot_left(m2, v, 3)
        for k in range(step2):
            w = o[:, k * LANES:(k + 1) * LANES]
            y2[c * step2 + k] = jnp.where(
                lane < tz, w[:ty], jnp.where(lane < 2 * tz, w[ty:2 * ty], w[2 * ty:])
            )

    parts = []
    for r in range(ex):
        acc = c2[r, pl.ds(0, 1)] * y2[0]
        for q in range(1, n2x):
            acc = acc + c2[r, pl.ds(q, 1)] * y2[q]
        parts.append(acc)
    v = dot_right(jnp.concatenate(parts, axis=0), (pz2, None))
    fill = up(ty, 16) - ty
    pro = []
    for r in range(ex):
        w = v[r * ty:(r + 1) * ty]
        if fill:
            w = jnp.concatenate([w, jnp.zeros((fill, LANES), F32)], axis=0)
        pro.append(dot_left(py2, w, 2))
    arrive(zb)
    near = lax.rem(lane, cz) < cz // 2
    step1 = 5 if (half1 + 2) % 5 == 0 else 1
    for c in range(0, half1 + 2, step1):
        parts = []
        for q in range(c, c + step1):
            own = h1[q]
            other = jnp.where(near & has_r, h1r[q], jnp.where(jnp.logical_not(near) & has_l, h1l[q], 0.0))
            parts.append(jnp.where(lane < cz, own, pltpu.roll(other, cz, 1)))
            parts.append(jnp.where(lane < cz, pltpu.roll(own, cz, 1), other))
        v = dot_right(jnp.concatenate(parts, axis=0), (w1h, w1l))
        for k in range(2 * step1):
            d1[2 * c + k] = v[k * ry1:(k + 1) * ry1]
    for p in range(cx + 4):
        m = (p - 2) // 2 + 2
        if p % 2 == 0:
            w = pro[m]
        else:
            w = 0.5625 * (pro[m] + pro[m + 1]) - 0.0625 * (pro[m - 1] + pro[m + 2])
        d1[p] = (d1[p] + w) * seen(p)

    fill1 = up(ry1, 16) - ry1

    @pl.loop(0, (cx + 4) // 2, unroll=5)
    def _(c):
        v = jnp.concatenate([d1[2 * c], d1[2 * c + 1]], axis=1)
        if fill1:
            v = jnp.concatenate([v, jnp.zeros((fill1, 2 * LANES), F32)], axis=0)
        o = dot_left(py1, v, 2)
        pr[2 * c] = o[:, :LANES]
        pr[2 * c + 1] = o[:, LANES:]

    for group in xa:
        arrive(group)
    pl.loop(0, 8)(conv0)
    pl.loop(bx - 8, bx)(conv0)

    @pl.loop(0, cx)
    def _(m):
        at = m + 2
        out_ref[2 * m] = out_ref[2 * m] + pr[at]
        out_ref[2 * m + 1] = out_ref[2 * m + 1] + (
            0.5625 * (pr[at] + pr[at + 1]) - 0.0625 * (pr[at - 1] + pr[at + 2])
        )

    for group in (ya, za, zf, z2, yp, *xa, xb, yb, zb):
        left_over(group)
    for group in (ca, cb, cc):
        for to, _, copy, _ in group:
            pl.when(to)(copy.wait_send)


def per_device(counts, charges, kernel_taps):
    nx, ny, nz = counts
    bx, by, bz = dims = charges.shape
    assert bz == LANES
    cx, cy, cz = bx // 2, by // 2, bz // 2
    fx, fy, fz = bx // 4, by // 4, bz // 4
    n2x, n2y, n2z = nx * fx, ny * fy, nz * fz
    np2 = fx // (LANES // fz)
    half1 = cx // 2
    ry1 = up(cy + 4, 8)
    ty = up(fy + 5, 8)
    tiles = up(n2z, LANES) // LANES
    V = pltpu.VMEM
    ext0 = (bx, by + 16, LANES)
    wide = max(nx, ny, nz) * 2
    dma = pltpu.SemaphoreType.DMA
    row = lambda n, r: V((n, r, LANES), F32)
    scratch = [
        V(ext0, F32), V(ext0, F32), V(ext0, F32),
        row(bx + 16, by), row(bx + 16, cy),
        row(half1 + 2, cy), row(6, cy), row(6, cy), row(half1 + 10, cy), row(half1 + 9, cy),
        row(half1 + 2, cy + 32), row(half1 + 2, ry1), row(half1 + 2, ry1), row(half1 + 2, ry1),
        row(cx + 4, ry1), row(cx + 4, by),
        row(bx + 16, fy + 16), row(cx + 15, fy + 16),
        row(fx + 5, fy + 16), row(fx + 5, fy + 16), row(fx + 5, fy + 16),
        row(np2 + 2, fy + 16), row(np2 + 2, 8), row(np2 + 2, 8),
        V((nx, np2 + 2, fy, LANES), F32),
        V((nz, ny, nx * np2, fy, LANES), F32),
        V((tiles, n2x, n2y, LANES), F32),
        row(n2x, ty),
        V((2 * bz, bz + LANES), BF16), V((2 * bz, bz + LANES), BF16),
        V((by + cy, 3 * (by + 16)), BF16),
        V((2 * cz, bz), BF16), V((2 * cz, bz), BF16),
        V((ry1, 3 * (cy + 32)), BF16),
        V((tiles * LANES, LANES), BF16), V((tiles * LANES, LANES), BF16),
        V((3 * ty, 3 * n2y), BF16),
        row(fx + 5, n2x),
        V((LANES, bz), BF16), V((ry1, 2 * up(ty, 16)), BF16),
        V((by, 2 * up(ry1, 16)), BF16),
        V((fy + 16, 2 * by), BF16), V((2 * bz, LANES), BF16),
        dma((32,)), dma((32,)), dma((3, wide)), dma((3, wide)),
    ]
    return pl.pallas_call(
        functools.partial(kernel, counts, dims),
        out_shape=jax.ShapeDtypeStruct(dims, F32),
        in_specs=[pl.BlockSpec(memory_space=pltpu.SMEM), pl.BlockSpec(memory_space=pltpu.VMEM)],
        out_specs=pl.BlockSpec(memory_space=pltpu.VMEM),
        scratch_shapes=scratch,
        compiler_params=pltpu.CompilerParams(
            collective_id=0, has_side_effects=True, vmem_limit_bytes=28 * 2**20
        ),
    )(kernel_taps, charges)


def solution(mesh):
    counts = tuple(mesh.shape[a] for a in AXES)
    return jax.shard_map(
        functools.partial(per_device, counts), mesh=mesh,
        in_specs=(P("gx", "gy", "gz"), P()), out_specs=P("gx", "gy", "gz"), check_vma=False,
    )
```

```python
import functools

import jax
import jax.numpy as jnp
from jax import lax
from jax.experimental import pallas as pl
from jax.experimental.pallas import tpu as pltpu
from jax.sharding import PartitionSpec as P

F32, BF16 = jnp.float32, jnp.bfloat16
LANES = 128
U0, U1, U2, U3 = 4, 4, 4, 5
AXES = ("gx", "gy", "gz")
ODD = (-0.0625, 0.5625, 0.5625, -0.0625)
SIDES = tuple((a, b) for a in (-1, 0, 1) for b in (-1, 0, 1) if (a, b) != (0, 0))


def split(v):
    hi = v.astype(BF16)
    return hi, (v - hi.astype(F32)).astype(BF16)


def mm(a, b):
    return jnp.dot(a, b, preferred_element_type=F32)


def exact(a, b):
    return jnp.dot(a, b, preferred_element_type=F32, precision=lax.Precision.HIGHEST)


def dot_right(v, w):
    hi, lo = split(v)
    out = mm(hi, w[0][...]) + mm(lo, w[0][...])
    return out if w[1] is None else out + mm(hi, w[1][...])


def dot_left(w_ref, v, terms):
    hi, lo = split(v)
    return mm(w_ref[...], jnp.concatenate([hi, lo, hi][:terms], axis=0))


def grids(rows, cols):
    return (
        lax.broadcasted_iota(jnp.int32, (rows, cols), 0),
        lax.broadcasted_iota(jnp.int32, (rows, cols), 1),
    )


def pick(taps, level, axis, diff, ok):
    out = jnp.zeros(diff.shape, F32)
    for t in range(17):
        out = jnp.where(diff == t, taps[level, axis, t], out)
    return jnp.where(ok, out, 0.0)


def cubic(diff, ok):
    d = jnp.abs(diff)
    out = jnp.where(d == 0, 1.0, jnp.where(d == 1, 0.5625, jnp.where(d == 3, -0.0625, 0.0)))
    return jnp.where(ok, out, 0.0).astype(F32)


def up(n, m):
    return -(-n // m) * m


def inside(v, n):
    return (v >= 0) & (v < n)


def kernel(counts, dims, taps_hbm, x_hbm, out_ref, taps, x_ref, l0, r0, hy, hl, hr, zh, zl, y0, y1, t1, t1l, t1r, e1, sw, f1, h1, h1l, h1r, d1, pr,
           ua, am, v2, v2l, v2r, pq, yu, yd, xg, g2, z2h, z2l, y2,
           w0h, w0l, m0, w1h, w1l, m1, w2h, w2l, m2, c2, pz2, py2, py1, my2, wz2, own_sem, ss, rs, sg, rg):
    nx, ny, nz = counts
    bx, by, bz = dims
    here = tuple(lax.axis_index(a) for a in AXES)
    loads = [
        pltpu.make_async_copy(x_hbm, x_ref, own_sem.at[0]),
        pltpu.make_async_copy(taps_hbm, taps, own_sem.at[1]),
    ]
    for load in loads:
        load.start()
    gx, gy, gz = here
    cx, cy, cz = bx // 2, by // 2, bz // 2
    fx, fy, fz = bx // 4, by // 4, bz // 4
    half1 = cx // 2
    per = LANES // fz
    np2 = fx // per

    def there(dx, dy, dz):
        return inside(gx + dx, nx) & inside(gy + dy, ny) & inside(gz + dz, nz)

    partners = []
    for dim, n in enumerate(counts):
        for d in range(1, n):
            for sgn in (-d, d):
                partners.append(tuple(sgn if k == dim else 0 for k in range(3)))
    barrier = pltpu.get_barrier_semaphore()
    total = jnp.int32(0)
    for p in partners:
        ok = there(*p)
        total = total + ok.astype(jnp.int32)

        @pl.when(ok)
        def _(p=p):
            pl.semaphore_signal(
                barrier, inc=1, device_id=(gx + p[0], gy + p[1], gz + p[2]),
                device_id_type=pl.DeviceIdType.MESH,
            )

    def clear(ref, d, *at):
        @pl.when(jnp.logical_not(there(*d)))
        def _():
            view = ref.at[at]
            view[...] = jnp.zeros(view.shape, F32)

    every = slice(None)
    clear(hy, (0, -1, 0), every, pl.ds(0, 8))
    clear(hy, (0, 1, 0), every, pl.ds(8, 8))
    clear(y0, (-1, 0, 0), pl.ds(0, 8))
    clear(y0, (1, 0, 0), pl.ds(8 + bx, 8))
    clear(t1l, (-1, 0, 0), every)
    clear(t1r, (1, 0, 0), every)
    clear(f1, (0, -1, 0), every, pl.ds(0, 16))
    clear(f1, (0, 1, 0), every, pl.ds(16 + cy, 16))
    clear(yu, (0, -1, 0), every)
    clear(yd, (0, 1, 0), every)
    for ref in (ua, y1):
        ref[pl.ds(0, 8)] = jnp.zeros((8,) + ref.shape[1:], F32)
        ref[pl.ds(8 + bx, 8)] = jnp.zeros((8,) + ref.shape[1:], F32)
    am[pl.ds(0, 6)] = jnp.zeros((6,) + am.shape[1:], F32)
    am[pl.ds(cx + 9, 6)] = jnp.zeros((6,) + am.shape[1:], F32)
    for load in loads:
        load.wait()
    pl.semaphore_wait(barrier, total)

    count = [0]

    def remote(src, dst, d):
        k = count[0]
        count[0] += 1
        copy = pltpu.make_async_remote_copy(
            src_ref=src, dst_ref=dst, send_sem=ss.at[k], recv_sem=rs.at[k],
            device_id=(gx + d[0], gy + d[1], gz + d[2]), device_id_type=pl.DeviceIdType.MESH,
        )
        return there(*d), there(-d[0], -d[1], -d[2]), copy

    def start(copies):
        for to, _, copy in copies:
            pl.when(to)(copy.start)

    def arrive(copies):
        for _, fro, copy in copies:
            pl.when(fro)(copy.wait_recv)

    def left_over(copies):
        for to, _, copy in copies:
            pl.when(to)(copy.wait_send)

    right, left, ahead, behind, above, below = (
        (1, 0, 0), (-1, 0, 0), (0, 1, 0), (0, -1, 0), (0, 0, 1), (0, 0, -1)
    )
    ends = (pl.ds(0, 8), pl.ds(bx - 8, 8)), (pl.ds(8, bx - 16),)
    ya, zf = [], []
    for xs in ends:
        ya.append([
            remote(x_ref.at[x, pl.ds(by - 8, 8)], hy.at[x, pl.ds(0, 8)], ahead) for x in xs
        ] + [
            remote(x_ref.at[x, pl.ds(0, 8)], hy.at[x, pl.ds(8, 8)], behind) for x in xs
        ])
        zf.append([remote(hy.at[x], hl.at[x], above) for x in xs] + [remote(hy.at[x], hr.at[x], below) for x in xs])
    za = [remote(x_ref, l0, above), remote(x_ref, r0, below)]
    z2 = [remote(v2, v2l, above), remote(v2, v2r, below)]
    yp = [
        remote(pq.at[:, pl.ds(fy, 8)], yu, ahead),
        remote(pq.at[:, pl.ds(fy + 8, 8)], yd, behind),
    ]
    xa = [
        [
            remote(y0.at[pl.ds(bx + k, n)], y0.at[pl.ds(k, n)], right),
            remote(y0.at[pl.ds(8 + k, n)], y0.at[pl.ds(8 + bx + k, n)], left),
        ]
        for k, n in ((0, 2), (2, 6))
    ]
    xb = [remote(t1.at[pl.ds(half1 - 4, 6)], t1l, right), remote(t1.at[pl.ds(0, 6)], t1r, left)]
    yb = [
        remote(f1.at[:, pl.ds(cy, 16)], f1.at[:, pl.ds(0, 16)], ahead),
        remote(f1.at[:, pl.ds(16, 16)], f1.at[:, pl.ds(16 + cy, 16)], behind),
    ]
    zb = [remote(h1, h1l, above), remote(h1, h1r, below)]
    start(ya[0])
    start(za)
    start(ya[1])

    def put(h, l, v):
        hi, lo = split(v)
        h[...] = hi
        if l is not None:
            l[...] = lo

    def stack(ref, v, terms):
        hi, lo = split(v)
        ref[...] = jnp.concatenate([hi, hi, lo][:terms], axis=1)

    def twice(pos, at, base, n):
        out = jnp.zeros(pos.shape, F32)
        for k, w in ((-3, -0.0625), (-1, 0.5625), (0, 1.0), (1, 0.5625), (3, -0.0625)):
            m = 2 * at + k
            out = out + w * cubic(pos - 2 * m, inside(base + m, n))
        return out

    def restrict_x(ref, at):
        return (
            ref[at] + 0.5625 * (ref[at - 1] + ref[at + 1]) - 0.0625 * (ref[at - 3] + ref[at + 3])
        )

    lane = lax.broadcasted_iota(jnp.int32, (1, LANES), 1)
    has_r, has_l = there(*above), there(*below)
    mask_r, mask_l = (lane < LANES // 2) & has_r, (lane >= LANES // 2) & has_l
    rows2 = fy + 16
    i, j = grids(rows2, by)
    stack(my2, twice(j, jnp.where(i < fy + 8, i, i - rows2), gy * cy, ny * cy), 2)
    i, j = grids(2 * bz, LANES)
    pos = jnp.where(i < bz + bz // 2, i, i - 2 * bz)
    put(wz2, None, jnp.where(j < fz, twice(pos, j, gz * cz, nz * cz), 0.0))

    @pl.loop(0, bx // 2, unroll=4)
    def _(c):
        o = dot_left(my2, jnp.concatenate([x_ref[2 * c], x_ref[2 * c + 1]], axis=1), 2)
        ua[8 + 2 * c] = o[:, :LANES]
        ua[9 + 2 * c] = o[:, LANES:]

    for m in range(-1, cx + 2):
        am[m + 7] = restrict_x(ua, 8 + 2 * m) * inside(gx * cx + m, nx * cx).astype(F32)
    for e in range(fx + 5):
        v2[e] = restrict_x(am, 3 + 2 * e)
    start(z2)

    i, j = grids(2 * bz, bz)
    pos = jnp.where(i < bz + bz // 2, i, i - 2 * bz)
    k0 = pick(taps, 0, 2, pos - j + 8, inside(pos, bz + 8) | inside(pos + 8, 8))
    rz = cubic(pos - 2 * j, j < cz)
    put(w0h, w0l, jnp.concatenate([k0, rz], axis=1))
    i, j = grids(by + cy, by + 16)
    j = jnp.where(j < by, j + 8, jnp.where(j < by + 8, j - by, j))
    stack(m0, jnp.where(i < by, pick(taps, 0, 1, j - i, i < by), cubic(j - 8 - 2 * (i - by), i >= by)), 3)

    step0 = 4

    def across(own, lo, hi):
        rows = own.shape[0] * own.shape[1]
        other = jnp.where(
            mask_r, hi.reshape(rows, LANES), jnp.where(mask_l, lo.reshape(rows, LANES), 0.0)
        )
        v = jnp.concatenate([own.reshape(rows, LANES), other], axis=1)
        return split(dot_right(v, (w0h, w0l)))

    def level0_own(c):
        at = pl.ds(c * step0, step0)
        hi, lo = across(x_ref[at], l0[at], r0[at])
        zh[at, pl.ds(0, by), :] = hi.reshape(step0, by, 2 * LANES)
        zl[at, pl.ds(0, by), :] = lo.reshape(step0, by, 2 * LANES)

    def level0_halo(x, n):
        at = pl.ds(x, n)
        hi, lo = across(hy[at], hl[at], hr[at])
        zh[at, pl.ds(by, 16), :] = hi.reshape(n, 16, 2 * LANES)
        zl[at, pl.ds(by, 16), :] = lo.reshape(n, 16, 2 * LANES)

    def level0(k):
        hi = zh[k]
        o = mm(m0[...], jnp.concatenate([hi, zl[k], hi], axis=0))
        y0[8 + k] = o[:by, :LANES]
        y1[8 + k] = o[by:, LANES:]

    arrive(za)
    edge = 8 // step0
    for c in range(edge):
        level0_own(c)
        level0_own(bx // step0 - edge + c)
    arrive(z2)
    parts = []
    for e in range(fx + 5):
        other = jnp.where(mask_r, v2r[e], jnp.where(mask_l, v2l[e], 0.0))
        parts.append(jnp.concatenate([v2[e], other], axis=1))
    v = dot_right(jnp.concatenate(parts, axis=0), (wz2, None))
    for g in range(np2 + 2):
        acc = None
        for s in range(per):
            e = per * (g - 1) + s + 2
            if 0 <= e < fx + 5:
                w = v[e * rows2:(e + 1) * rows2]
                w = pltpu.roll(w, fz * s, 1) if s else w
                acc = w if acc is None else acc + w
        pq[g] = acc
    start(yp)

    arrive(ya[0])
    start(zf[0])
    pl.loop(edge, bx // step0 - edge, unroll=4)(level0_own)
    arrive(ya[1])
    start(zf[1])
    arrive(zf[0])
    level0_halo(0, 8)
    level0_halo(bx - 8, 8)
    for k in range(8):
        level0(k)
        level0(bx - 8 + k)
    def spread(dim, n, ref, k0):
        out = []
        for m, d in enumerate([d for d in range(-(n - 1), n) if d]):
            dev = tuple(here[k] + (d if k == dim else 0) for k in range(3))
            copy = pltpu.make_async_remote_copy(
                src_ref=ref(here[dim]), dst_ref=ref(here[dim]),
                send_sem=sg.at[dim, m], recv_sem=rg.at[dim, m],
                device_id=dev, device_id_type=pl.DeviceIdType.MESH,
            )
            land = pltpu.make_async_remote_copy(
                src_ref=ref(here[dim]), dst_ref=ref(here[dim] - d),
                send_sem=sg.at[dim, m], recv_sem=rg.at[dim, m],
                device_id=dev, device_id_type=pl.DeviceIdType.MESH,
            )
            to = inside(here[dim] + d, n)
            fro = inside(here[dim] - d, n)
            out.append((to, fro, copy, land))
        return out

    def begin(copies):
        for to, _, copy, _ in copies:
            pl.when(to)(copy.start)

    def landed(copies):
        for _, fro, _, land in copies:
            pl.when(fro)(land.wait_recv)

    arrive(yp)
    own = [pq[:, pl.ds(0, 8)] + yu[...]]
    if fy > 16:
        own.append(pq[:, pl.ds(8, fy - 16)])
    own.append(pq[:, pl.ds(fy - 8, 8)] + yd[...])
    xg[gx] = jnp.concatenate(own, axis=1)
    ca = spread(0, nx, lambda k: xg.at[k], 0)
    begin(ca)
    start(xa[0])
    arrive(zf[1])
    level0_halo(8, bx - 16)
    pl.loop(8, bx - 8, unroll=8)(level0)

    for p in range(half1 + 2):
        a = restrict_x(y1, 4 + 4 * p)
        b = restrict_x(y1, 6 + 4 * p)
        t1[p] = jnp.where(lane < cz, a, pltpu.roll(b, cz, 1))
    start(xb)
    start(xa[1])

    def conv0(p):
        acc = taps[0, 0, 0] * y0[p]
        for t in range(1, 17):
            acc = acc + taps[0, 0, t] * y0[p + t]
        out_ref[p] = acc

    pl.loop(8, bx - 8)(conv0)

    landed(ca)
    for m in range(np2 * nx):
        acc = None
        for b in range(nx):
            k = m - np2 * b + 1
            if 0 <= k < np2 + 2:
                acc = xg[b, k] if acc is None else acc + xg[b, k]
        g2[gz, gy, m] = acc
    cb = spread(1, ny, lambda k: g2.at[gz, k], 0)
    begin(cb)

    i, j = grids(2 * cz, LANES)
    pos = jnp.where(i < cz + cz // 2, i, i - 2 * cz)
    kk = j - 2
    top = cz + 4
    ok = (j < top) & inside(gz * cz + kk, nz * cz)
    k1 = pick(taps, 1, 2, pos - kk + 8, ok)
    i, j = grids(LANES, bz)
    fine_z = cubic(j - 2 * (i - 2), i < top)
    put(w1h, w1l, exact(k1, fine_z))
    ry1 = up(cy + 4, 8)
    i, j = grids(ry1, cy + 32)
    ok = (i < cy + 4) & inside(gy * cy + i - 2, ny * cy)
    stack(m1, pick(taps, 1, 1, j - 16 - (i - 2) + 8, ok), 3)
    i, j = grids(by, up(ry1, 16))
    stack(py1, cubic(i - 2 * (j - 2), j < cy + 4), 2)

    def plain(axis, level, n, pad, turned):
        i, j = grids(pad, pad)
        d = (i - j if turned else j - i) + 8
        return pick(taps, level, axis, d, (i < n) & (j < n))

    def rest(n, pad, big, turned_r):
        i, j = grids(*((big, pad) if turned_r else (pad, big)))
        c, f = (j, i) if turned_r else (i, j)
        return cubic(f - 2 * c, (c < n) & (f < 2 * n))

    def operators(axis, n2, first, rows, count):
        n3, n4 = n2 // 2, n2 // 4
        q = up(n2, LANES)
        i, j = grids(rows, q)
        g = first + i
        ok = (i < count) & inside(g, n2)
        one = pick(taps, 2, axis, j - g + 8, ok & (j < n2))
        pr = cubic(g - 2 * j, ok & (j < n3))
        r23, r34 = rest(n3, q, q, False), rest(n4, q, q, False)
        p34 = rest(n4, q, q, True)
        two = exact(exact(pr, plain(axis, 3, n3, q, False)), r23)
        three = exact(exact(exact(exact(pr, p34), plain(axis, 4, n4, q, False)), r34), r23)
        return one, two, three

    n2x, n2y, n2z = nx * fx, ny * fy, nz * fz
    ez, ey, ex = fz + 5, fy + 5, fx + 5
    tz = 40
    ops = operators(2, n2z, gz * fz - 2, tz, ez)
    cols = jnp.concatenate(list(ops) + [jnp.zeros((LANES - 3 * tz, ops[0].shape[1]), F32)], axis=0)
    hi, lo = split(cols.T)
    for ref, v in ((w2h, hi), (w2l, lo)):
        ref[...] = jnp.zeros(ref.shape, BF16)
        for b in range(nz):
            for k in range(per):
                ref[pl.ds(b * LANES + k * fz, fz), pl.ds(k * LANES, LANES)] = v[b * fz:(b + 1) * fz]
    ty = up(ey, 8)
    ops = operators(1, n2y, gy * fy - 2, ty, ey)
    stack(m2, jnp.concatenate(list(ops), axis=0)[:, :n2y], 3)
    tx = up(ex, 8)
    ops = operators(0, n2x, gx * fx - 2, tx, ex)
    tall = [o.T for o in ops]
    for r in range(ex):
        a, b, c = (o[:n2x, r:r + 1] for o in tall)
        c2[r] = jnp.where(lane < tz, a, jnp.where(lane < 2 * tz, b, c))
    i, j = grids(LANES, LANES)
    src = i - jnp.where(i < tz, 0, jnp.where(i < 2 * tz, tz, 2 * tz)) - 2
    e1_z = cubic((j - 2) - 2 * src, (i < 3 * tz) & (src < fz + 3) & (j < top) & inside(gz * cz + j - 2, nz * cz))
    put(pz2, None, exact(e1_z, fine_z))
    i, j = grids(ry1, up(ty, 16))
    stack(py2, cubic((i - 2) - 2 * (j - 2), (j < ey) & (i < cy + 4) & inside(gy * cy + i - 2, ny * cy)), 2)
    arrive(xb)
    n1 = half1 + 10
    to_l, to_r = there(*left).astype(F32), there(*right).astype(F32)
    for k in range(n1):
        if k < 4:
            v = t1l[k]
        elif k < 6:
            v = t1l[k] + (t1[k - 4] * to_l if k == 4 else t1[k - 4])
        elif k < half1 + 4:
            v = t1[k - 4]
        elif k < half1 + 6:
            v = t1r[k - half1 - 4] + (t1[k - 4] * to_r if k == half1 + 5 else t1[k - 4])
        else:
            v = t1r[k - half1 - 4]
        e1[k] = v
        back = pltpu.roll(v, cz, 1)
        if k:
            sw[k - 1] = jnp.where(lane < cz, last, back)
        last = back

    @pl.loop(0, half1 + 2)
    def _(q):
        acc = taps[1, 0, 0] * e1[q]
        for t in range(1, 17):
            acc = acc + taps[1, 0, t] * (sw[q + (t - 1) // 2] if t % 2 else e1[q + t // 2])
        f1[q, pl.ds(16, cy), :] = acc

    start(yb)
    landed(cb)
    cc = spread(2, nz, lambda k: g2.at[k], 0)
    begin(cc)
    arrive(yb)
    for q in range(0, half1 + 2, 2):
        o = dot_left(m1, jnp.concatenate([f1[q], f1[q + 1]], axis=1), 3)
        h1[q] = o[:, :LANES]
        h1[q + 1] = o[:, LANES:]
    start(zb)
    landed(cc)
    seen = lambda r: inside(gx * cx + r - 2, nx * cx).astype(F32)
    batch = max(1, min(nx * np2, 256 // n2y))
    for m in range(0, nx * np2, batch):
        v = jnp.concatenate([
            jnp.concatenate([g2[b, :, k].reshape(n2y, LANES) for b in range(nz)], axis=1)
            for k in range(m, m + batch)
        ], axis=0)
        hi, lo = split(dot_right(v, (w2h, w2l)))
        z2h[pl.ds(m, batch)] = hi.reshape(batch, n2y, per * LANES)
        z2l[pl.ds(m, batch)] = lo.reshape(batch, n2y, per * LANES)

    @pl.loop(0, nx * np2, unroll=4)
    def _(m):
        hi = z2h[m]
        o = mm(m2[...], jnp.concatenate([hi, z2l[m], hi], axis=0))
        for k in range(per):
            w = o[:, k * LANES:(k + 1) * LANES]
            y2[per * m + k] = jnp.where(
                lane < tz, w[:ty], jnp.where(lane < 2 * tz, w[ty:2 * ty], w[2 * ty:])
            )

    parts = []
    for r in range(ex):
        acc = c2[r, pl.ds(0, 1)] * y2[0]
        for q in range(1, n2x):
            acc = acc + c2[r, pl.ds(q, 1)] * y2[q]
        parts.append(acc)
    v = dot_right(jnp.concatenate(parts, axis=0), (pz2, None))
    fill = up(ty, 16) - ty
    pro = []
    for r in range(ex):
        w = v[r * ty:(r + 1) * ty]
        if fill:
            w = jnp.concatenate([w, jnp.zeros((fill, LANES), F32)], axis=0)
        pro.append(dot_left(py2, w, 2))
    arrive(zb)
    near = lax.rem(lane, cz) < cz // 2
    step1 = 5 if (half1 + 2) % 5 == 0 else 1
    for c in range(0, half1 + 2, step1):
        parts = []
        for q in range(c, c + step1):
            own = h1[q]
            other = jnp.where(near & has_r, h1r[q], jnp.where(jnp.logical_not(near) & has_l, h1l[q], 0.0))
            parts.append(jnp.where(lane < cz, own, pltpu.roll(other, cz, 1)))
            parts.append(jnp.where(lane < cz, pltpu.roll(own, cz, 1), other))
        v = dot_right(jnp.concatenate(parts, axis=0), (w1h, w1l))
        for k in range(2 * step1):
            d1[2 * c + k] = v[k * ry1:(k + 1) * ry1]
    for p in range(cx + 4):
        m = (p - 2) // 2 + 2
        if p % 2 == 0:
            w = pro[m]
        else:
            w = 0.5625 * (pro[m] + pro[m + 1]) - 0.0625 * (pro[m - 1] + pro[m + 2])
        d1[p] = (d1[p] + w) * seen(p)

    fill1 = up(ry1, 16) - ry1

    @pl.loop(0, (cx + 4) // 2, unroll=5)
    def _(c):
        v = jnp.concatenate([d1[2 * c], d1[2 * c + 1]], axis=1)
        if fill1:
            v = jnp.concatenate([v, jnp.zeros((fill1, 2 * LANES), F32)], axis=0)
        o = dot_left(py1, v, 2)
        pr[2 * c] = o[:, :LANES]
        pr[2 * c + 1] = o[:, LANES:]

    for group in xa:
        arrive(group)
    pl.loop(0, 8)(conv0)
    pl.loop(bx - 8, bx)(conv0)

    @pl.loop(0, cx)
    def _(m):
        at = m + 2
        out_ref[2 * m] = out_ref[2 * m] + pr[at]
        out_ref[2 * m + 1] = out_ref[2 * m + 1] + (
            0.5625 * (pr[at] + pr[at + 1]) - 0.0625 * (pr[at - 1] + pr[at + 2])
        )

    for group in (*ya, za, *zf, z2, yp, *xa, xb, yb, zb):
        left_over(group)
    for group in (ca, cb, cc):
        for to, _, copy, _ in group:
            pl.when(to)(copy.wait_send)


def per_device(counts, charges, kernel_taps):
    nx, ny, nz = counts
    bx, by, bz = dims = charges.shape
    assert bz == LANES
    cx, cy, cz = bx // 2, by // 2, bz // 2
    fx, fy, fz = bx // 4, by // 4, bz // 4
    n2x, n2y, n2z = nx * fx, ny * fy, nz * fz
    per = LANES // fz
    np2 = fx // per
    half1 = cx // 2
    ry1 = up(cy + 4, 8)
    ty = up(fy + 5, 8)
    V = pltpu.VMEM
    wide = max(nx, ny, nz) * 2
    dma = pltpu.SemaphoreType.DMA
    row = lambda n, r: V((n, r, LANES), F32)
    scratch = [
        pltpu.SMEM(kernel_taps.shape, F32), V(dims, F32),
        row(bx, by), row(bx, by), row(bx, 16), row(bx, 16), row(bx, 16),
        V((bx, by + 16, 2 * LANES), BF16), V((bx, by + 16, 2 * LANES), BF16),
        row(bx + 16, by), row(bx + 16, cy),
        row(half1 + 2, cy), row(6, cy), row(6, cy), row(half1 + 10, cy), row(half1 + 9, cy),
        row(half1 + 2, cy + 32), row(half1 + 2, ry1), row(half1 + 2, ry1), row(half1 + 2, ry1),
        row(cx + 4, ry1), row(cx + 4, by),
        row(bx + 16, fy + 16), row(cx + 15, fy + 16),
        row(fx + 5, fy + 16), row(fx + 5, fy + 16), row(fx + 5, fy + 16),
        row(np2 + 2, fy + 16), row(np2 + 2, 8), row(np2 + 2, 8),
        V((nx, np2 + 2, fy, LANES), F32),
        V((nz, ny, nx * np2, fy, LANES), F32),
        V((nx * np2, n2y, per * LANES), BF16), V((nx * np2, n2y, per * LANES), BF16),
        row(n2x, ty),
        V((2 * bz, bz + LANES), BF16), V((2 * bz, bz + LANES), BF16),
        V((by + cy, 3 * (by + 16)), BF16),
        V((2 * cz, bz), BF16), V((2 * cz, bz), BF16),
        V((ry1, 3 * (cy + 32)), BF16),
        V((nz * LANES, per * LANES), BF16), V((nz * LANES, per * LANES), BF16),
        V((3 * ty, 3 * n2y), BF16),
        row(fx + 5, n2x),
        V((LANES, bz), BF16), V((ry1, 2 * up(ty, 16)), BF16),
        V((by, 2 * up(ry1, 16)), BF16),
        V((fy + 16, 2 * by), BF16), V((2 * bz, LANES), BF16),
        dma((2,)), dma((32,)), dma((32,)), dma((3, wide)), dma((3, wide)),
    ]
    return pl.pallas_call(
        functools.partial(kernel, counts, dims),
        out_shape=jax.ShapeDtypeStruct(dims, F32),
        in_specs=[pl.BlockSpec(memory_space=pltpu.HBM)] * 2,
        out_specs=pl.BlockSpec(memory_space=pltpu.VMEM),
        scratch_shapes=scratch,
        compiler_params=pltpu.CompilerParams(
            collective_id=0, has_side_effects=True, vmem_limit_bytes=105 * 2**19
        ),
    )(kernel_taps, charges)


def solution(mesh):
    counts = tuple(mesh.shape[a] for a in AXES)
    return jax.shard_map(
        functools.partial(per_device, counts), mesh=mesh,
        in_specs=(P("gx", "gy", "gz"), P()), out_specs=P("gx", "gy", "gz"), check_vma=False,
    )
```

```python
import functools

import jax
import jax.numpy as jnp
from jax import lax
from jax.experimental import pallas as pl
from jax.experimental.pallas import tpu as pltpu
from jax.sharding import PartitionSpec as P

F32, BF16 = jnp.float32, jnp.bfloat16
LANES = 128
U0, U1, U2, U3 = 4, 4, 4, 5
AXES = ("gx", "gy", "gz")
ODD = (-0.0625, 0.5625, 0.5625, -0.0625)
SIDES = tuple((a, b) for a in (-1, 0, 1) for b in (-1, 0, 1) if (a, b) != (0, 0))


def split(v):
    hi = v.astype(BF16)
    return hi, (v - hi.astype(F32)).astype(BF16)


def mm(a, b):
    return jnp.dot(a, b, preferred_element_type=F32)


def exact(a, b):
    return jnp.dot(a, b, preferred_element_type=F32, precision=lax.Precision.HIGHEST)


def dot_right(v, w):
    hi, lo = split(v)
    out = mm(hi, w[0][...]) + mm(lo, w[0][...])
    return out if w[1] is None else out + mm(hi, w[1][...])


def dot_left(w_ref, v, terms):
    hi, lo = split(v)
    return mm(w_ref[...], jnp.concatenate([hi, lo, hi][:terms], axis=0))


def grids(rows, cols):
    return (
        lax.broadcasted_iota(jnp.int32, (rows, cols), 0),
        lax.broadcasted_iota(jnp.int32, (rows, cols), 1),
    )


def pick(taps, level, axis, diff, ok):
    out = jnp.zeros(diff.shape, F32)
    for t in range(17):
        out = jnp.where(diff == t, taps[level, axis, t], out)
    return jnp.where(ok, out, 0.0)


def cubic(diff, ok):
    d = jnp.abs(diff)
    out = jnp.where(d == 0, 1.0, jnp.where(d == 1, 0.5625, jnp.where(d == 3, -0.0625, 0.0)))
    return jnp.where(ok, out, 0.0).astype(F32)


def up(n, m):
    return -(-n // m) * m


def inside(v, n):
    return (v >= 0) & (v < n)


def kernel(counts, dims, taps_hbm, x_hbm, out_ref, taps, x_ref, l0, r0, hy, hl, hr, zh, zl, relay, y0, y1, t1, t1l, t1r, e1, sw, f1, h1, h1l, h1r, d1, pr,
           ua, am, v2, v2l, v2r, pq, yu, yd, xg, g2, z2h, z2l, y2,
           w0h, w0l, m0, w1h, w1l, m1, w2h, w2l, m2, c2, pz2, py2, py1, my2, wz2, own_sem, ss, rs, sg, rg):
    nx, ny, nz = counts
    bx, by, bz = dims
    here = tuple(lax.axis_index(a) for a in AXES)
    loads = [
        pltpu.make_async_copy(x_hbm, x_ref, own_sem.at[0]),
        pltpu.make_async_copy(taps_hbm, taps, own_sem.at[1]),
    ]
    for load in loads:
        load.start()
    gx, gy, gz = here
    cx, cy, cz = bx // 2, by // 2, bz // 2
    fx, fy, fz = bx // 4, by // 4, bz // 4
    half1 = cx // 2
    per = LANES // fz
    np2 = fx // per

    def there(dx, dy, dz):
        return inside(gx + dx, nx) & inside(gy + dy, ny) & inside(gz + dz, nz)

    partners = []
    for dim, n in enumerate(counts):
        for d in range(1, n):
            for sgn in (-d, d):
                partners.append(tuple(sgn if k == dim else 0 for k in range(3)))
    barrier = pltpu.get_barrier_semaphore()
    total = jnp.int32(0)
    for p in partners:
        ok = there(*p)
        total = total + ok.astype(jnp.int32)

        @pl.when(ok)
        def _(p=p):
            pl.semaphore_signal(
                barrier, inc=1, device_id=(gx + p[0], gy + p[1], gz + p[2]),
                device_id_type=pl.DeviceIdType.MESH,
            )

    def clear(ref, d, *at):
        @pl.when(jnp.logical_not(there(*d)))
        def _():
            view = ref.at[at]
            view[...] = jnp.zeros(view.shape, F32)

    every = slice(None)
    clear(hy, (0, -1, 0), every, pl.ds(0, 8))
    clear(hy, (0, 1, 0), every, pl.ds(8, 8))
    clear(y0, (-1, 0, 0), pl.ds(0, 8))
    clear(y0, (1, 0, 0), pl.ds(8 + bx, 8))
    clear(t1l, (-1, 0, 0), every)
    clear(t1r, (1, 0, 0), every)
    clear(f1, (0, -1, 0), every, pl.ds(0, 16))
    clear(f1, (0, 1, 0), every, pl.ds(16 + cy, 16))
    clear(yu, (0, -1, 0), every)
    clear(yd, (0, 1, 0), every)
    for ref in (ua, y1):
        ref[pl.ds(0, 8)] = jnp.zeros((8,) + ref.shape[1:], F32)
        ref[pl.ds(8 + bx, 8)] = jnp.zeros((8,) + ref.shape[1:], F32)
    am[pl.ds(0, 6)] = jnp.zeros((6,) + am.shape[1:], F32)
    am[pl.ds(cx + 9, 6)] = jnp.zeros((6,) + am.shape[1:], F32)
    right, left, ahead, behind, above, below = (
        (1, 0, 0), (-1, 0, 0), (0, 1, 0), (0, -1, 0), (0, 0, 1), (0, 0, -1)
    )
    def put(h, l, v):
        hi, lo = split(v)
        h[...] = hi
        if l is not None:
            l[...] = lo

    def stack(ref, v, terms):
        hi, lo = split(v)
        ref[...] = jnp.concatenate([hi, hi, lo][:terms], axis=1)

    def twice(pos, at, base, n):
        out = jnp.zeros(pos.shape, F32)
        for k, w in ((-3, -0.0625), (-1, 0.5625), (0, 1.0), (1, 0.5625), (3, -0.0625)):
            m = 2 * at + k
            out = out + w * cubic(pos - 2 * m, inside(base + m, n))
        return out

    def restrict_x(ref, at):
        return (
            ref[at] + 0.5625 * (ref[at - 1] + ref[at + 1]) - 0.0625 * (ref[at - 3] + ref[at + 3])
        )

    lane = lax.broadcasted_iota(jnp.int32, (1, LANES), 1)
    has_r, has_l = there(*above), there(*below)
    mask_r, mask_l = (lane < LANES // 2) & has_r, (lane >= LANES // 2) & has_l
    rows2 = fy + 16
    i, j = grids(rows2, by)
    stack(my2, twice(j, jnp.where(i < fy + 8, i, i - rows2), gy * cy, ny * cy), 2)
    i, j = grids(2 * bz, LANES)
    pos = jnp.where(i < bz + bz // 2, i, i - 2 * bz)
    put(wz2, None, jnp.where(j < fz, twice(pos, j, gz * cz, nz * cz), 0.0))

    loads[1].wait()
    i, j = grids(2 * bz, bz)
    pos = jnp.where(i < bz + bz // 2, i, i - 2 * bz)
    k0 = pick(taps, 0, 2, pos - j + 8, inside(pos, bz + 8) | inside(pos + 8, 8))
    rz = cubic(pos - 2 * j, j < cz)
    put(w0h, w0l, jnp.concatenate([k0, rz], axis=1))
    i, j = grids(by + cy, by + 16)
    j = jnp.where(j < by, j + 8, jnp.where(j < by + 8, j - by, j))
    stack(m0, jnp.where(i < by, pick(taps, 0, 1, j - i, i < by), cubic(j - 8 - 2 * (i - by), i >= by)), 3)

    i, j = grids(2 * cz, LANES)
    pos = jnp.where(i < cz + cz // 2, i, i - 2 * cz)
    kk = j - 2
    top = cz + 4
    ok = (j < top) & inside(gz * cz + kk, nz * cz)
    k1 = pick(taps, 1, 2, pos - kk + 8, ok)
    i, j = grids(LANES, bz)
    fine_z = cubic(j - 2 * (i - 2), i < top)
    put(w1h, w1l, exact(k1, fine_z))
    ry1 = up(cy + 4, 8)
    i, j = grids(ry1, cy + 32)
    ok = (i < cy + 4) & inside(gy * cy + i - 2, ny * cy)
    stack(m1, pick(taps, 1, 1, j - 16 - (i - 2) + 8, ok), 3)
    i, j = grids(by, up(ry1, 16))
    stack(py1, cubic(i - 2 * (j - 2), j < cy + 4), 2)

    loads[0].wait()

    @pl.loop(0, bx // 2, unroll=4)
    def _(c):
        o = dot_left(my2, jnp.concatenate([x_ref[2 * c], x_ref[2 * c + 1]], axis=1), 2)
        ua[8 + 2 * c] = o[:, :LANES]
        ua[9 + 2 * c] = o[:, LANES:]

    for m in range(-1, cx + 2):
        am[m + 7] = restrict_x(ua, 8 + 2 * m) * inside(gx * cx + m, nx * cx).astype(F32)
    for e in range(fx + 5):
        v2[e] = restrict_x(am, 3 + 2 * e)
    pl.semaphore_wait(barrier, total)

    count = [0]

    def remote(src, dst, d, to=None, fro=None):
        k = count[0]
        count[0] += 1
        copy = pltpu.make_async_remote_copy(
            src_ref=src, dst_ref=dst, send_sem=ss.at[k], recv_sem=rs.at[k],
            device_id=(gx + d[0], gy + d[1], gz + d[2]), device_id_type=pl.DeviceIdType.MESH,
        )
        to = there(*d) if to is None else to
        fro = there(-d[0], -d[1], -d[2]) if fro is None else fro
        return to, fro, copy

    def start(copies):
        for to, _, copy in copies:
            pl.when(to)(copy.start)

    def arrive(copies):
        for _, fro, copy in copies:
            pl.when(fro)(copy.wait_recv)

    def left_over(copies):
        for to, _, copy in copies:
            pl.when(to)(copy.wait_send)

    ends = (pl.ds(0, 8), pl.ds(bx - 8, 8)), (pl.ds(8, bx - 16),)
    ya, zf = [], []
    for xs in ends:
        ya.append([
            remote(x_ref.at[x, pl.ds(by - 8, 8)], hy.at[x, pl.ds(0, 8)], ahead) for x in xs
        ] + [
            remote(x_ref.at[x, pl.ds(0, 8)], hy.at[x, pl.ds(8, 8)], behind) for x in xs
        ])
        zf.append([remote(hy.at[x], hl.at[x], above) for x in xs] + [remote(hy.at[x], hr.at[x], below) for x in xs])
    za = [remote(x_ref, l0, above), remote(x_ref, r0, below)]
    z2 = [remote(v2, v2l, above), remote(v2, v2r, below)]
    yp = [
        remote(pq.at[:, pl.ds(fy, 8)], yu, ahead),
        remote(pq.at[:, pl.ds(fy + 8, 8)], yd, behind),
    ]
    mid_l, mid_r = (gx == 1, gx == 2) if nx == 4 else (jnp.bool_(False), jnp.bool_(False))
    end_l, end_r = (gx == 0, gx == 3) if nx == 4 else (jnp.bool_(False), jnp.bool_(False))
    near, rest = 2, 6

    def to_left(k, n, **ok):
        return remote(y0.at[pl.ds(8 + k, n)], y0.at[pl.ds(8 + bx + k, n)], left, **ok)

    def to_right(k, n, **ok):
        return remote(y0.at[pl.ds(bx + k, n)], y0.at[pl.ds(k, n)], right, **ok)

    xa = [
        [to_left(0, near)],
        [
            to_left(near, rest, to=there(*left) & jnp.logical_not(mid_r), fro=there(*right) & jnp.logical_not(mid_l)),
            to_right(0, near),
            to_right(near, rest, to=there(*right) & jnp.logical_not(mid_l), fro=there(*left) & jnp.logical_not(mid_r)),
        ],
    ]
    hop1, hop2 = [], []
    if nx == 4:
        hop1 = [
            remote(y0.at[pl.ds(bx + near, rest)], relay, (2, 0, 0), to=mid_l, fro=end_r),
            remote(y0.at[pl.ds(8 + near, rest)], relay, (-2, 0, 0), to=mid_r, fro=end_l),
        ]
        hop2 = [
            remote(relay, y0.at[pl.ds(near, rest)], left, to=end_r, fro=mid_r),
            remote(relay, y0.at[pl.ds(8 + bx + near, rest)], right, to=end_l, fro=mid_l),
        ]
    xb = [remote(t1.at[pl.ds(0, 6)], t1r, left), remote(t1.at[pl.ds(half1 - 4, 6)], t1l, right)]
    yb = [
        remote(f1.at[:, pl.ds(cy, 16)], f1.at[:, pl.ds(0, 16)], ahead),
        remote(f1.at[:, pl.ds(16, 16)], f1.at[:, pl.ds(16 + cy, 16)], behind),
    ]
    zb = [remote(h1, h1l, above), remote(h1, h1r, below)]
    start(z2)
    start(ya[0])
    start(za)
    arrive(z2)
    parts = []
    for e in range(fx + 5):
        other = jnp.where(mask_r, v2r[e], jnp.where(mask_l, v2l[e], 0.0))
        parts.append(jnp.concatenate([v2[e], other], axis=1))
    v = dot_right(jnp.concatenate(parts, axis=0), (wz2, None))
    for g in range(np2 + 2):
        acc = None
        for s in range(per):
            e = per * (g - 1) + s + 2
            if 0 <= e < fx + 5:
                w = v[e * rows2:(e + 1) * rows2]
                w = pltpu.roll(w, fz * s, 1) if s else w
                acc = w if acc is None else acc + w
        pq[g] = acc
    start(yp)

    start(ya[1])
    def plain(axis, level, n, pad, turned):
        i, j = grids(pad, pad)
        d = (i - j if turned else j - i) + 8
        return pick(taps, level, axis, d, (i < n) & (j < n))

    def rest(n, pad, big, turned_r):
        i, j = grids(*((big, pad) if turned_r else (pad, big)))
        c, f = (j, i) if turned_r else (i, j)
        return cubic(f - 2 * c, (c < n) & (f < 2 * n))

    def operators(axis, n2, first, rows, count):
        n3, n4 = n2 // 2, n2 // 4
        q = up(n2, LANES)
        i, j = grids(rows, q)
        g = first + i
        ok = (i < count) & inside(g, n2)
        one = pick(taps, 2, axis, j - g + 8, ok & (j < n2))
        pr = cubic(g - 2 * j, ok & (j < n3))
        r23, r34 = rest(n3, q, q, False), rest(n4, q, q, False)
        p34 = rest(n4, q, q, True)
        two = exact(exact(pr, plain(axis, 3, n3, q, False)), r23)
        three = exact(exact(exact(exact(pr, p34), plain(axis, 4, n4, q, False)), r34), r23)
        return one, two, three

    n2x, n2y, n2z = nx * fx, ny * fy, nz * fz
    ez, ey, ex = fz + 5, fy + 5, fx + 5
    tz = 40
    ops = operators(2, n2z, gz * fz - 2, tz, ez)
    cols = jnp.concatenate(list(ops) + [jnp.zeros((LANES - 3 * tz, ops[0].shape[1]), F32)], axis=0)
    hi, lo = split(cols.T)
    for ref, v in ((w2h, hi), (w2l, lo)):
        ref[...] = jnp.zeros(ref.shape, BF16)
        for b in range(nz):
            for k in range(per):
                ref[pl.ds(b * LANES + k * fz, fz), pl.ds(k * LANES, LANES)] = v[b * fz:(b + 1) * fz]
    ty = up(ey, 8)
    ops = operators(1, n2y, gy * fy - 2, ty, ey)
    stack(m2, jnp.concatenate(list(ops), axis=0)[:, :n2y], 3)
    tx = up(ex, 8)
    ops = operators(0, n2x, gx * fx - 2, tx, ex)
    tall = [o.T for o in ops]
    for r in range(ex):
        a, b, c = (o[:n2x, r:r + 1] for o in tall)
        c2[r] = jnp.where(lane < tz, a, jnp.where(lane < 2 * tz, b, c))
    i, j = grids(LANES, LANES)
    src = i - jnp.where(i < tz, 0, jnp.where(i < 2 * tz, tz, 2 * tz)) - 2
    e1_z = cubic((j - 2) - 2 * src, (i < 3 * tz) & (src < fz + 3) & (j < top) & inside(gz * cz + j - 2, nz * cz))
    put(pz2, None, exact(e1_z, fine_z))
    i, j = grids(ry1, up(ty, 16))
    stack(py2, cubic((i - 2) - 2 * (j - 2), (j < ey) & (i < cy + 4) & inside(gy * cy + i - 2, ny * cy)), 2)
    arrive(ya[0])
    start(zf[0])
    def spread(dim, n, ref, k0):
        out = []
        for m, d in enumerate([d for d in range(-(n - 1), n) if d]):
            dev = tuple(here[k] + (d if k == dim else 0) for k in range(3))
            copy = pltpu.make_async_remote_copy(
                src_ref=ref(here[dim]), dst_ref=ref(here[dim]),
                send_sem=sg.at[dim, m], recv_sem=rg.at[dim, m],
                device_id=dev, device_id_type=pl.DeviceIdType.MESH,
            )
            land = pltpu.make_async_remote_copy(
                src_ref=ref(here[dim]), dst_ref=ref(here[dim] - d),
                send_sem=sg.at[dim, m], recv_sem=rg.at[dim, m],
                device_id=dev, device_id_type=pl.DeviceIdType.MESH,
            )
            to = inside(here[dim] + d, n)
            fro = inside(here[dim] - d, n)
            out.append((to, fro, copy, land))
        return out

    def begin(copies):
        for to, _, copy, _ in copies:
            pl.when(to)(copy.start)

    def landed(copies):
        for _, fro, _, land in copies:
            pl.when(fro)(land.wait_recv)

    arrive(yp)
    own = [pq[:, pl.ds(0, 8)] + yu[...]]
    if fy > 16:
        own.append(pq[:, pl.ds(8, fy - 16)])
    own.append(pq[:, pl.ds(fy - 8, 8)] + yd[...])
    xg[gx] = jnp.concatenate(own, axis=1)
    ca = spread(0, nx, lambda k: xg.at[k], 0)
    begin(ca)


    step0 = 4

    def across(own, lo, hi):
        rows = own.shape[0] * own.shape[1]
        other = jnp.where(
            mask_r, hi.reshape(rows, LANES), jnp.where(mask_l, lo.reshape(rows, LANES), 0.0)
        )
        v = jnp.concatenate([own.reshape(rows, LANES), other], axis=1)
        return split(dot_right(v, (w0h, w0l)))

    def level0_own(c):
        at = pl.ds(c * step0, step0)
        hi, lo = across(x_ref[at], l0[at], r0[at])
        zh[at, pl.ds(0, by), :] = hi.reshape(step0, by, 2 * LANES)
        zl[at, pl.ds(0, by), :] = lo.reshape(step0, by, 2 * LANES)

    def level0_halo(x, n):
        at = pl.ds(x, n)
        hi, lo = across(hy[at], hl[at], hr[at])
        zh[at, pl.ds(by, 16), :] = hi.reshape(n, 16, 2 * LANES)
        zl[at, pl.ds(by, 16), :] = lo.reshape(n, 16, 2 * LANES)

    def level0(k):
        hi = zh[k]
        o = mm(m0[...], jnp.concatenate([hi, zl[k], hi], axis=0))
        y0[8 + k] = o[:by, :LANES]
        y1[8 + k] = o[by:, LANES:]

    arrive(za)
    edge = 8 // step0
    for c in range(edge):
        level0_own(c)
        level0_own(bx // step0 - edge + c)
    pl.loop(edge, bx // step0 - edge, unroll=4)(level0_own)
    arrive(ya[1])
    start(zf[1])
    arrive(zf[0])
    level0_halo(0, 8)
    level0_halo(bx - 8, 8)
    for k in range(8):
        level0(k)
        level0(bx - 8 + k)
    start(xa[0])
    start(hop1)
    arrive(zf[1])
    level0_halo(8, bx - 16)
    pl.loop(8, bx - 8, unroll=8)(level0)

    for p in range(half1 + 2):
        a = restrict_x(y1, 4 + 4 * p)
        b = restrict_x(y1, 6 + 4 * p)
        t1[p] = jnp.where(lane < cz, a, pltpu.roll(b, cz, 1))
    start(xb)
    start(xa[1])

    def conv0(p, ts):
        acc = None
        for t in ts:
            v = taps[0, 0, t] * y0[p + t]
            acc = v if acc is None else acc + v
        return acc

    @pl.loop(8, bx - 8)
    def _(p):
        out_ref[p] = conv0(p, range(17))

    landed(ca)
    for m in range(np2 * nx):
        acc = None
        for b in range(nx):
            k = m - np2 * b + 1
            if 0 <= k < np2 + 2:
                acc = xg[b, k] if acc is None else acc + xg[b, k]
        g2[gz, gy, m] = acc
    cb = spread(1, ny, lambda k: g2.at[gz, k], 0)
    begin(cb)

    for p in range(8):
        out_ref[p] = conv0(p, range(8 - p, 17))
        out_ref[bx - 8 + p] = conv0(bx - 8 + p, range(16 - p))
    arrive(hop1)
    start(hop2)
    arrive(xb)
    n1 = half1 + 10
    to_l, to_r = there(*left).astype(F32), there(*right).astype(F32)
    for k in range(n1):
        if k < 4:
            v = t1l[k]
        elif k < 6:
            v = t1l[k] + (t1[k - 4] * to_l if k == 4 else t1[k - 4])
        elif k < half1 + 4:
            v = t1[k - 4]
        elif k < half1 + 6:
            v = t1r[k - half1 - 4] + (t1[k - 4] * to_r if k == half1 + 5 else t1[k - 4])
        else:
            v = t1r[k - half1 - 4]
        e1[k] = v
        back = pltpu.roll(v, cz, 1)
        if k:
            sw[k - 1] = jnp.where(lane < cz, last, back)
        last = back

    @pl.loop(0, half1 + 2)
    def _(q):
        acc = taps[1, 0, 0] * e1[q]
        for t in range(1, 17):
            acc = acc + taps[1, 0, t] * (sw[q + (t - 1) // 2] if t % 2 else e1[q + t // 2])
        f1[q, pl.ds(16, cy), :] = acc

    start(yb)
    landed(cb)
    cc = spread(2, nz, lambda k: g2.at[k], 0)
    begin(cc)
    landed(cc)
    seen = lambda r: inside(gx * cx + r - 2, nx * cx).astype(F32)
    batch = max(1, min(nx * np2, 256 // n2y))
    for m in range(0, nx * np2, batch):
        v = jnp.concatenate([
            jnp.concatenate([g2[b, :, k].reshape(n2y, LANES) for b in range(nz)], axis=1)
            for k in range(m, m + batch)
        ], axis=0)
        hi, lo = split(dot_right(v, (w2h, w2l)))
        z2h[pl.ds(m, batch)] = hi.reshape(batch, n2y, per * LANES)
        z2l[pl.ds(m, batch)] = lo.reshape(batch, n2y, per * LANES)

    @pl.loop(0, nx * np2, unroll=4)
    def _(m):
        hi = z2h[m]
        o = mm(m2[...], jnp.concatenate([hi, z2l[m], hi], axis=0))
        for k in range(per):
            w = o[:, k * LANES:(k + 1) * LANES]
            y2[per * m + k] = jnp.where(
                lane < tz, w[:ty], jnp.where(lane < 2 * tz, w[ty:2 * ty], w[2 * ty:])
            )

    arrive(yb)
    for q in range(0, half1 + 2, 2):
        o = dot_left(m1, jnp.concatenate([f1[q], f1[q + 1]], axis=1), 3)
        h1[q] = o[:, :LANES]
        h1[q + 1] = o[:, LANES:]
    start(zb)
    parts = []
    for r in range(ex):
        acc = c2[r, pl.ds(0, 1)] * y2[0]
        for q in range(1, n2x):
            acc = acc + c2[r, pl.ds(q, 1)] * y2[q]
        parts.append(acc)
    v = dot_right(jnp.concatenate(parts, axis=0), (pz2, None))
    fill = up(ty, 16) - ty
    pro = []
    for r in range(ex):
        w = v[r * ty:(r + 1) * ty]
        if fill:
            w = jnp.concatenate([w, jnp.zeros((fill, LANES), F32)], axis=0)
        pro.append(dot_left(py2, w, 2))
    arrive(zb)
    inner = lax.rem(lane, cz) < cz // 2
    step1 = 5 if (half1 + 2) % 5 == 0 else 1
    for c in range(0, half1 + 2, step1):
        parts = []
        for q in range(c, c + step1):
            own = h1[q]
            other = jnp.where(inner & has_r, h1r[q], jnp.where(jnp.logical_not(inner) & has_l, h1l[q], 0.0))
            parts.append(jnp.where(lane < cz, own, pltpu.roll(other, cz, 1)))
            parts.append(jnp.where(lane < cz, pltpu.roll(own, cz, 1), other))
        v = dot_right(jnp.concatenate(parts, axis=0), (w1h, w1l))
        for k in range(2 * step1):
            d1[2 * c + k] = v[k * ry1:(k + 1) * ry1]
    for p in range(cx + 4):
        m = (p - 2) // 2 + 2
        if p % 2 == 0:
            w = pro[m]
        else:
            w = 0.5625 * (pro[m] + pro[m + 1]) - 0.0625 * (pro[m - 1] + pro[m + 2])
        d1[p] = (d1[p] + w) * seen(p)

    fill1 = up(ry1, 16) - ry1

    @pl.loop(0, (cx + 4) // 2, unroll=5)
    def _(c):
        v = jnp.concatenate([d1[2 * c], d1[2 * c + 1]], axis=1)
        if fill1:
            v = jnp.concatenate([v, jnp.zeros((fill1, 2 * LANES), F32)], axis=0)
        o = dot_left(py1, v, 2)
        pr[2 * c] = o[:, :LANES]
        pr[2 * c + 1] = o[:, LANES:]

    for group in (*xa, hop2):
        arrive(group)
    for p in range(8):
        out_ref[p] = out_ref[p] + conv0(p, range(8 - p))
        out_ref[bx - 8 + p] = out_ref[bx - 8 + p] + conv0(bx - 8 + p, range(16 - p, 17))

    @pl.loop(0, cx)
    def _(m):
        at = m + 2
        out_ref[2 * m] = out_ref[2 * m] + pr[at]
        out_ref[2 * m + 1] = out_ref[2 * m + 1] + (
            0.5625 * (pr[at] + pr[at + 1]) - 0.0625 * (pr[at - 1] + pr[at + 2])
        )

    for group in (*ya, za, *zf, z2, yp, *xa, hop1, hop2, xb, yb, zb):
        left_over(group)
    for group in (ca, cb, cc):
        for to, _, copy, _ in group:
            pl.when(to)(copy.wait_send)


def per_device(counts, charges, kernel_taps):
    nx, ny, nz = counts
    bx, by, bz = dims = charges.shape
    assert bz == LANES
    cx, cy, cz = bx // 2, by // 2, bz // 2
    fx, fy, fz = bx // 4, by // 4, bz // 4
    n2x, n2y, n2z = nx * fx, ny * fy, nz * fz
    per = LANES // fz
    np2 = fx // per
    half1 = cx // 2
    ry1 = up(cy + 4, 8)
    ty = up(fy + 5, 8)
    V = pltpu.VMEM
    wide = max(nx, ny, nz) * 2
    dma = pltpu.SemaphoreType.DMA
    row = lambda n, r: V((n, r, LANES), F32)
    scratch = [
        pltpu.SMEM(kernel_taps.shape, F32), V(dims, F32),
        row(bx, by), row(bx, by), row(bx, 16), row(bx, 16), row(bx, 16),
        V((bx, by + 16, 2 * LANES), BF16), V((bx, by + 16, 2 * LANES), BF16),
        row(6, by), row(bx + 16, by), row(bx + 16, cy),
        row(half1 + 2, cy), row(6, cy), row(6, cy), row(half1 + 10, cy), row(half1 + 9, cy),
        row(half1 + 2, cy + 32), row(half1 + 2, ry1), row(half1 + 2, ry1), row(half1 + 2, ry1),
        row(cx + 4, ry1), row(cx + 4, by),
        row(bx + 16, fy + 16), row(cx + 15, fy + 16),
        row(fx + 5, fy + 16), row(fx + 5, fy + 16), row(fx + 5, fy + 16),
        row(np2 + 2, fy + 16), row(np2 + 2, 8), row(np2 + 2, 8),
        V((nx, np2 + 2, fy, LANES), F32),
        V((nz, ny, nx * np2, fy, LANES), F32),
        V((nx * np2, n2y, per * LANES), BF16), V((nx * np2, n2y, per * LANES), BF16),
        row(n2x, ty),
        V((2 * bz, bz + LANES), BF16), V((2 * bz, bz + LANES), BF16),
        V((by + cy, 3 * (by + 16)), BF16),
        V((2 * cz, bz), BF16), V((2 * cz, bz), BF16),
        V((ry1, 3 * (cy + 32)), BF16),
        V((nz * LANES, per * LANES), BF16), V((nz * LANES, per * LANES), BF16),
        V((3 * ty, 3 * n2y), BF16),
        row(fx + 5, n2x),
        V((LANES, bz), BF16), V((ry1, 2 * up(ty, 16)), BF16),
        V((by, 2 * up(ry1, 16)), BF16),
        V((fy + 16, 2 * by), BF16), V((2 * bz, LANES), BF16),
        dma((2,)), dma((32,)), dma((32,)), dma((3, wide)), dma((3, wide)),
    ]
    return pl.pallas_call(
        functools.partial(kernel, counts, dims),
        out_shape=jax.ShapeDtypeStruct(dims, F32),
        in_specs=[pl.BlockSpec(memory_space=pltpu.HBM)] * 2,
        out_specs=pl.BlockSpec(memory_space=pltpu.VMEM),
        scratch_shapes=scratch,
        compiler_params=pltpu.CompilerParams(
            collective_id=0, has_side_effects=True, vmem_limit_bytes=105 * 2**19
        ),
    )(kernel_taps, charges)


def solution(mesh):
    counts = tuple(mesh.shape[a] for a in AXES)
    return jax.shard_map(
        functools.partial(per_device, counts), mesh=mesh,
        in_specs=(P("gx", "gy", "gz"), P()), out_specs=P("gx", "gy", "gz"), check_vma=False,
    )
```

```python
import functools

import jax
import jax.numpy as jnp
from jax import lax
from jax.experimental import pallas as pl
from jax.experimental.pallas import tpu as pltpu
from jax.sharding import PartitionSpec as P

F32, BF16 = jnp.float32, jnp.bfloat16
LANES = 128
U0, U1, U2, U3 = 4, 4, 4, 5
AXES = ("gx", "gy", "gz")
ODD = (-0.0625, 0.5625, 0.5625, -0.0625)
SIDES = tuple((a, b) for a in (-1, 0, 1) for b in (-1, 0, 1) if (a, b) != (0, 0))


def split(v):
    hi = v.astype(BF16)
    return hi, (v - hi.astype(F32)).astype(BF16)


def mm(a, b):
    return jnp.dot(a, b, preferred_element_type=F32)


def exact(a, b):
    return jnp.dot(a, b, preferred_element_type=F32, precision=lax.Precision.HIGHEST)


def dot_right(v, w):
    hi, lo = split(v)
    out = mm(hi, w[0][...]) + mm(lo, w[0][...])
    return out if w[1] is None else out + mm(hi, w[1][...])


def dot_left(w_ref, v, terms):
    hi, lo = split(v)
    return mm(w_ref[...], jnp.concatenate([hi, lo, hi][:terms], axis=0))


def grids(rows, cols):
    return (
        lax.broadcasted_iota(jnp.int32, (rows, cols), 0),
        lax.broadcasted_iota(jnp.int32, (rows, cols), 1),
    )


def pick(taps, level, axis, diff, ok):
    out = jnp.zeros(diff.shape, F32)
    for t in range(17):
        out = jnp.where(diff == t, taps[level, axis, t], out)
    return jnp.where(ok, out, 0.0)


def cubic(diff, ok):
    d = jnp.abs(diff)
    out = jnp.where(d == 0, 1.0, jnp.where(d == 1, 0.5625, jnp.where(d == 3, -0.0625, 0.0)))
    return jnp.where(ok, out, 0.0).astype(F32)


def up(n, m):
    return -(-n // m) * m


def inside(v, n):
    return (v >= 0) & (v < n)


def kernel(counts, dims, taps_hbm, x_hbm, out_ref, taps, x_ref, l0, r0, hy, hl, hr, zh, zl, relay, y0, y1, t1, t1l, t1r, e1, sw, f1, h1, h1l, h1r, d1, pr,
           ua, am, v2, v2l, v2r, pq, yu, yd, xg, g2, z2h, z2l, y2,
           w0h, w0l, m0, w1h, w1l, m1, w2h, w2l, m2, c2, pz2, py2, py1, my2, wz2, own_sem, ss, rs, sg, rg):
    nx, ny, nz = counts
    bx, by, bz = dims
    here = tuple(lax.axis_index(a) for a in AXES)
    loads = [
        pltpu.make_async_copy(x_hbm.at[pl.ds(k, bx // 4)], x_ref.at[pl.ds(k, bx // 4)], own_sem.at[4 * k // bx])
        for k in range(0, bx, bx // 4)
    ]
    loads.append(pltpu.make_async_copy(taps_hbm, taps, own_sem.at[4]))
    for load in loads:
        load.start()
    gx, gy, gz = here
    cx, cy, cz = bx // 2, by // 2, bz // 2
    fx, fy, fz = bx // 4, by // 4, bz // 4
    half1 = cx // 2
    per = LANES // fz
    np2 = fx // per

    def there(dx, dy, dz):
        return inside(gx + dx, nx) & inside(gy + dy, ny) & inside(gz + dz, nz)

    partners = []
    for dim, n in enumerate(counts):
        for d in range(1, n):
            for sgn in (-d, d):
                partners.append(tuple(sgn if k == dim else 0 for k in range(3)))
    barrier = pltpu.get_barrier_semaphore()
    total = jnp.int32(0)
    for p in partners:
        ok = there(*p)
        total = total + ok.astype(jnp.int32)

        @pl.when(ok)
        def _(p=p):
            pl.semaphore_signal(
                barrier, inc=1, device_id=(gx + p[0], gy + p[1], gz + p[2]),
                device_id_type=pl.DeviceIdType.MESH,
            )

    def clear(ref, d, *at):
        @pl.when(jnp.logical_not(there(*d)))
        def _():
            view = ref.at[at]
            view[...] = jnp.zeros(view.shape, F32)

    every = slice(None)
    clear(hy, (0, -1, 0), every, pl.ds(0, 8))
    clear(hy, (0, 1, 0), every, pl.ds(8, 8))
    clear(y0, (-1, 0, 0), pl.ds(0, 8))
    clear(y0, (1, 0, 0), pl.ds(8 + bx, 8))
    clear(t1l, (-1, 0, 0), every)
    clear(t1r, (1, 0, 0), every)
    clear(f1, (0, -1, 0), every, pl.ds(0, 16))
    clear(f1, (0, 1, 0), every, pl.ds(16 + cy, 16))
    clear(yu, (0, -1, 0), every)
    clear(yd, (0, 1, 0), every)
    for ref in (ua, y1):
        ref[pl.ds(0, 8)] = jnp.zeros((8,) + ref.shape[1:], F32)
        ref[pl.ds(8 + bx, 8)] = jnp.zeros((8,) + ref.shape[1:], F32)
    am[pl.ds(0, 6)] = jnp.zeros((6,) + am.shape[1:], F32)
    am[pl.ds(cx + 9, 6)] = jnp.zeros((6,) + am.shape[1:], F32)
    right, left, ahead, behind, above, below = (
        (1, 0, 0), (-1, 0, 0), (0, 1, 0), (0, -1, 0), (0, 0, 1), (0, 0, -1)
    )
    def put(h, l, v):
        hi, lo = split(v)
        h[...] = hi
        if l is not None:
            l[...] = lo

    def stack(ref, v, terms):
        hi, lo = split(v)
        ref[...] = jnp.concatenate([hi, hi, lo][:terms], axis=1)

    def twice(pos, at, base, n):
        out = jnp.zeros(pos.shape, F32)
        for k, w in ((-3, -0.0625), (-1, 0.5625), (0, 1.0), (1, 0.5625), (3, -0.0625)):
            m = 2 * at + k
            out = out + w * cubic(pos - 2 * m, inside(base + m, n))
        return out

    def restrict_x(ref, at):
        return (
            ref[at] + 0.5625 * (ref[at - 1] + ref[at + 1]) - 0.0625 * (ref[at - 3] + ref[at + 3])
        )

    lane = lax.broadcasted_iota(jnp.int32, (1, LANES), 1)
    has_r, has_l = there(*above), there(*below)
    mask_r, mask_l = (lane < LANES // 2) & has_r, (lane >= LANES // 2) & has_l
    rows2 = fy + 16
    i, j = grids(rows2, by)
    stack(my2, twice(j, jnp.where(i < fy + 8, i, i - rows2), gy * cy, ny * cy), 2)
    i, j = grids(2 * bz, LANES)
    pos = jnp.where(i < bz + bz // 2, i, i - 2 * bz)
    put(wz2, None, jnp.where(j < fz, twice(pos, j, gz * cz, nz * cz), 0.0))


    for k in range(4):
        loads[k].wait()
        for c in range(k * (bx // 8), (k + 1) * (bx // 8)):
            o = dot_left(my2, jnp.concatenate([x_ref[2 * c], x_ref[2 * c + 1]], axis=1), 2)
            ua[8 + 2 * c] = o[:, :LANES]
            ua[9 + 2 * c] = o[:, LANES:]

    for m in range(-1, cx + 2):
        am[m + 7] = restrict_x(ua, 8 + 2 * m) * inside(gx * cx + m, nx * cx).astype(F32)
    for e in range(fx + 5):
        v2[e] = restrict_x(am, 3 + 2 * e)
    pl.semaphore_wait(barrier, total)

    count = [0]

    def remote(src, dst, d, to=None, fro=None):
        k = count[0]
        count[0] += 1
        copy = pltpu.make_async_remote_copy(
            src_ref=src, dst_ref=dst, send_sem=ss.at[k], recv_sem=rs.at[k],
            device_id=(gx + d[0], gy + d[1], gz + d[2]), device_id_type=pl.DeviceIdType.MESH,
        )
        to = there(*d) if to is None else to
        fro = there(-d[0], -d[1], -d[2]) if fro is None else fro
        return to, fro, copy

    def start(copies):
        for to, _, copy in copies:
            pl.when(to)(copy.start)

    def arrive(copies):
        for _, fro, copy in copies:
            pl.when(fro)(copy.wait_recv)

    def left_over(copies):
        for to, _, copy in copies:
            pl.when(to)(copy.wait_send)

    ends = (pl.ds(0, 8), pl.ds(bx - 8, 8)), (pl.ds(8, bx - 16),)
    ya, zf = [], []
    for xs in ends:
        ya.append([
            remote(x_ref.at[x, pl.ds(by - 8, 8)], hy.at[x, pl.ds(0, 8)], ahead) for x in xs
        ] + [
            remote(x_ref.at[x, pl.ds(0, 8)], hy.at[x, pl.ds(8, 8)], behind) for x in xs
        ])
        zf.append([remote(hy.at[x], hl.at[x], above) for x in xs] + [remote(hy.at[x], hr.at[x], below) for x in xs])
    za = [remote(x_ref, l0, above), remote(x_ref, r0, below)]
    z2 = [remote(v2, v2l, above), remote(v2, v2r, below)]
    yp = [
        remote(pq.at[:, pl.ds(fy, 8)], yu, ahead),
        remote(pq.at[:, pl.ds(fy + 8, 8)], yd, behind),
    ]
    mid_l, mid_r = (gx == 1, gx == 2) if nx == 4 else (jnp.bool_(False), jnp.bool_(False))
    end_l, end_r = (gx == 0, gx == 3) if nx == 4 else (jnp.bool_(False), jnp.bool_(False))
    near, rest = 3, 5

    def to_left(k, n, **ok):
        return remote(y0.at[pl.ds(8 + k, n)], y0.at[pl.ds(8 + bx + k, n)], left, **ok)

    def to_right(k, n, **ok):
        return remote(y0.at[pl.ds(bx + k, n)], y0.at[pl.ds(k, n)], right, **ok)

    xa = [
        [to_left(0, 1), to_right(0, 1)],
        [
            to_left(1, near - 1),
            to_left(near, rest, to=there(*left) & jnp.logical_not(mid_r), fro=there(*right) & jnp.logical_not(mid_l)),
            to_right(1, near - 1),
            to_right(near, rest, to=there(*right) & jnp.logical_not(mid_l), fro=there(*left) & jnp.logical_not(mid_r)),
        ],
    ]
    hop1, hop2 = [], []
    if nx == 4:
        hop1 = [
            remote(y0.at[pl.ds(bx + near, rest)], relay, (2, 0, 0), to=mid_l, fro=end_r),
            remote(y0.at[pl.ds(8 + near, rest)], relay, (-2, 0, 0), to=mid_r, fro=end_l),
        ]
        hop2 = [
            remote(relay, y0.at[pl.ds(near, rest)], left, to=end_r, fro=mid_r),
            remote(relay, y0.at[pl.ds(8 + bx + near, rest)], right, to=end_l, fro=mid_l),
        ]
    xb = [remote(t1.at[pl.ds(0, 6)], t1r, left), remote(t1.at[pl.ds(half1 - 4, 6)], t1l, right)]
    yb = [
        remote(f1.at[:, pl.ds(cy, 16)], f1.at[:, pl.ds(0, 16)], ahead),
        remote(f1.at[:, pl.ds(16, 16)], f1.at[:, pl.ds(16 + cy, 16)], behind),
    ]
    zb = [remote(h1, h1l, above), remote(h1, h1r, below)]
    start(z2)
    start(ya[0])
    start(za)
    loads[4].wait()
    i, j = grids(2 * bz, bz)
    pos = jnp.where(i < bz + bz // 2, i, i - 2 * bz)
    k0 = pick(taps, 0, 2, pos - j + 8, inside(pos, bz + 8) | inside(pos + 8, 8))
    rz = cubic(pos - 2 * j, j < cz)
    put(w0h, w0l, jnp.concatenate([k0, rz], axis=1))
    i, j = grids(by + cy, by + 16)
    j = jnp.where(j < by, j + 8, jnp.where(j < by + 8, j - by, j))
    stack(m0, jnp.where(i < by, pick(taps, 0, 1, j - i, i < by), cubic(j - 8 - 2 * (i - by), i >= by)), 3)

    i, j = grids(2 * cz, LANES)
    pos = jnp.where(i < cz + cz // 2, i, i - 2 * cz)
    kk = j - 2
    top = cz + 4
    ok = (j < top) & inside(gz * cz + kk, nz * cz)
    k1 = pick(taps, 1, 2, pos - kk + 8, ok)
    i, j = grids(LANES, bz)
    fine_z = cubic(j - 2 * (i - 2), i < top)
    put(w1h, w1l, exact(k1, fine_z))
    ry1 = up(cy + 4, 8)
    i, j = grids(ry1, cy + 32)
    ok = (i < cy + 4) & inside(gy * cy + i - 2, ny * cy)
    stack(m1, pick(taps, 1, 1, j - 16 - (i - 2) + 8, ok), 3)
    i, j = grids(by, up(ry1, 16))
    stack(py1, cubic(i - 2 * (j - 2), j < cy + 4), 2)

    arrive(z2)
    parts = []
    for e in range(fx + 5):
        other = jnp.where(mask_r, v2r[e], jnp.where(mask_l, v2l[e], 0.0))
        parts.append(jnp.concatenate([v2[e], other], axis=1))
    v = dot_right(jnp.concatenate(parts, axis=0), (wz2, None))
    for g in range(np2 + 2):
        acc = None
        for s in range(per):
            e = per * (g - 1) + s + 2
            if 0 <= e < fx + 5:
                w = v[e * rows2:(e + 1) * rows2]
                w = pltpu.roll(w, fz * s, 1) if s else w
                acc = w if acc is None else acc + w
        pq[g] = acc
    start(yp)

    start(ya[1])
    arrive(ya[0])
    start(zf[0])
    step0 = 4

    def across(own, lo, hi):
        rows = own.shape[0] * own.shape[1]
        other = jnp.where(
            mask_r, hi.reshape(rows, LANES), jnp.where(mask_l, lo.reshape(rows, LANES), 0.0)
        )
        v = jnp.concatenate([own.reshape(rows, LANES), other], axis=1)
        return split(dot_right(v, (w0h, w0l)))

    def level0_own(c):
        at = pl.ds(c * step0, step0)
        hi, lo = across(x_ref[at], l0[at], r0[at])
        zh[at, pl.ds(0, by), :] = hi.reshape(step0, by, 2 * LANES)
        zl[at, pl.ds(0, by), :] = lo.reshape(step0, by, 2 * LANES)

    def level0_halo(x, n):
        at = pl.ds(x, n)
        hi, lo = across(hy[at], hl[at], hr[at])
        zh[at, pl.ds(by, 16), :] = hi.reshape(n, 16, 2 * LANES)
        zl[at, pl.ds(by, 16), :] = lo.reshape(n, 16, 2 * LANES)

    def level0(k):
        hi = zh[k]
        o = mm(m0[...], jnp.concatenate([hi, zl[k], hi], axis=0))
        y0[8 + k] = o[:by, :LANES]
        y1[8 + k] = o[by:, LANES:]

    arrive(za)
    edge = 8 // step0
    for c in range(edge):
        level0_own(c)
        level0_own(bx // step0 - edge + c)
    def spread(dim, n, ref, k0):
        out = []
        for m, d in enumerate([d for d in range(-(n - 1), n) if d]):
            dev = tuple(here[k] + (d if k == dim else 0) for k in range(3))
            copy = pltpu.make_async_remote_copy(
                src_ref=ref(here[dim]), dst_ref=ref(here[dim]),
                send_sem=sg.at[dim, m], recv_sem=rg.at[dim, m],
                device_id=dev, device_id_type=pl.DeviceIdType.MESH,
            )
            land = pltpu.make_async_remote_copy(
                src_ref=ref(here[dim]), dst_ref=ref(here[dim] - d),
                send_sem=sg.at[dim, m], recv_sem=rg.at[dim, m],
                device_id=dev, device_id_type=pl.DeviceIdType.MESH,
            )
            to = inside(here[dim] + d, n)
            fro = inside(here[dim] - d, n)
            out.append((to, fro, copy, land))
        return out

    def begin(copies):
        for to, _, copy, _ in copies:
            pl.when(to)(copy.start)

    def landed(copies):
        for _, fro, _, land in copies:
            pl.when(fro)(land.wait_recv)

    arrive(yp)
    own = [pq[:, pl.ds(0, 8)] + yu[...]]
    if fy > 16:
        own.append(pq[:, pl.ds(8, fy - 16)])
    own.append(pq[:, pl.ds(fy - 8, 8)] + yd[...])
    xg[gx] = jnp.concatenate(own, axis=1)
    ca = spread(0, nx, lambda k: xg.at[k], 0)
    begin(ca)


    pl.loop(edge, bx // step0 - edge, unroll=4)(level0_own)
    arrive(ya[1])
    start(zf[1])
    arrive(zf[0])
    level0_halo(0, 8)
    level0_halo(bx - 8, 8)
    for k in range(8):
        level0(k)
        level0(bx - 8 + k)
    start(xa[0])
    start(hop1)
    arrive(zf[1])
    level0_halo(8, bx - 16)
    pl.loop(8, bx - 8, unroll=8)(level0)

    for p in range(half1 + 2):
        a = restrict_x(y1, 4 + 4 * p)
        b = restrict_x(y1, 6 + 4 * p)
        t1[p] = jnp.where(lane < cz, a, pltpu.roll(b, cz, 1))
    start(xb)
    start(xa[1])

    landed(ca)
    for m in range(np2 * nx):
        acc = None
        for b in range(nx):
            k = m - np2 * b + 1
            if 0 <= k < np2 + 2:
                acc = xg[b, k] if acc is None else acc + xg[b, k]
        g2[gz, gy, m] = acc
    cb = spread(1, ny, lambda k: g2.at[gz, k], 0)
    begin(cb)

    def conv0(p, ts):
        acc = None
        for t in ts:
            v = taps[0, 0, t] * y0[p + t]
            acc = v if acc is None else acc + v
        return acc

    @pl.loop(8, bx - 8)
    def _(p):
        out_ref[p] = conv0(p, range(17))

    def plain(axis, level, n, pad, turned):
        i, j = grids(pad, pad)
        d = (i - j if turned else j - i) + 8
        return pick(taps, level, axis, d, (i < n) & (j < n))

    def rest(n, pad, big, turned_r):
        i, j = grids(*((big, pad) if turned_r else (pad, big)))
        c, f = (j, i) if turned_r else (i, j)
        return cubic(f - 2 * c, (c < n) & (f < 2 * n))

    def operators(axis, n2, first, rows, count):
        n3, n4 = n2 // 2, n2 // 4
        q = up(n2, LANES)
        i, j = grids(rows, q)
        g = first + i
        ok = (i < count) & inside(g, n2)
        one = pick(taps, 2, axis, j - g + 8, ok & (j < n2))
        pr = cubic(g - 2 * j, ok & (j < n3))
        r23, r34 = rest(n3, q, q, False), rest(n4, q, q, False)
        p34 = rest(n4, q, q, True)
        two = exact(exact(pr, plain(axis, 3, n3, q, False)), r23)
        three = exact(exact(exact(exact(pr, p34), plain(axis, 4, n4, q, False)), r34), r23)
        return one, two, three

    n2x, n2y, n2z = nx * fx, ny * fy, nz * fz
    ez, ey, ex = fz + 5, fy + 5, fx + 5
    tz = 40
    ops = operators(2, n2z, gz * fz - 2, tz, ez)
    cols = jnp.concatenate(list(ops) + [jnp.zeros((LANES - 3 * tz, ops[0].shape[1]), F32)], axis=0)
    hi, lo = split(cols.T)
    for ref, v in ((w2h, hi), (w2l, lo)):
        ref[...] = jnp.zeros(ref.shape, BF16)
        for b in range(nz):
            for k in range(per):
                ref[pl.ds(b * LANES + k * fz, fz), pl.ds(k * LANES, LANES)] = v[b * fz:(b + 1) * fz]
    ty = up(ey, 8)
    ops = operators(1, n2y, gy * fy - 2, ty, ey)
    stack(m2, jnp.concatenate(list(ops), axis=0)[:, :n2y], 3)
    tx = up(ex, 8)
    ops = operators(0, n2x, gx * fx - 2, tx, ex)
    tall = [o.T for o in ops]
    for r in range(ex):
        a, b, c = (o[:n2x, r:r + 1] for o in tall)
        c2[r] = jnp.where(lane < tz, a, jnp.where(lane < 2 * tz, b, c))
    i, j = grids(LANES, LANES)
    src = i - jnp.where(i < tz, 0, jnp.where(i < 2 * tz, tz, 2 * tz)) - 2
    e1_z = cubic((j - 2) - 2 * src, (i < 3 * tz) & (src < fz + 3) & (j < top) & inside(gz * cz + j - 2, nz * cz))
    put(pz2, None, exact(e1_z, fine_z))
    i, j = grids(ry1, up(ty, 16))
    stack(py2, cubic((i - 2) - 2 * (j - 2), (j < ey) & (i < cy + 4) & inside(gy * cy + i - 2, ny * cy)), 2)
    for p in range(8):
        out_ref[p] = conv0(p, range(8 - p, 17))
        out_ref[bx - 8 + p] = conv0(bx - 8 + p, range(16 - p))
    arrive(hop1)
    start(hop2)
    arrive(xb)
    n1 = half1 + 10
    to_l, to_r = there(*left).astype(F32), there(*right).astype(F32)
    for k in range(n1):
        if k < 4:
            v = t1l[k]
        elif k < 6:
            v = t1l[k] + (t1[k - 4] * to_l if k == 4 else t1[k - 4])
        elif k < half1 + 4:
            v = t1[k - 4]
        elif k < half1 + 6:
            v = t1r[k - half1 - 4] + (t1[k - 4] * to_r if k == half1 + 5 else t1[k - 4])
        else:
            v = t1r[k - half1 - 4]
        e1[k] = v
        back = pltpu.roll(v, cz, 1)
        if k:
            sw[k - 1] = jnp.where(lane < cz, last, back)
        last = back

    @pl.loop(0, half1 + 2)
    def _(q):
        acc = taps[1, 0, 0] * e1[q]
        for t in range(1, 17):
            acc = acc + taps[1, 0, t] * (sw[q + (t - 1) // 2] if t % 2 else e1[q + t // 2])
        f1[q, pl.ds(16, cy), :] = acc

    start(yb)
    landed(cb)
    cc = spread(2, nz, lambda k: g2.at[k], 0)
    begin(cc)
    landed(cc)
    seen = lambda r: inside(gx * cx + r - 2, nx * cx).astype(F32)
    batch = max(1, min(nx * np2, 256 // n2y))
    for m in range(0, nx * np2, batch):
        v = jnp.concatenate([
            jnp.concatenate([g2[b, :, k].reshape(n2y, LANES) for b in range(nz)], axis=1)
            for k in range(m, m + batch)
        ], axis=0)
        hi, lo = split(dot_right(v, (w2h, w2l)))
        z2h[pl.ds(m, batch)] = hi.reshape(batch, n2y, per * LANES)
        z2l[pl.ds(m, batch)] = lo.reshape(batch, n2y, per * LANES)

    @pl.loop(0, nx * np2, unroll=4)
    def _(m):
        hi = z2h[m]
        o = mm(m2[...], jnp.concatenate([hi, z2l[m], hi], axis=0))
        for k in range(per):
            w = o[:, k * LANES:(k + 1) * LANES]
            y2[per * m + k] = jnp.where(
                lane < tz, w[:ty], jnp.where(lane < 2 * tz, w[ty:2 * ty], w[2 * ty:])
            )

    arrive(yb)
    for q in range(0, half1 + 2, 2):
        o = dot_left(m1, jnp.concatenate([f1[q], f1[q + 1]], axis=1), 3)
        h1[q] = o[:, :LANES]
        h1[q + 1] = o[:, LANES:]
    start(zb)
    parts = []
    for r in range(ex):
        acc = c2[r, pl.ds(0, 1)] * y2[0]
        for q in range(1, n2x):
            acc = acc + c2[r, pl.ds(q, 1)] * y2[q]
        parts.append(acc)
    v = dot_right(jnp.concatenate(parts, axis=0), (pz2, None))
    fill = up(ty, 16) - ty
    pro = []
    for r in range(ex):
        w = v[r * ty:(r + 1) * ty]
        if fill:
            w = jnp.concatenate([w, jnp.zeros((fill, LANES), F32)], axis=0)
        pro.append(dot_left(py2, w, 2))
    arrive(zb)
    inner = lax.rem(lane, cz) < cz // 2
    step1 = 5 if (half1 + 2) % 5 == 0 else 1
    for c in range(0, half1 + 2, step1):
        parts = []
        for q in range(c, c + step1):
            own = h1[q]
            other = jnp.where(inner & has_r, h1r[q], jnp.where(jnp.logical_not(inner) & has_l, h1l[q], 0.0))
            parts.append(jnp.where(lane < cz, own, pltpu.roll(other, cz, 1)))
            parts.append(jnp.where(lane < cz, pltpu.roll(own, cz, 1), other))
        v = dot_right(jnp.concatenate(parts, axis=0), (w1h, w1l))
        for k in range(2 * step1):
            d1[2 * c + k] = v[k * ry1:(k + 1) * ry1]
    for p in range(cx + 4):
        m = (p - 2) // 2 + 2
        if p % 2 == 0:
            w = pro[m]
        else:
            w = 0.5625 * (pro[m] + pro[m + 1]) - 0.0625 * (pro[m - 1] + pro[m + 2])
        d1[p] = (d1[p] + w) * seen(p)

    fill1 = up(ry1, 16) - ry1

    @pl.loop(0, (cx + 4) // 2, unroll=5)
    def _(c):
        v = jnp.concatenate([d1[2 * c], d1[2 * c + 1]], axis=1)
        if fill1:
            v = jnp.concatenate([v, jnp.zeros((fill1, 2 * LANES), F32)], axis=0)
        o = dot_left(py1, v, 2)
        pr[2 * c] = o[:, :LANES]
        pr[2 * c + 1] = o[:, LANES:]

    for group in (*xa, hop2):
        arrive(group)
    for p in range(8):
        out_ref[p] = out_ref[p] + conv0(p, range(8 - p))
        out_ref[bx - 8 + p] = out_ref[bx - 8 + p] + conv0(bx - 8 + p, range(16 - p, 17))

    @pl.loop(0, cx)
    def _(m):
        at = m + 2
        out_ref[2 * m] = out_ref[2 * m] + pr[at]
        out_ref[2 * m + 1] = out_ref[2 * m + 1] + (
            0.5625 * (pr[at] + pr[at + 1]) - 0.0625 * (pr[at - 1] + pr[at + 2])
        )

    for group in (*ya, za, *zf, z2, yp, *xa, hop1, hop2, xb, yb, zb):
        left_over(group)
    for group in (ca, cb, cc):
        for to, _, copy, _ in group:
            pl.when(to)(copy.wait_send)


def per_device(counts, charges, kernel_taps):
    nx, ny, nz = counts
    bx, by, bz = dims = charges.shape
    assert bz == LANES
    cx, cy, cz = bx // 2, by // 2, bz // 2
    fx, fy, fz = bx // 4, by // 4, bz // 4
    n2x, n2y, n2z = nx * fx, ny * fy, nz * fz
    per = LANES // fz
    np2 = fx // per
    half1 = cx // 2
    ry1 = up(cy + 4, 8)
    ty = up(fy + 5, 8)
    V = pltpu.VMEM
    wide = max(nx, ny, nz) * 2
    dma = pltpu.SemaphoreType.DMA
    row = lambda n, r: V((n, r, LANES), F32)
    scratch = [
        pltpu.SMEM(kernel_taps.shape, F32), V(dims, F32),
        row(bx, by), row(bx, by), row(bx, 16), row(bx, 16), row(bx, 16),
        V((bx, by + 16, 2 * LANES), BF16), V((bx, by + 16, 2 * LANES), BF16),
        row(5, by), row(bx + 16, by), row(bx + 16, cy),
        row(half1 + 2, cy), row(6, cy), row(6, cy), row(half1 + 10, cy), row(half1 + 9, cy),
        row(half1 + 2, cy + 32), row(half1 + 2, ry1), row(half1 + 2, ry1), row(half1 + 2, ry1),
        row(cx + 4, ry1), row(cx + 4, by),
        row(bx + 16, fy + 16), row(cx + 15, fy + 16),
        row(fx + 5, fy + 16), row(fx + 5, fy + 16), row(fx + 5, fy + 16),
        row(np2 + 2, fy + 16), row(np2 + 2, 8), row(np2 + 2, 8),
        V((nx, np2 + 2, fy, LANES), F32),
        V((nz, ny, nx * np2, fy, LANES), F32),
        V((nx * np2, n2y, per * LANES), BF16), V((nx * np2, n2y, per * LANES), BF16),
        row(n2x, ty),
        V((2 * bz, bz + LANES), BF16), V((2 * bz, bz + LANES), BF16),
        V((by + cy, 3 * (by + 16)), BF16),
        V((2 * cz, bz), BF16), V((2 * cz, bz), BF16),
        V((ry1, 3 * (cy + 32)), BF16),
        V((nz * LANES, per * LANES), BF16), V((nz * LANES, per * LANES), BF16),
        V((3 * ty, 3 * n2y), BF16),
        row(fx + 5, n2x),
        V((LANES, bz), BF16), V((ry1, 2 * up(ty, 16)), BF16),
        V((by, 2 * up(ry1, 16)), BF16),
        V((fy + 16, 2 * by), BF16), V((2 * bz, LANES), BF16),
        dma((5,)), dma((40,)), dma((40,)), dma((3, wide)), dma((3, wide)),
    ]
    return pl.pallas_call(
        functools.partial(kernel, counts, dims),
        out_shape=jax.ShapeDtypeStruct(dims, F32),
        in_specs=[pl.BlockSpec(memory_space=pltpu.HBM)] * 2,
        out_specs=pl.BlockSpec(memory_space=pltpu.VMEM),
        scratch_shapes=scratch,
        compiler_params=pltpu.CompilerParams(
            collective_id=0, has_side_effects=True, vmem_limit_bytes=105 * 2**19
        ),
    )(pltpu.with_memory_space_constraint(kernel_taps, pltpu.HBM), charges)


def solution(mesh):
    counts = tuple(mesh.shape[a] for a in AXES)
    return jax.shard_map(
        functools.partial(per_device, counts), mesh=mesh,
        in_specs=(P("gx", "gy", "gz"), P()), out_specs=P("gx", "gy", "gz"), check_vma=False,
    )
```

```python
import functools

import jax
import jax.numpy as jnp
from jax import lax
from jax.experimental import pallas as pl
from jax.experimental.pallas import tpu as pltpu
from jax.sharding import PartitionSpec as P

F32, BF16 = jnp.float32, jnp.bfloat16
LANES = 128
U0, U1, U2, U3 = 4, 4, 4, 5
AXES = ("gx", "gy", "gz")
ODD = (-0.0625, 0.5625, 0.5625, -0.0625)
SIDES = tuple((a, b) for a in (-1, 0, 1) for b in (-1, 0, 1) if (a, b) != (0, 0))


def split(v):
    hi = v.astype(BF16)
    return hi, (v - hi.astype(F32)).astype(BF16)


def mm(a, b):
    return jnp.dot(a, b, preferred_element_type=F32)


def exact(a, b):
    return jnp.dot(a, b, preferred_element_type=F32, precision=lax.Precision.HIGHEST)


def dot_right(v, w):
    hi, lo = split(v)
    out = mm(hi, w[0][...]) + mm(lo, w[0][...])
    return out if w[1] is None else out + mm(hi, w[1][...])


def dot_left(w_ref, v, terms):
    hi, lo = split(v)
    return mm(w_ref[...], jnp.concatenate([hi, lo, hi][:terms], axis=0))


def grids(rows, cols):
    return (
        lax.broadcasted_iota(jnp.int32, (rows, cols), 0),
        lax.broadcasted_iota(jnp.int32, (rows, cols), 1),
    )


def pick(taps, level, axis, diff, ok):
    out = jnp.zeros(diff.shape, F32)
    for t in range(17):
        out = jnp.where(diff == t, taps[level, axis, t], out)
    return jnp.where(ok, out, 0.0)


def cubic(diff, ok):
    d = jnp.abs(diff)
    out = jnp.where(d == 0, 1.0, jnp.where(d == 1, 0.5625, jnp.where(d == 3, -0.0625, 0.0)))
    return jnp.where(ok, out, 0.0).astype(F32)


def up(n, m):
    return -(-n // m) * m


def inside(v, n):
    return (v >= 0) & (v < n)


def kernel(counts, dims, taps_hbm, x_hbm, out_ref, taps, x_ref, l0, r0, hy, hl, hr, zh, zl, relay, y0, y1, t1, t1l, t1r, e1, sw, f1, h1, h1l, h1r, d1, pr,
           ua, am, v2, v2l, v2r, pq, yu, yd, xg, g2, z2h, z2l, y2,
           w0h, w0l, m0, w1h, w1l, m1, w2h, w2l, m2, c2, pz2, py2, py1, my2, wz2, own_sem, ss, rs, sg, rg):
    nx, ny, nz = counts
    bx, by, bz = dims
    here = tuple(lax.axis_index(a) for a in AXES)
    loads = [
        pltpu.make_async_copy(x_hbm.at[pl.ds(k, bx // 4)], x_ref.at[pl.ds(k, bx // 4)], own_sem.at[4 * k // bx])
        for k in range(0, bx, bx // 4)
    ]
    loads.append(pltpu.make_async_copy(taps_hbm, taps, own_sem.at[4]))
    for load in loads:
        load.start()
    gx, gy, gz = here
    cx, cy, cz = bx // 2, by // 2, bz // 2
    fx, fy, fz = bx // 4, by // 4, bz // 4
    half1 = cx // 2
    per = LANES // fz
    np2 = fx // per

    def there(dx, dy, dz):
        return inside(gx + dx, nx) & inside(gy + dy, ny) & inside(gz + dz, nz)

    partners = []
    for dim, n in enumerate(counts):
        for d in range(1, n):
            for sgn in (-d, d):
                partners.append(tuple(sgn if k == dim else 0 for k in range(3)))
    barrier = pltpu.get_barrier_semaphore()
    total = jnp.int32(0)
    for p in partners:
        ok = there(*p)
        total = total + ok.astype(jnp.int32)

        @pl.when(ok)
        def _(p=p):
            pl.semaphore_signal(
                barrier, inc=1, device_id=(gx + p[0], gy + p[1], gz + p[2]),
                device_id_type=pl.DeviceIdType.MESH,
            )

    def clear(ref, d, *at):
        @pl.when(jnp.logical_not(there(*d)))
        def _():
            view = ref.at[at]
            view[...] = jnp.zeros(view.shape, F32)

    every = slice(None)
    clear(hy, (0, -1, 0), every, pl.ds(0, 8))
    clear(hy, (0, 1, 0), every, pl.ds(8, 8))
    clear(y0, (-1, 0, 0), pl.ds(0, 8))
    clear(y0, (1, 0, 0), pl.ds(8 + bx, 8))
    clear(t1l, (-1, 0, 0), every)
    clear(t1r, (1, 0, 0), every)
    clear(f1, (0, -1, 0), every, pl.ds(0, 16))
    clear(f1, (0, 1, 0), every, pl.ds(16 + cy, 16))
    clear(yu, (0, -1, 0), every)
    clear(yd, (0, 1, 0), every)
    f1[:, pl.ds(0, 6)] = jnp.zeros((half1 + 2, 6, LANES), F32)
    f1[:, pl.ds(cy + 26, 6)] = jnp.zeros((half1 + 2, 6, LANES), F32)
    for ref in (ua, y1):
        ref[pl.ds(0, 8)] = jnp.zeros((8,) + ref.shape[1:], F32)
        ref[pl.ds(8 + bx, 8)] = jnp.zeros((8,) + ref.shape[1:], F32)
    am[pl.ds(0, 6)] = jnp.zeros((6,) + am.shape[1:], F32)
    am[pl.ds(cx + 9, 6)] = jnp.zeros((6,) + am.shape[1:], F32)
    right, left, ahead, behind, above, below = (
        (1, 0, 0), (-1, 0, 0), (0, 1, 0), (0, -1, 0), (0, 0, 1), (0, 0, -1)
    )
    def put(h, l, v):
        hi, lo = split(v)
        h[...] = hi
        if l is not None:
            l[...] = lo

    def stack(ref, v, terms):
        hi, lo = split(v)
        ref[...] = jnp.concatenate([hi, hi, lo][:terms], axis=1)

    def twice(pos, at, base, n):
        out = jnp.zeros(pos.shape, F32)
        for k, w in ((-3, -0.0625), (-1, 0.5625), (0, 1.0), (1, 0.5625), (3, -0.0625)):
            m = 2 * at + k
            out = out + w * cubic(pos - 2 * m, inside(base + m, n))
        return out

    def restrict_x(ref, at):
        return (
            ref[at] + 0.5625 * (ref[at - 1] + ref[at + 1]) - 0.0625 * (ref[at - 3] + ref[at + 3])
        )

    lane = lax.broadcasted_iota(jnp.int32, (1, LANES), 1)
    has_r, has_l = there(*above), there(*below)
    mask_r, mask_l = (lane < LANES // 2) & has_r, (lane >= LANES // 2) & has_l
    rows2 = fy + 16
    i, j = grids(rows2, by)
    stack(my2, twice(j, jnp.where(i < fy + 8, i, i - rows2), gy * cy, ny * cy), 2)
    i, j = grids(2 * bz, LANES)
    pos = jnp.where(i < bz + bz // 2, i, i - 2 * bz)
    put(wz2, None, jnp.where(j < fz, twice(pos, j, gz * cz, nz * cz), 0.0))


    for k in range(4):
        loads[k].wait()
        for c in range(k * (bx // 8), (k + 1) * (bx // 8)):
            o = dot_left(my2, jnp.concatenate([x_ref[2 * c], x_ref[2 * c + 1]], axis=1), 2)
            ua[8 + 2 * c] = o[:, :LANES]
            ua[9 + 2 * c] = o[:, LANES:]

    for m in range(-1, cx + 2):
        am[m + 7] = restrict_x(ua, 8 + 2 * m) * inside(gx * cx + m, nx * cx).astype(F32)
    for e in range(fx + 5):
        v2[e] = restrict_x(am, 3 + 2 * e)
    pl.semaphore_wait(barrier, total)

    count = [0]

    def remote(src, dst, d, to=None, fro=None):
        k = count[0]
        count[0] += 1
        copy = pltpu.make_async_remote_copy(
            src_ref=src, dst_ref=dst, send_sem=ss.at[k], recv_sem=rs.at[k],
            device_id=(gx + d[0], gy + d[1], gz + d[2]), device_id_type=pl.DeviceIdType.MESH,
        )
        to = there(*d) if to is None else to
        fro = there(-d[0], -d[1], -d[2]) if fro is None else fro
        return to, fro, copy

    def start(copies):
        for to, _, copy in copies:
            pl.when(to)(copy.start)

    def arrive(copies):
        for _, fro, copy in copies:
            pl.when(fro)(copy.wait_recv)

    def left_over(copies):
        for to, _, copy in copies:
            pl.when(to)(copy.wait_send)

    ends = (pl.ds(0, 8), pl.ds(bx - 8, 8)), (pl.ds(8, bx - 16),)
    ya, zf = [], []
    for xs in ends:
        ya.append([
            remote(x_ref.at[x, pl.ds(by - 8, 8)], hy.at[x, pl.ds(0, 8)], ahead) for x in xs
        ] + [
            remote(x_ref.at[x, pl.ds(0, 8)], hy.at[x, pl.ds(8, 8)], behind) for x in xs
        ])
        zf.append([remote(hy.at[x], hl.at[x], above) for x in xs] + [remote(hy.at[x], hr.at[x], below) for x in xs])
    za = [remote(x_ref, l0, above), remote(x_ref, r0, below)]
    z2 = [remote(v2, v2l, above), remote(v2, v2r, below)]
    yp = [
        remote(pq.at[:, pl.ds(fy, 8)], yu, ahead),
        remote(pq.at[:, pl.ds(fy + 8, 8)], yd, behind),
    ]
    mid_l, mid_r = (gx == 1, gx == 2) if nx == 4 else (jnp.bool_(False), jnp.bool_(False))
    end_l, end_r = (gx == 0, gx == 3) if nx == 4 else (jnp.bool_(False), jnp.bool_(False))
    near, rest = 3, 5

    def to_left(k, n, **ok):
        return remote(y0.at[pl.ds(8 + k, n)], y0.at[pl.ds(8 + bx + k, n)], left, **ok)

    def to_right(k, n, **ok):
        return remote(y0.at[pl.ds(bx + k, n)], y0.at[pl.ds(k, n)], right, **ok)

    xa = [
        [to_left(0, 1), to_right(0, 1)],
        [
            to_left(1, near - 1),
            to_left(near, rest, to=there(*left) & jnp.logical_not(mid_r), fro=there(*right) & jnp.logical_not(mid_l)),
            to_right(1, near - 1),
            to_right(near, rest, to=there(*right) & jnp.logical_not(mid_l), fro=there(*left) & jnp.logical_not(mid_r)),
        ],
    ]
    hop1, hop2 = [], []
    if nx == 4:
        hop1 = [
            remote(y0.at[pl.ds(bx + near, rest)], relay, (2, 0, 0), to=mid_l, fro=end_r),
            remote(y0.at[pl.ds(8 + near, rest)], relay, (-2, 0, 0), to=mid_r, fro=end_l),
        ]
        hop2 = [
            remote(relay, y0.at[pl.ds(near, rest)], left, to=end_r, fro=mid_r),
            remote(relay, y0.at[pl.ds(8 + bx + near, rest)], right, to=end_l, fro=mid_l),
        ]
    xb = [remote(t1.at[pl.ds(0, 6)], t1r, left), remote(t1.at[pl.ds(half1 - 4, 6)], t1l, right)]
    yb = [
        remote(f1.at[:, pl.ds(cy + 6, 10)], f1.at[:, pl.ds(6, 10)], ahead),
        remote(f1.at[:, pl.ds(16, 10)], f1.at[:, pl.ds(16 + cy, 10)], behind),
    ]
    zb = [remote(h1, h1l, above), remote(h1, h1r, below)]
    start(z2)
    start(ya[0])
    start(za)
    loads[4].wait()
    i, j = grids(2 * bz, bz)
    pos = jnp.where(i < bz + bz // 2, i, i - 2 * bz)
    k0 = pick(taps, 0, 2, pos - j + 8, inside(pos, bz + 8) | inside(pos + 8, 8))
    rz = cubic(pos - 2 * j, j < cz)
    put(w0h, w0l, jnp.concatenate([k0, rz], axis=1))
    i, j = grids(by + cy, by + 16)
    j = jnp.where(j < by, j + 8, jnp.where(j < by + 8, j - by, j))
    stack(m0, jnp.where(i < by, pick(taps, 0, 1, j - i, i < by), cubic(j - 8 - 2 * (i - by), i >= by)), 3)

    i, j = grids(2 * cz, LANES)
    pos = jnp.where(i < cz + cz // 2, i, i - 2 * cz)
    kk = j - 2
    top = cz + 4
    ok = (j < top) & inside(gz * cz + kk, nz * cz)
    k1 = pick(taps, 1, 2, pos - kk + 8, ok)
    i, j = grids(LANES, bz)
    fine_z = cubic(j - 2 * (i - 2), i < top)
    put(w1h, w1l, exact(k1, fine_z))
    ry1 = up(cy + 4, 8)
    i, j = grids(ry1, cy + 32)
    ok = (i < cy + 4) & inside(gy * cy + i - 2, ny * cy)
    stack(m1, pick(taps, 1, 1, j - 16 - (i - 2) + 8, ok), 3)
    i, j = grids(by, up(ry1, 16))
    stack(py1, cubic(i - 2 * (j - 2), j < cy + 4), 2)

    arrive(z2)
    parts = []
    for e in range(fx + 5):
        other = jnp.where(mask_r, v2r[e], jnp.where(mask_l, v2l[e], 0.0))
        parts.append(jnp.concatenate([v2[e], other], axis=1))
    v = dot_right(jnp.concatenate(parts, axis=0), (wz2, None))
    for g in range(np2 + 2):
        acc = None
        for s in range(per):
            e = per * (g - 1) + s + 2
            if 0 <= e < fx + 5:
                w = v[e * rows2:(e + 1) * rows2]
                w = pltpu.roll(w, fz * s, 1) if s else w
                acc = w if acc is None else acc + w
        pq[g] = acc
    start(yp)

    start(ya[1])
    arrive(ya[0])
    start(zf[0])
    step0 = 4

    def across(own, lo, hi):
        rows = own.shape[0] * own.shape[1]
        other = jnp.where(
            mask_r, hi.reshape(rows, LANES), jnp.where(mask_l, lo.reshape(rows, LANES), 0.0)
        )
        v = jnp.concatenate([own.reshape(rows, LANES), other], axis=1)
        return split(dot_right(v, (w0h, w0l)))

    def level0_own(c):
        at = pl.ds(c * step0, step0)
        hi, lo = across(x_ref[at], l0[at], r0[at])
        zh[at, pl.ds(0, by), :] = hi.reshape(step0, by, 2 * LANES)
        zl[at, pl.ds(0, by), :] = lo.reshape(step0, by, 2 * LANES)

    def level0_halo(x, n):
        at = pl.ds(x, n)
        hi, lo = across(hy[at], hl[at], hr[at])
        zh[at, pl.ds(by, 16), :] = hi.reshape(n, 16, 2 * LANES)
        zl[at, pl.ds(by, 16), :] = lo.reshape(n, 16, 2 * LANES)

    def level0(k):
        hi = zh[k]
        o = mm(m0[...], jnp.concatenate([hi, zl[k], hi], axis=0))
        y0[8 + k] = o[:by, :LANES]
        y1[8 + k] = o[by:, LANES:]

    arrive(za)
    edge = 8 // step0
    for c in range(edge):
        level0_own(c)
        level0_own(bx // step0 - edge + c)
    def spread(dim, n, ref, k0):
        out = []
        for m, d in enumerate([d for d in range(-(n - 1), n) if d]):
            dev = tuple(here[k] + (d if k == dim else 0) for k in range(3))
            copy = pltpu.make_async_remote_copy(
                src_ref=ref(here[dim]), dst_ref=ref(here[dim]),
                send_sem=sg.at[dim, m], recv_sem=rg.at[dim, m],
                device_id=dev, device_id_type=pl.DeviceIdType.MESH,
            )
            land = pltpu.make_async_remote_copy(
                src_ref=ref(here[dim]), dst_ref=ref(here[dim] - d),
                send_sem=sg.at[dim, m], recv_sem=rg.at[dim, m],
                device_id=dev, device_id_type=pl.DeviceIdType.MESH,
            )
            to = inside(here[dim] + d, n)
            fro = inside(here[dim] - d, n)
            out.append((to, fro, copy, land))
        return out

    def begin(copies):
        for to, _, copy, _ in copies:
            pl.when(to)(copy.start)

    def landed(copies):
        for _, fro, _, land in copies:
            pl.when(fro)(land.wait_recv)

    arrive(yp)
    own = [pq[:, pl.ds(0, 8)] + yu[...]]
    if fy > 16:
        own.append(pq[:, pl.ds(8, fy - 16)])
    own.append(pq[:, pl.ds(fy - 8, 8)] + yd[...])
    xg[gx] = jnp.concatenate(own, axis=1)
    ca = spread(0, nx, lambda k: xg.at[k], 0)
    begin(ca)


    pl.loop(edge, bx // step0 - edge, unroll=4)(level0_own)
    arrive(ya[1])
    start(zf[1])
    arrive(zf[0])
    level0_halo(0, 8)
    level0_halo(bx - 8, 8)
    for k in range(8):
        level0(k)
        level0(bx - 8 + k)
    start(xa[0])
    start(hop1)
    arrive(zf[1])
    level0_halo(8, bx - 16)
    pl.loop(8, bx - 8, unroll=True)(level0)

    for p in range(half1 + 2):
        a = restrict_x(y1, 4 + 4 * p)
        b = restrict_x(y1, 6 + 4 * p)
        t1[p] = jnp.where(lane < cz, a, pltpu.roll(b, cz, 1))
    start(xb)
    start(xa[1])

    landed(ca)
    for m in range(np2 * nx):
        acc = None
        for b in range(nx):
            k = m - np2 * b + 1
            if 0 <= k < np2 + 2:
                acc = xg[b, k] if acc is None else acc + xg[b, k]
        g2[gz, gy, m] = acc
    cb = spread(1, ny, lambda k: g2.at[gz, k], 0)
    begin(cb)

    def conv0(p, ts):
        acc = None
        for t in ts:
            v = taps[0, 0, t] * y0[p + t]
            acc = v if acc is None else acc + v
        return acc

    @pl.loop(8, bx - 8, unroll=4)
    def _(p):
        out_ref[p] = conv0(p, range(17))

    def plain(axis, level, n, pad, turned):
        i, j = grids(pad, pad)
        d = (i - j if turned else j - i) + 8
        return pick(taps, level, axis, d, (i < n) & (j < n))

    def rest(n, pad, big, turned_r):
        i, j = grids(*((big, pad) if turned_r else (pad, big)))
        c, f = (j, i) if turned_r else (i, j)
        return cubic(f - 2 * c, (c < n) & (f < 2 * n))

    def operators(axis, n2, first, rows, count):
        n3, n4 = n2 // 2, n2 // 4
        q = up(n2, LANES)
        i, j = grids(rows, q)
        g = first + i
        ok = (i < count) & inside(g, n2)
        one = pick(taps, 2, axis, j - g + 8, ok & (j < n2))
        pr = cubic(g - 2 * j, ok & (j < n3))
        r23, r34 = rest(n3, q, q, False), rest(n4, q, q, False)
        p34 = rest(n4, q, q, True)
        two = exact(exact(pr, plain(axis, 3, n3, q, False)), r23)
        three = exact(exact(exact(exact(pr, p34), plain(axis, 4, n4, q, False)), r34), r23)
        return one, two, three

    n2x, n2y, n2z = nx * fx, ny * fy, nz * fz
    ez, ey, ex = fz + 5, fy + 5, fx + 5
    tz = 40
    ops = operators(2, n2z, gz * fz - 2, tz, ez)
    cols = jnp.concatenate(list(ops) + [jnp.zeros((LANES - 3 * tz, ops[0].shape[1]), F32)], axis=0)
    hi, lo = split(cols.T)
    for ref, v in ((w2h, hi), (w2l, lo)):
        ref[...] = jnp.zeros(ref.shape, BF16)
        for b in range(nz):
            for k in range(per):
                ref[pl.ds(b * LANES + k * fz, fz), pl.ds(k * LANES, LANES)] = v[b * fz:(b + 1) * fz]
    ty = up(ey, 8)
    ops = operators(1, n2y, gy * fy - 2, ty, ey)
    stack(m2, jnp.concatenate(list(ops), axis=0)[:, :n2y], 3)
    tx = up(ex, 8)
    ops = operators(0, n2x, gx * fx - 2, tx, ex)
    tall = [o.T for o in ops]
    for r in range(ex):
        a, b, c = (o[:n2x, r:r + 1] for o in tall)
        c2[r] = jnp.where(lane < tz, a, jnp.where(lane < 2 * tz, b, c))
    i, j = grids(LANES, LANES)
    src = i - jnp.where(i < tz, 0, jnp.where(i < 2 * tz, tz, 2 * tz)) - 2
    e1_z = cubic((j - 2) - 2 * src, (i < 3 * tz) & (src < fz + 3) & (j < top) & inside(gz * cz + j - 2, nz * cz))
    put(pz2, None, exact(e1_z, fine_z))
    i, j = grids(ry1, up(ty, 16))
    stack(py2, cubic((i - 2) - 2 * (j - 2), (j < ey) & (i < cy + 4) & inside(gy * cy + i - 2, ny * cy)), 2)
    for p in range(8):
        out_ref[p] = conv0(p, range(8 - p, 17))
        out_ref[bx - 8 + p] = conv0(bx - 8 + p, range(16 - p))
    arrive(hop1)
    start(hop2)
    arrive(xb)
    n1 = half1 + 10
    to_l, to_r = there(*left).astype(F32), there(*right).astype(F32)
    for k in range(n1):
        if k < 4:
            v = t1l[k]
        elif k < 6:
            v = t1l[k] + (t1[k - 4] * to_l if k == 4 else t1[k - 4])
        elif k < half1 + 4:
            v = t1[k - 4]
        elif k < half1 + 6:
            v = t1r[k - half1 - 4] + (t1[k - 4] * to_r if k == half1 + 5 else t1[k - 4])
        else:
            v = t1r[k - half1 - 4]
        e1[k] = v
        back = pltpu.roll(v, cz, 1)
        if k:
            sw[k - 1] = jnp.where(lane < cz, last, back)
        last = back

    @pl.loop(0, half1 + 2, unroll=5)
    def _(q):
        acc = taps[1, 0, 0] * e1[q]
        for t in range(1, 17):
            acc = acc + taps[1, 0, t] * (sw[q + (t - 1) // 2] if t % 2 else e1[q + t // 2])
        f1[q, pl.ds(16, cy), :] = acc

    start(yb)
    landed(cb)
    cc = spread(2, nz, lambda k: g2.at[k], 0)
    begin(cc)
    landed(cc)
    seen = lambda r: inside(gx * cx + r - 2, nx * cx).astype(F32)
    batch = max(1, min(nx * np2, 256 // n2y))
    for m in range(0, nx * np2, batch):
        v = jnp.concatenate([
            jnp.concatenate([g2[b, :, k].reshape(n2y, LANES) for b in range(nz)], axis=1)
            for k in range(m, m + batch)
        ], axis=0)
        hi, lo = split(dot_right(v, (w2h, w2l)))
        z2h[pl.ds(m, batch)] = hi.reshape(batch, n2y, per * LANES)
        z2l[pl.ds(m, batch)] = lo.reshape(batch, n2y, per * LANES)

    @pl.loop(0, nx * np2, unroll=8)
    def _(m):
        hi = z2h[m]
        o = mm(m2[...], jnp.concatenate([hi, z2l[m], hi], axis=0))
        for k in range(per):
            w = o[:, k * LANES:(k + 1) * LANES]
            y2[per * m + k] = jnp.where(
                lane < tz, w[:ty], jnp.where(lane < 2 * tz, w[ty:2 * ty], w[2 * ty:])
            )

    arrive(yb)
    for q in range(0, half1 + 2, 2):
        o = dot_left(m1, jnp.concatenate([f1[q], f1[q + 1]], axis=1), 3)
        h1[q] = o[:, :LANES]
        h1[q + 1] = o[:, LANES:]
    start(zb)
    parts = []
    for r in range(ex):
        acc = c2[r, pl.ds(0, 1)] * y2[0]
        for q in range(1, n2x):
            acc = acc + c2[r, pl.ds(q, 1)] * y2[q]
        parts.append(acc)
    v = dot_right(jnp.concatenate(parts, axis=0), (pz2, None))
    fill = up(ty, 16) - ty
    pro = []
    for r in range(ex):
        w = v[r * ty:(r + 1) * ty]
        if fill:
            w = jnp.concatenate([w, jnp.zeros((fill, LANES), F32)], axis=0)
        pro.append(dot_left(py2, w, 2))
    arrive(zb)
    inner = lax.rem(lane, cz) < cz // 2
    step1 = 5 if (half1 + 2) % 5 == 0 else 1
    for c in range(0, half1 + 2, step1):
        parts = []
        for q in range(c, c + step1):
            own = h1[q]
            other = jnp.where(inner & has_r, h1r[q], jnp.where(jnp.logical_not(inner) & has_l, h1l[q], 0.0))
            parts.append(jnp.where(lane < cz, own, pltpu.roll(other, cz, 1)))
            parts.append(jnp.where(lane < cz, pltpu.roll(own, cz, 1), other))
        v = dot_right(jnp.concatenate(parts, axis=0), (w1h, w1l))
        for k in range(2 * step1):
            d1[2 * c + k] = v[k * ry1:(k + 1) * ry1]
    for p in range(cx + 4):
        m = (p - 2) // 2 + 2
        if p % 2 == 0:
            w = pro[m]
        else:
            w = 0.5625 * (pro[m] + pro[m + 1]) - 0.0625 * (pro[m - 1] + pro[m + 2])
        d1[p] = (d1[p] + w) * seen(p)

    fill1 = up(ry1, 16) - ry1

    @pl.loop(0, (cx + 4) // 2, unroll=True)
    def _(c):
        v = jnp.concatenate([d1[2 * c], d1[2 * c + 1]], axis=1)
        if fill1:
            v = jnp.concatenate([v, jnp.zeros((fill1, 2 * LANES), F32)], axis=0)
        o = dot_left(py1, v, 2)
        pr[2 * c] = o[:, :LANES]
        pr[2 * c + 1] = o[:, LANES:]

    def finish(m):
        at = m + 2
        for k in range(2):
            p = 2 * m + k
            v = pr[at] if k == 0 else (
                0.5625 * (pr[at] + pr[at + 1]) - 0.0625 * (pr[at - 1] + pr[at + 2])
            )
            if isinstance(m, int):
                v = v + conv0(p, range(8 - p) if p < 8 else range(8 + bx - p, 17))
            out_ref[p] = out_ref[p] + v

    pl.loop(4, cx - 4, unroll=4)(finish)
    for group in (*xa, hop2):
        arrive(group)
    for m in (*range(4), *range(cx - 4, cx)):
        finish(m)

    for group in (*ya, za, *zf, z2, yp, *xa, hop1, hop2, xb, yb, zb):
        left_over(group)
    for group in (ca, cb, cc):
        for to, _, copy, _ in group:
            pl.when(to)(copy.wait_send)


def per_device(counts, charges, kernel_taps):
    nx, ny, nz = counts
    bx, by, bz = dims = charges.shape
    assert bz == LANES
    cx, cy, cz = bx // 2, by // 2, bz // 2
    fx, fy, fz = bx // 4, by // 4, bz // 4
    n2x, n2y, n2z = nx * fx, ny * fy, nz * fz
    per = LANES // fz
    np2 = fx // per
    half1 = cx // 2
    ry1 = up(cy + 4, 8)
    ty = up(fy + 5, 8)
    V = pltpu.VMEM
    wide = max(nx, ny, nz) * 2
    dma = pltpu.SemaphoreType.DMA
    row = lambda n, r: V((n, r, LANES), F32)
    scratch = [
        pltpu.SMEM(kernel_taps.shape, F32), V(dims, F32),
        row(bx, by), row(bx, by), row(bx, 16), row(bx, 16), row(bx, 16),
        V((bx, by + 16, 2 * LANES), BF16), V((bx, by + 16, 2 * LANES), BF16),
        row(5, by), row(bx + 16, by), row(bx + 16, cy),
        row(half1 + 2, cy), row(6, cy), row(6, cy), row(half1 + 10, cy), row(half1 + 9, cy),
        row(half1 + 2, cy + 32), row(half1 + 2, ry1), row(half1 + 2, ry1), row(half1 + 2, ry1),
        row(cx + 4, ry1), row(cx + 4, by),
        row(bx + 16, fy + 16), row(cx + 15, fy + 16),
        row(fx + 5, fy + 16), row(fx + 5, fy + 16), row(fx + 5, fy + 16),
        row(np2 + 2, fy + 16), row(np2 + 2, 8), row(np2 + 2, 8),
        V((nx, np2 + 2, fy, LANES), F32),
        V((nz, ny, nx * np2, fy, LANES), F32),
        V((nx * np2, n2y, per * LANES), BF16), V((nx * np2, n2y, per * LANES), BF16),
        row(n2x, ty),
        V((2 * bz, bz + LANES), BF16), V((2 * bz, bz + LANES), BF16),
        V((by + cy, 3 * (by + 16)), BF16),
        V((2 * cz, bz), BF16), V((2 * cz, bz), BF16),
        V((ry1, 3 * (cy + 32)), BF16),
        V((nz * LANES, per * LANES), BF16), V((nz * LANES, per * LANES), BF16),
        V((3 * ty, 3 * n2y), BF16),
        row(fx + 5, n2x),
        V((LANES, bz), BF16), V((ry1, 2 * up(ty, 16)), BF16),
        V((by, 2 * up(ry1, 16)), BF16),
        V((fy + 16, 2 * by), BF16), V((2 * bz, LANES), BF16),
        dma((5,)), dma((40,)), dma((40,)), dma((3, wide)), dma((3, wide)),
    ]
    return pl.pallas_call(
        functools.partial(kernel, counts, dims),
        out_shape=jax.ShapeDtypeStruct(dims, F32),
        in_specs=[pl.BlockSpec(memory_space=pltpu.HBM)] * 2,
        out_specs=pl.BlockSpec(memory_space=pltpu.VMEM),
        scratch_shapes=scratch,
        compiler_params=pltpu.CompilerParams(
            collective_id=0, has_side_effects=True, vmem_limit_bytes=105 * 2**19
        ),
    )(pltpu.with_memory_space_constraint(kernel_taps, pltpu.HBM), charges)


def solution(mesh):
    counts = tuple(mesh.shape[a] for a in AXES)
    return jax.shard_map(
        functools.partial(per_device, counts), mesh=mesh,
        in_specs=(P("gx", "gy", "gz"), P()), out_specs=P("gx", "gy", "gz"), check_vma=False,
    )
```

```python
import functools

import jax
import jax.numpy as jnp
from jax import lax
from jax.experimental import pallas as pl
from jax.experimental.pallas import tpu as pltpu
from jax.sharding import PartitionSpec as P

F32, BF16 = jnp.float32, jnp.bfloat16
LANES = 128
U0, U1, U2, U3 = 4, 4, 4, 5
AXES = ("gx", "gy", "gz")
ODD = (-0.0625, 0.5625, 0.5625, -0.0625)
SIDES = tuple((a, b) for a in (-1, 0, 1) for b in (-1, 0, 1) if (a, b) != (0, 0))


def split(v):
    hi = v.astype(BF16)
    return hi, (v - hi.astype(F32)).astype(BF16)


def mm(a, b):
    return jnp.dot(a, b, preferred_element_type=F32)


def exact(a, b):
    return jnp.dot(a, b, preferred_element_type=F32, precision=lax.Precision.HIGHEST)


def dot_right(v, w):
    hi, lo = split(v)
    out = mm(hi, w[0][...]) + mm(lo, w[0][...])
    return out if w[1] is None else out + mm(hi, w[1][...])


def dot_left(w_ref, v, terms):
    hi, lo = split(v)
    return mm(w_ref[...], jnp.concatenate([hi, lo, hi][:terms], axis=0))


def grids(rows, cols):
    return (
        lax.broadcasted_iota(jnp.int32, (rows, cols), 0),
        lax.broadcasted_iota(jnp.int32, (rows, cols), 1),
    )


def pick(taps, level, axis, diff, ok):
    out = jnp.zeros(diff.shape, F32)
    for t in range(17):
        out = jnp.where(diff == t, taps[level, axis, t], out)
    return jnp.where(ok, out, 0.0)


def cubic(diff, ok):
    d = jnp.abs(diff)
    out = jnp.where(d == 0, 1.0, jnp.where(d == 1, 0.5625, jnp.where(d == 3, -0.0625, 0.0)))
    return jnp.where(ok, out, 0.0).astype(F32)


def up(n, m):
    return -(-n // m) * m


def inside(v, n):
    return (v >= 0) & (v < n)


def kernel(counts, dims, taps_hbm, x_hbm, out_ref, taps, x_ref, l0, r0, hy, hl, hr, zh, zl, relay, y0, y1, t1, t1l, t1r, e1, sw, f1, h1, h1l, h1r, d1, pr,
           ua, am, v2, v2l, v2r, pq, yu, yd, xg, g2, z2h, z2l, y2,
           w0h, w0l, m0, w1h, w1l, m1, w2h, w2l, m2, c2, pz2, py2, py1, my2, wz2, own_sem, ss, rs, sg, rg):
    nx, ny, nz = counts
    bx, by, bz = dims
    here = tuple(lax.axis_index(a) for a in AXES)
    loads = [
        pltpu.make_async_copy(x_hbm.at[pl.ds(k, bx // 4)], x_ref.at[pl.ds(k, bx // 4)], own_sem.at[4 * k // bx])
        for k in range(0, bx, bx // 4)
    ]
    loads.append(pltpu.make_async_copy(taps_hbm, taps, own_sem.at[4]))
    for load in loads:
        load.start()
    gx, gy, gz = here
    cx, cy, cz = bx // 2, by // 2, bz // 2
    fx, fy, fz = bx // 4, by // 4, bz // 4
    half1 = cx // 2
    per = LANES // fz
    np2 = fx // per

    def there(dx, dy, dz):
        return inside(gx + dx, nx) & inside(gy + dy, ny) & inside(gz + dz, nz)

    partners = []
    for dim, n in enumerate(counts):
        for d in range(1, n):
            for sgn in (-d, d):
                partners.append(tuple(sgn if k == dim else 0 for k in range(3)))
    barrier = pltpu.get_barrier_semaphore()
    total = jnp.int32(0)
    for p in partners:
        ok = there(*p)
        total = total + ok.astype(jnp.int32)

        @pl.when(ok)
        def _(p=p):
            pl.semaphore_signal(
                barrier, inc=1, device_id=(gx + p[0], gy + p[1], gz + p[2]),
                device_id_type=pl.DeviceIdType.MESH,
            )

    def clear(ref, d, *at):
        @pl.when(jnp.logical_not(there(*d)))
        def _():
            view = ref.at[at]
            view[...] = jnp.zeros(view.shape, F32)

    every = slice(None)
    clear(hy, (0, -1, 0), every, pl.ds(0, 8))
    clear(hy, (0, 1, 0), every, pl.ds(8, 8))
    clear(y0, (-1, 0, 0), pl.ds(0, 8))
    clear(y0, (1, 0, 0), pl.ds(8 + bx, 8))
    clear(t1l, (-1, 0, 0), every)
    clear(t1r, (1, 0, 0), every)
    clear(f1, (0, -1, 0), every, pl.ds(0, 16))
    clear(f1, (0, 1, 0), every, pl.ds(16 + cy, 16))
    clear(yu, (0, -1, 0), every)
    clear(yd, (0, 1, 0), every)
    f1[:, pl.ds(0, 6)] = jnp.zeros((half1 + 2, 6, LANES), F32)
    f1[:, pl.ds(cy + 26, 6)] = jnp.zeros((half1 + 2, 6, LANES), F32)
    for ref in (ua, y1):
        ref[pl.ds(0, 8)] = jnp.zeros((8,) + ref.shape[1:], F32)
        ref[pl.ds(8 + bx, 8)] = jnp.zeros((8,) + ref.shape[1:], F32)
    am[pl.ds(0, 6)] = jnp.zeros((6,) + am.shape[1:], F32)
    am[pl.ds(cx + 9, 6)] = jnp.zeros((6,) + am.shape[1:], F32)
    right, left, ahead, behind, above, below = (
        (1, 0, 0), (-1, 0, 0), (0, 1, 0), (0, -1, 0), (0, 0, 1), (0, 0, -1)
    )
    def put(h, l, v):
        hi, lo = split(v)
        h[...] = hi
        if l is not None:
            l[...] = lo

    def stack(ref, v, terms):
        hi, lo = split(v)
        ref[...] = jnp.concatenate([hi, hi, lo][:terms], axis=1)

    def twice(pos, at, base, n):
        out = jnp.zeros(pos.shape, F32)
        for k, w in ((-3, -0.0625), (-1, 0.5625), (0, 1.0), (1, 0.5625), (3, -0.0625)):
            m = 2 * at + k
            out = out + w * cubic(pos - 2 * m, inside(base + m, n))
        return out

    def restrict_x(ref, at):
        return (
            ref[at] + 0.5625 * (ref[at - 1] + ref[at + 1]) - 0.0625 * (ref[at - 3] + ref[at + 3])
        )

    lane = lax.broadcasted_iota(jnp.int32, (1, LANES), 1)
    has_r, has_l = there(*above), there(*below)
    mask_r, mask_l = (lane < LANES // 2) & has_r, (lane >= LANES // 2) & has_l
    rows2 = fy + 16
    i, j = grids(rows2, by)
    stack(my2, twice(j, jnp.where(i < fy + 8, i, i - rows2), gy * cy, ny * cy), 2)
    i, j = grids(2 * bz, LANES)
    pos = jnp.where(i < bz + bz // 2, i, i - 2 * bz)
    put(wz2, None, jnp.where(j < fz, twice(pos, j, gz * cz, nz * cz), 0.0))


    for k in range(4):
        loads[k].wait()
        for c in range(k * (bx // 8), (k + 1) * (bx // 8)):
            o = dot_left(my2, jnp.concatenate([x_ref[2 * c], x_ref[2 * c + 1]], axis=1), 2)
            ua[8 + 2 * c] = o[:, :LANES]
            ua[9 + 2 * c] = o[:, LANES:]

    for m in range(-1, cx + 2):
        am[m + 7] = restrict_x(ua, 8 + 2 * m) * inside(gx * cx + m, nx * cx).astype(F32)
    for e in range(fx + 5):
        v2[e] = restrict_x(am, 3 + 2 * e)
    pl.semaphore_wait(barrier, total)

    count = [0]

    def remote(src, dst, d, to=None, fro=None):
        k = count[0]
        count[0] += 1
        copy = pltpu.make_async_remote_copy(
            src_ref=src, dst_ref=dst, send_sem=ss.at[k], recv_sem=rs.at[k],
            device_id=(gx + d[0], gy + d[1], gz + d[2]), device_id_type=pl.DeviceIdType.MESH,
        )
        to = there(*d) if to is None else to
        fro = there(-d[0], -d[1], -d[2]) if fro is None else fro
        return to, fro, copy

    def start(copies):
        for to, _, copy in copies:
            pl.when(to)(copy.start)

    def arrive(copies):
        for _, fro, copy in copies:
            pl.when(fro)(copy.wait_recv)

    def left_over(copies):
        for to, _, copy in copies:
            pl.when(to)(copy.wait_send)

    ends = (pl.ds(0, 8), pl.ds(bx - 8, 8)), (pl.ds(8, bx - 16),)
    ya, zf = [], []
    for xs in ends:
        ya.append([
            remote(x_ref.at[x, pl.ds(by - 8, 8)], hy.at[x, pl.ds(0, 8)], ahead) for x in xs
        ] + [
            remote(x_ref.at[x, pl.ds(0, 8)], hy.at[x, pl.ds(8, 8)], behind) for x in xs
        ])
        zf.append([remote(hy.at[x], hl.at[x], above) for x in xs] + [remote(hy.at[x], hr.at[x], below) for x in xs])
    za = [
        [remote(x_ref.at[x], ref.at[x], d) for x in xs for ref, d in ((l0, above), (r0, below))]
        for xs in ends
    ]
    z2 = [remote(v2, v2l, above), remote(v2, v2r, below)]
    yp = [
        remote(pq.at[:, pl.ds(fy, 8)], yu, ahead),
        remote(pq.at[:, pl.ds(fy + 8, 8)], yd, behind),
    ]
    mid_l, mid_r = (gx == 1, gx == 2) if nx == 4 else (jnp.bool_(False), jnp.bool_(False))
    end_l, end_r = (gx == 0, gx == 3) if nx == 4 else (jnp.bool_(False), jnp.bool_(False))
    near, rest = 3, 5

    def to_left(k, n, **ok):
        return remote(y0.at[pl.ds(8 + k, n)], y0.at[pl.ds(8 + bx + k, n)], left, **ok)

    def to_right(k, n, **ok):
        return remote(y0.at[pl.ds(bx + k, n)], y0.at[pl.ds(k, n)], right, **ok)

    xa = [
        [to_left(0, 1), to_right(0, 1)],
        [
            to_left(1, near - 1),
            to_left(near, rest, to=there(*left) & jnp.logical_not(mid_r), fro=there(*right) & jnp.logical_not(mid_l)),
            to_right(1, near - 1),
            to_right(near, rest, to=there(*right) & jnp.logical_not(mid_l), fro=there(*left) & jnp.logical_not(mid_r)),
        ],
    ]
    hop1, hop2 = [], []
    if nx == 4:
        hop1 = [
            remote(y0.at[pl.ds(bx + near, rest)], relay, (2, 0, 0), to=mid_l, fro=end_r),
            remote(y0.at[pl.ds(8 + near, rest)], relay, (-2, 0, 0), to=mid_r, fro=end_l),
        ]
        hop2 = [
            remote(relay, y0.at[pl.ds(near, rest)], left, to=end_r, fro=mid_r),
            remote(relay, y0.at[pl.ds(8 + bx + near, rest)], right, to=end_l, fro=mid_l),
        ]
    xb = [remote(t1.at[pl.ds(0, 6)], t1r, left), remote(t1.at[pl.ds(half1 - 4, 6)], t1l, right)]
    yb = [
        remote(f1.at[:, pl.ds(cy + 6, 10)], f1.at[:, pl.ds(6, 10)], ahead),
        remote(f1.at[:, pl.ds(16, 10)], f1.at[:, pl.ds(16 + cy, 10)], behind),
    ]
    zb = [remote(h1, h1l, above), remote(h1, h1r, below)]
    start(z2)
    start(ya[0])
    start(za[0])
    loads[4].wait()
    i, j = grids(2 * bz, bz)
    pos = jnp.where(i < bz + bz // 2, i, i - 2 * bz)
    k0 = pick(taps, 0, 2, pos - j + 8, inside(pos, bz + 8) | inside(pos + 8, 8))
    rz = cubic(pos - 2 * j, j < cz)
    put(w0h, w0l, jnp.concatenate([k0, rz], axis=1))
    i, j = grids(by + cy, by + 16)
    j = jnp.where(j < by, j + 8, jnp.where(j < by + 8, j - by, j))
    stack(m0, jnp.where(i < by, pick(taps, 0, 1, j - i, i < by), cubic(j - 8 - 2 * (i - by), i >= by)), 3)

    i, j = grids(2 * cz, LANES)
    pos = jnp.where(i < cz + cz // 2, i, i - 2 * cz)
    kk = j - 2
    top = cz + 4
    ok = (j < top) & inside(gz * cz + kk, nz * cz)
    k1 = pick(taps, 1, 2, pos - kk + 8, ok)
    i, j = grids(LANES, bz)
    fine_z = cubic(j - 2 * (i - 2), i < top)
    put(w1h, w1l, exact(k1, fine_z))
    ry1 = up(cy + 4, 8)
    i, j = grids(ry1, cy + 32)
    ok = (i < cy + 4) & inside(gy * cy + i - 2, ny * cy)
    stack(m1, pick(taps, 1, 1, j - 16 - (i - 2) + 8, ok), 3)
    i, j = grids(by, up(ry1, 16))
    stack(py1, cubic(i - 2 * (j - 2), j < cy + 4), 2)

    arrive(z2)
    parts = []
    for e in range(fx + 5):
        other = jnp.where(mask_r, v2r[e], jnp.where(mask_l, v2l[e], 0.0))
        parts.append(jnp.concatenate([v2[e], other], axis=1))
    v = dot_right(jnp.concatenate(parts, axis=0), (wz2, None))
    for g in range(np2 + 2):
        acc = None
        for s in range(per):
            e = per * (g - 1) + s + 2
            if 0 <= e < fx + 5:
                w = v[e * rows2:(e + 1) * rows2]
                w = pltpu.roll(w, fz * s, 1) if s else w
                acc = w if acc is None else acc + w
        pq[g] = acc
    start(yp)

    start(za[1])
    start(ya[1])
    arrive(ya[0])
    start(zf[0])
    step0 = 4

    def across(own, lo, hi):
        rows = own.shape[0] * own.shape[1]
        other = jnp.where(
            mask_r, hi.reshape(rows, LANES), jnp.where(mask_l, lo.reshape(rows, LANES), 0.0)
        )
        v = jnp.concatenate([own.reshape(rows, LANES), other], axis=1)
        return split(dot_right(v, (w0h, w0l)))

    def level0_own(c):
        at = pl.ds(c * step0, step0)
        hi, lo = across(x_ref[at], l0[at], r0[at])
        zh[at, pl.ds(0, by), :] = hi.reshape(step0, by, 2 * LANES)
        zl[at, pl.ds(0, by), :] = lo.reshape(step0, by, 2 * LANES)

    def level0_halo(x, n):
        at = pl.ds(x, n)
        hi, lo = across(hy[at], hl[at], hr[at])
        zh[at, pl.ds(by, 16), :] = hi.reshape(n, 16, 2 * LANES)
        zl[at, pl.ds(by, 16), :] = lo.reshape(n, 16, 2 * LANES)

    def level0(k):
        hi = zh[k]
        o = mm(m0[...], jnp.concatenate([hi, zl[k], hi], axis=0))
        y0[8 + k] = o[:by, :LANES]
        y1[8 + k] = o[by:, LANES:]

    arrive(za[0])
    edge = 8 // step0
    for c in range(edge):
        level0_own(c)
        level0_own(bx // step0 - edge + c)
    def spread(dim, n, ref, k0):
        out = []
        for m, d in enumerate([d for d in range(-(n - 1), n) if d]):
            dev = tuple(here[k] + (d if k == dim else 0) for k in range(3))
            copy = pltpu.make_async_remote_copy(
                src_ref=ref(here[dim]), dst_ref=ref(here[dim]),
                send_sem=sg.at[dim, m], recv_sem=rg.at[dim, m],
                device_id=dev, device_id_type=pl.DeviceIdType.MESH,
            )
            land = pltpu.make_async_remote_copy(
                src_ref=ref(here[dim]), dst_ref=ref(here[dim] - d),
                send_sem=sg.at[dim, m], recv_sem=rg.at[dim, m],
                device_id=dev, device_id_type=pl.DeviceIdType.MESH,
            )
            to = inside(here[dim] + d, n)
            fro = inside(here[dim] - d, n)
            out.append((to, fro, copy, land))
        return out

    def begin(copies):
        for to, _, copy, _ in copies:
            pl.when(to)(copy.start)

    def landed(copies):
        for _, fro, _, land in copies:
            pl.when(fro)(land.wait_recv)

    arrive(yp)
    own = [pq[:, pl.ds(0, 8)] + yu[...]]
    if fy > 16:
        own.append(pq[:, pl.ds(8, fy - 16)])
    own.append(pq[:, pl.ds(fy - 8, 8)] + yd[...])
    xg[gx] = jnp.concatenate(own, axis=1)
    ca = spread(0, nx, lambda k: xg.at[k], 0)
    begin(ca)


    arrive(za[1])
    pl.loop(edge, bx // step0 - edge, unroll=4)(level0_own)
    arrive(ya[1])
    start(zf[1])
    arrive(zf[0])
    level0_halo(0, 8)
    level0_halo(bx - 8, 8)
    for k in range(8):
        level0(k)
        level0(bx - 8 + k)
    start(xa[0])
    start(hop1)
    arrive(zf[1])
    level0_halo(8, bx - 16)
    pl.loop(8, bx - 8, unroll=True)(level0)

    for p in range(half1 + 2):
        a = restrict_x(y1, 4 + 4 * p)
        b = restrict_x(y1, 6 + 4 * p)
        t1[p] = jnp.where(lane < cz, a, pltpu.roll(b, cz, 1))
    start(xb)
    start(xa[1])

    landed(ca)
    for m in range(np2 * nx):
        acc = None
        for b in range(nx):
            k = m - np2 * b + 1
            if 0 <= k < np2 + 2:
                acc = xg[b, k] if acc is None else acc + xg[b, k]
        g2[gz, gy, m] = acc
    cb = spread(1, ny, lambda k: g2.at[gz, k], 0)
    begin(cb)

    def conv0(p, ts):
        acc = None
        for t in ts:
            v = taps[0, 0, t] * y0[p + t]
            acc = v if acc is None else acc + v
        return acc

    @pl.loop(8, bx - 8, unroll=4)
    def _(p):
        out_ref[p] = conv0(p, range(17))

    def plain(axis, level, n, pad, turned):
        i, j = grids(pad, pad)
        d = (i - j if turned else j - i) + 8
        return pick(taps, level, axis, d, (i < n) & (j < n))

    def rest(n, pad, big, turned_r):
        i, j = grids(*((big, pad) if turned_r else (pad, big)))
        c, f = (j, i) if turned_r else (i, j)
        return cubic(f - 2 * c, (c < n) & (f < 2 * n))

    def operators(axis, n2, first, rows, count):
        n3, n4 = n2 // 2, n2 // 4
        q = up(n2, LANES)
        i, j = grids(rows, q)
        g = first + i
        ok = (i < count) & inside(g, n2)
        one = pick(taps, 2, axis, j - g + 8, ok & (j < n2))
        pr = cubic(g - 2 * j, ok & (j < n3))
        r23, r34 = rest(n3, q, q, False), rest(n4, q, q, False)
        p34 = rest(n4, q, q, True)
        two = exact(exact(pr, plain(axis, 3, n3, q, False)), r23)
        three = exact(exact(exact(exact(pr, p34), plain(axis, 4, n4, q, False)), r34), r23)
        return one, two, three

    n2x, n2y, n2z = nx * fx, ny * fy, nz * fz
    ez, ey, ex = fz + 5, fy + 5, fx + 5
    tz = 40
    ops = operators(2, n2z, gz * fz - 2, tz, ez)
    cols = jnp.concatenate(list(ops) + [jnp.zeros((LANES - 3 * tz, ops[0].shape[1]), F32)], axis=0)
    hi, lo = split(cols.T)
    for ref, v in ((w2h, hi), (w2l, lo)):
        ref[...] = jnp.zeros(ref.shape, BF16)
        for b in range(nz):
            for k in range(per):
                ref[pl.ds(b * LANES + k * fz, fz), pl.ds(k * LANES, LANES)] = v[b * fz:(b + 1) * fz]
    ty = up(ey, 8)
    ops = operators(1, n2y, gy * fy - 2, ty, ey)
    stack(m2, jnp.concatenate(list(ops), axis=0)[:, :n2y], 3)
    tx = up(ex, 8)
    ops = operators(0, n2x, gx * fx - 2, tx, ex)
    tall = [o.T for o in ops]
    for r in range(ex):
        a, b, c = (o[:n2x, r:r + 1] for o in tall)
        c2[r] = jnp.where(lane < tz, a, jnp.where(lane < 2 * tz, b, c))
    i, j = grids(LANES, LANES)
    src = i - jnp.where(i < tz, 0, jnp.where(i < 2 * tz, tz, 2 * tz)) - 2
    e1_z = cubic((j - 2) - 2 * src, (i < 3 * tz) & (src < fz + 3) & (j < top) & inside(gz * cz + j - 2, nz * cz))
    put(pz2, None, exact(e1_z, fine_z))
    i, j = grids(ry1, up(ty, 16))
    stack(py2, cubic((i - 2) - 2 * (j - 2), (j < ey) & (i < cy + 4) & inside(gy * cy + i - 2, ny * cy)), 2)
    for p in range(8):
        out_ref[p] = conv0(p, range(8 - p, 17))
        out_ref[bx - 8 + p] = conv0(bx - 8 + p, range(16 - p))
    arrive(hop1)
    start(hop2)
    arrive(xb)
    n1 = half1 + 10
    to_l, to_r = there(*left).astype(F32), there(*right).astype(F32)
    for k in range(n1):
        if k < 4:
            v = t1l[k]
        elif k < 6:
            v = t1l[k] + (t1[k - 4] * to_l if k == 4 else t1[k - 4])
        elif k < half1 + 4:
            v = t1[k - 4]
        elif k < half1 + 6:
            v = t1r[k - half1 - 4] + (t1[k - 4] * to_r if k == half1 + 5 else t1[k - 4])
        else:
            v = t1r[k - half1 - 4]
        e1[k] = v
        back = pltpu.roll(v, cz, 1)
        if k:
            sw[k - 1] = jnp.where(lane < cz, last, back)
        last = back

    @pl.loop(0, half1 + 2, unroll=5)
    def _(q):
        acc = taps[1, 0, 0] * e1[q]
        for t in range(1, 17):
            acc = acc + taps[1, 0, t] * (sw[q + (t - 1) // 2] if t % 2 else e1[q + t // 2])
        f1[q, pl.ds(16, cy), :] = acc

    start(yb)
    landed(cb)
    cc = spread(2, nz, lambda k: g2.at[k], 0)
    begin(cc)
    landed(cc)
    seen = lambda r: inside(gx * cx + r - 2, nx * cx).astype(F32)
    batch = max(1, min(nx * np2, 256 // n2y))
    for m in range(0, nx * np2, batch):
        v = jnp.concatenate([
            jnp.concatenate([g2[b, :, k].reshape(n2y, LANES) for b in range(nz)], axis=1)
            for k in range(m, m + batch)
        ], axis=0)
        hi, lo = split(dot_right(v, (w2h, w2l)))
        z2h[pl.ds(m, batch)] = hi.reshape(batch, n2y, per * LANES)
        z2l[pl.ds(m, batch)] = lo.reshape(batch, n2y, per * LANES)

    @pl.loop(0, nx * np2, unroll=8)
    def _(m):
        hi = z2h[m]
        o = mm(m2[...], jnp.concatenate([hi, z2l[m], hi], axis=0))
        for k in range(per):
            w = o[:, k * LANES:(k + 1) * LANES]
            y2[per * m + k] = jnp.where(
                lane < tz, w[:ty], jnp.where(lane < 2 * tz, w[ty:2 * ty], w[2 * ty:])
            )

    arrive(yb)
    for q in range(0, half1 + 2, 2):
        o = dot_left(m1, jnp.concatenate([f1[q], f1[q + 1]], axis=1), 3)
        h1[q] = o[:, :LANES]
        h1[q + 1] = o[:, LANES:]
    start(zb)
    parts = []
    for r in range(ex):
        acc = c2[r, pl.ds(0, 1)] * y2[0]
        for q in range(1, n2x):
            acc = acc + c2[r, pl.ds(q, 1)] * y2[q]
        parts.append(acc)
    v = dot_right(jnp.concatenate(parts, axis=0), (pz2, None))
    fill = up(ty, 16) - ty
    pro = []
    for r in range(ex):
        w = v[r * ty:(r + 1) * ty]
        if fill:
            w = jnp.concatenate([w, jnp.zeros((fill, LANES), F32)], axis=0)
        pro.append(dot_left(py2, w, 2))
    arrive(zb)
    inner = lax.rem(lane, cz) < cz // 2
    step1 = 5 if (half1 + 2) % 5 == 0 else 1
    for c in range(0, half1 + 2, step1):
        parts = []
        for q in range(c, c + step1):
            own = h1[q]
            other = jnp.where(inner & has_r, h1r[q], jnp.where(jnp.logical_not(inner) & has_l, h1l[q], 0.0))
            parts.append(jnp.where(lane < cz, own, pltpu.roll(other, cz, 1)))
            parts.append(jnp.where(lane < cz, pltpu.roll(own, cz, 1), other))
        v = dot_right(jnp.concatenate(parts, axis=0), (w1h, w1l))
        for k in range(2 * step1):
            d1[2 * c + k] = v[k * ry1:(k + 1) * ry1]
    for p in range(cx + 4):
        m = (p - 2) // 2 + 2
        if p % 2 == 0:
            w = pro[m]
        else:
            w = 0.5625 * (pro[m] + pro[m + 1]) - 0.0625 * (pro[m - 1] + pro[m + 2])
        d1[p] = (d1[p] + w) * seen(p)

    fill1 = up(ry1, 16) - ry1

    @pl.loop(0, (cx + 4) // 2, unroll=True)
    def _(c):
        v = jnp.concatenate([d1[2 * c], d1[2 * c + 1]], axis=1)
        if fill1:
            v = jnp.concatenate([v, jnp.zeros((fill1, 2 * LANES), F32)], axis=0)
        o = dot_left(py1, v, 2)
        pr[2 * c] = o[:, :LANES]
        pr[2 * c + 1] = o[:, LANES:]

    def finish(m):
        at = m + 2
        for k in range(2):
            p = 2 * m + k
            v = pr[at] if k == 0 else (
                0.5625 * (pr[at] + pr[at + 1]) - 0.0625 * (pr[at - 1] + pr[at + 2])
            )
            if isinstance(m, int):
                v = v + conv0(p, range(8 - p) if p < 8 else range(8 + bx - p, 17))
            out_ref[p] = out_ref[p] + v

    pl.loop(4, cx - 4, unroll=4)(finish)
    for group in (*xa, hop2):
        arrive(group)
    for m in (*range(4), *range(cx - 4, cx)):
        finish(m)

    for group in (*ya, *za, *zf, z2, yp, *xa, hop1, hop2, xb, yb, zb):
        left_over(group)
    for group in (ca, cb, cc):
        for to, _, copy, _ in group:
            pl.when(to)(copy.wait_send)


def per_device(counts, charges, kernel_taps):
    nx, ny, nz = counts
    bx, by, bz = dims = charges.shape
    assert bz == LANES
    cx, cy, cz = bx // 2, by // 2, bz // 2
    fx, fy, fz = bx // 4, by // 4, bz // 4
    n2x, n2y, n2z = nx * fx, ny * fy, nz * fz
    per = LANES // fz
    np2 = fx // per
    half1 = cx // 2
    ry1 = up(cy + 4, 8)
    ty = up(fy + 5, 8)
    V = pltpu.VMEM
    wide = max(nx, ny, nz) * 2
    dma = pltpu.SemaphoreType.DMA
    row = lambda n, r: V((n, r, LANES), F32)
    scratch = [
        pltpu.SMEM(kernel_taps.shape, F32), V(dims, F32),
        row(bx, by), row(bx, by), row(bx, 16), row(bx, 16), row(bx, 16),
        V((bx, by + 16, 2 * LANES), BF16), V((bx, by + 16, 2 * LANES), BF16),
        row(5, by), row(bx + 16, by), row(bx + 16, cy),
        row(half1 + 2, cy), row(6, cy), row(6, cy), row(half1 + 10, cy), row(half1 + 9, cy),
        row(half1 + 2, cy + 32), row(half1 + 2, ry1), row(half1 + 2, ry1), row(half1 + 2, ry1),
        row(cx + 4, ry1), row(cx + 4, by),
        row(bx + 16, fy + 16), row(cx + 15, fy + 16),
        row(fx + 5, fy + 16), row(fx + 5, fy + 16), row(fx + 5, fy + 16),
        row(np2 + 2, fy + 16), row(np2 + 2, 8), row(np2 + 2, 8),
        V((nx, np2 + 2, fy, LANES), F32),
        V((nz, ny, nx * np2, fy, LANES), F32),
        V((nx * np2, n2y, per * LANES), BF16), V((nx * np2, n2y, per * LANES), BF16),
        row(n2x, ty),
        V((2 * bz, bz + LANES), BF16), V((2 * bz, bz + LANES), BF16),
        V((by + cy, 3 * (by + 16)), BF16),
        V((2 * cz, bz), BF16), V((2 * cz, bz), BF16),
        V((ry1, 3 * (cy + 32)), BF16),
        V((nz * LANES, per * LANES), BF16), V((nz * LANES, per * LANES), BF16),
        V((3 * ty, 3 * n2y), BF16),
        row(fx + 5, n2x),
        V((LANES, bz), BF16), V((ry1, 2 * up(ty, 16)), BF16),
        V((by, 2 * up(ry1, 16)), BF16),
        V((fy + 16, 2 * by), BF16), V((2 * bz, LANES), BF16),
        dma((5,)), dma((40,)), dma((40,)), dma((3, wide)), dma((3, wide)),
    ]
    return pl.pallas_call(
        functools.partial(kernel, counts, dims),
        out_shape=jax.ShapeDtypeStruct(dims, F32),
        in_specs=[pl.BlockSpec(memory_space=pltpu.HBM)] * 2,
        out_specs=pl.BlockSpec(memory_space=pltpu.VMEM),
        scratch_shapes=scratch,
        compiler_params=pltpu.CompilerParams(
            collective_id=0, has_side_effects=True, vmem_limit_bytes=105 * 2**19
        ),
    )(pltpu.with_memory_space_constraint(kernel_taps, pltpu.HBM), charges)


def solution(mesh):
    counts = tuple(mesh.shape[a] for a in AXES)
    return jax.shard_map(
        functools.partial(per_device, counts), mesh=mesh,
        in_specs=(P("gx", "gy", "gz"), P()), out_specs=P("gx", "gy", "gz"), check_vma=False,
    )
```
